256 devices in a mesh: horiz: 16 (over y, x), depth: 16 (over z, core).
Axes of the slice: x: 4, y: 4, z: 8, core: 2. Of those that a mesh axis runs over, the one named last changes fastest.
Arguments:
- fields: float32 [3, 512, 512, 256], P(None, 'depth', 'horiz'), may hold values from -6 to 6
- diffusivity: float32 [512, 512, 256], P('depth', 'horiz'), may hold values from 0.05 to 0.24
- offsets: int32 [512], P('horiz'), may hold values from 0 to 3
- coupling: float32 [4, 512], P(None, 'depth'), may hold values from 200 to 1600, as said below
- inverse: float32 [4, 512, 32], P(None, 'depth'), as said below
Outputs:
- advanced: float32 [3, 512, 512, 256], P(None, 'depth', 'horiz')
The draws below stay inside these ranges and needn't reach their ends.
Inputs may be any that keep to these rules, and one draw needn't show every extreme that they name: coupling[o, k] = coupling[0, k + o] wherever both exist. inverse[o, r * 32 + i, j] is entry (i, j) of the inverse of a block matrix: on the levels k of block r it has diagonal 1 + coupling[o, k] + coupling[o, k + 1] (the first term 0 for k = 0, the second 0 for k = 511) and -coupling[o, k] between levels k - 1 and k; in every block, row and column 31 are those of the identity.
All inputs are finite; a program needn't handle non-finite values.
Results may differ from the reference program's by a relative error of at most 0.0003.
Values sent between devices are 32-bit elements; how exact they have to be, the bound alone decides.
A program may use at most 64 MiB of HBM per device.

```python
import jax
import jax.numpy as jnp
from jax import lax

LEV_DEV = 32
NY = 256
NOFF = 4
NZ = 512
NX = 512


def coupling_profile(key):
    base_key = jax.random.fold_in(key, 4211)
    profile = jnp.exp(jax.random.uniform(base_key, (NZ + NOFF,), jnp.float32, jnp.log(200.0), jnp.log(1600.0)))
    places = jnp.arange(NOFF)[:, None] + jnp.arange(NZ)[None, :]
    return profile[places]


def draw_coupling(key, part):
    return coupling_profile(key)


def draw_inverse(key, part):
    table = coupling_profile(key)
    level_count = LEV_DEV
    blocks = NZ // level_count
    levels_now = jnp.arange(NZ).reshape(blocks, level_count)
    lower_part = jnp.where(levels_now[None] > 0, table.reshape(NOFF, blocks, level_count), 0.0)
    upper_table = jnp.concatenate([table[:, 1:], jnp.zeros((NOFF, 1), jnp.float32)], axis=1)
    upper_part = upper_table.reshape(NOFF, blocks, level_count)
    main_part = 1.0 + lower_part + upper_part
    unit = jnp.eye(level_count, dtype=jnp.float32)
    below_unit = jnp.eye(level_count, k=-1, dtype=jnp.float32)
    above_unit = jnp.eye(level_count, k=1, dtype=jnp.float32)
    matrix = main_part[..., :, None] * unit - lower_part[..., :, None] * below_unit - upper_part[..., :, None] * above_unit
    last_mark = (jnp.arange(level_count) == level_count - 1).astype(jnp.float32)
    keep_mark = 1.0 - last_mark
    cut_matrix = matrix * keep_mark[:, None] * keep_mark[None, :] + last_mark[:, None] * last_mark[None, :]
    inverted = jnp.linalg.inv(cut_matrix)
    return inverted.reshape(NOFF, NZ, level_count).astype(jnp.float32)


def place_ends(drawn, own_key, smallest, largest):
    index_at = [jax.random.randint(jax.random.fold_in(own_key, axis), (), 0, length) for axis, length in enumerate(drawn.shape)]
    longest = drawn.shape.index(max(drawn.shape))
    neighbour = index_at[:longest] + [(index_at[longest] + 1) % drawn.shape[longest]] + index_at[longest + 1:]
    return drawn.at[tuple(index_at)].set(smallest).at[tuple(neighbour)].set(largest)


def block_levels(own_key, shape, cuts, low, top_value):
    level, own = 1.0, jax.random.fold_in(own_key, 6)
    for axis_at, parts in cuts:
        heights = jnp.exp(jax.random.uniform(jax.random.fold_in(own, axis_at), (parts,), jnp.float32, low / len(cuts), top_value / len(cuts)))
        level = level * jnp.repeat(heights, shape[axis_at] // parts).reshape([-1 if axis == axis_at else 1 for axis in range(len(shape))])
    return level


def scatter_about(key, shape, width, bound, split=(), kind=jnp.bfloat16):
    result = width * jax.random.normal(key, shape, jnp.float32)
    if split:
        result = result * block_levels(key, shape, split, -0.22, 0.18)
    return jnp.clip(result, -bound, bound).astype(kind)


def setup_inputs(seed: int = 0) -> dict:
    splits = jax.random.split(jax.random.key(seed), 6)
    return {
        "fields": scatter_about(splits[0], (3, NZ, NX, NY), 1.0, 6.0, ((1, 16), (2, 16)), jnp.float32),
        "diffusivity": jnp.clip(0.05 + 0.19 * jax.random.uniform(splits[1], (NZ, NX, NY), jnp.float32) ** block_levels(splits[1], (NZ, NX, NY), ((0, 16), (1, 16)), -0.2, 0.2), 0.05, 0.24),
        "offsets": place_ends(jax.random.randint(splits[2], (NX,), 0, NOFF), jax.random.fold_in(splits[2], 1), 0, NOFF - 1).astype(jnp.int32),
        "coupling": draw_coupling(jax.random.fold_in(splits[5], 71), 0),
        "inverse": draw_inverse(jax.random.fold_in(splits[5], 71), 0),
    }


exact_mode = lax.Precision.HIGHEST
wave_gain = 0.5

def tendency(centre, east_side, west_side, diffusivity):
    north_side = jnp.roll(centre, -1, axis=3)
    south_side = jnp.roll(centre, 1, axis=3)
    laplace = east_side + west_side + north_side + south_side - 4.0 * centre
    slope_along = 0.5 * (east_side - west_side)
    slope_across = 0.5 * (north_side - south_side)
    pushed = centre + diffusivity[None] * laplace
    first_part = pushed[0] - wave_gain * slope_along[2]
    second_part = pushed[1] - wave_gain * slope_across[2]
    third_part = pushed[2] - wave_gain * (slope_along[0] + slope_across[1])
    return jnp.stack([first_part, second_part, third_part])

def eliminate(level_slab, inverse_rows, coupling_rows, selector, block_index, blocks):
    chosen = jnp.einsum('jo,oab->jab', selector, inverse_rows, precision=exact_mode)
    line_coupling = jnp.dot(selector, coupling_rows, precision=exact_mode)
    solved = jnp.einsum('jab,fbjy->fajy', chosen, level_slab, precision=exact_mode)
    below_face = line_coupling[:, 0]
    upper_gate = line_coupling[:, -1]
    lower_gate = jnp.where(block_index > 0, below_face, jnp.zeros_like(below_face))
    spike_low = chosen[:, :, 0] * lower_gate[:, None]
    spike_high = chosen[:, :, -2] * upper_gate[:, None]
    return (solved, spike_low, spike_high, below_face, upper_gate)

def interface_rows(solved, spike_low, spike_high, upper_gate, got_rows, got_lines):
    lower_band = -upper_gate * spike_low[:, -2]
    main_band = 1.0 + upper_gate + got_lines[0] - upper_gate * spike_high[:, -2] - got_lines[1]
    upper_band = -got_lines[2]
    target = solved[:, -1] + upper_gate[None, :, None] * solved[:, -2] + got_rows
    return (lower_band, main_band, upper_band, target)

def thomas(lower_band, main_band, upper_band, target):

    def forward_step(state_now, row_data):
        prev_ratio, prev_value = state_now
        low_row, main_row, up_row, target_row = row_data
        pivot_value = main_row - low_row * prev_ratio
        ratio_now = up_row / pivot_value
        value_now = (target_row - low_row[None, :, None] * prev_value) / pivot_value[None, :, None]
        return ((ratio_now, value_now), (ratio_now, value_now))
    anchor = jnp.zeros_like(target[0])
    start_ratio = jnp.zeros_like(main_band[0])
    _, (ratios, values) = lax.scan(forward_step, (start_ratio, anchor), (lower_band, main_band, upper_band, target))

    def backward_step(next_value, row_data):
        ratio_now, value_now = row_data
        result_now = value_now - ratio_now[None, :, None] * next_value
        return (result_now, result_now)
    _, results = lax.scan(backward_step, anchor, (ratios, values), reverse=True)
    return results

def assemble(solved, spike_low, spike_high, previous, self_value):
    lifted = solved + spike_low.T[None, :, :, None] * previous[:, None] + spike_high.T[None, :, :, None] * self_value[:, None]
    return jnp.concatenate([lifted[:, :-1], self_value[:, None]], axis=1)

def solve_columns(slab_at, inverse, coupling, selector, total_levels):
    level_count = inverse.shape[2]
    blocks = total_levels // level_count

    def one_block(block_index):
        start_level = block_index * level_count
        level_slab = slab_at(start_level, level_count)
        inverse_rows = lax.dynamic_slice_in_dim(inverse, start_level, level_count, 1)
        coupling_rows = lax.dynamic_slice_in_dim(coupling, start_level, level_count, 1)
        return eliminate(level_slab, inverse_rows, coupling_rows, selector, block_index, blocks)
    solved, spike_low, spike_high, below_face, upper_gate = lax.map(one_block, jnp.arange(blocks, dtype=jnp.int32))
    send_lines = jnp.stack([below_face, below_face * spike_low[:, :, 0], below_face * spike_high[:, :, 0]], axis=1)
    send_rows = below_face[:, None, :, None] * solved[:, :, 0]
    got_lines = jnp.concatenate([send_lines[1:], jnp.zeros_like(send_lines[:1])], axis=0)
    got_rows = jnp.concatenate([send_rows[1:], jnp.zeros_like(send_rows[:1])], axis=0)
    lower_band, main_band, upper_band, target = jax.vmap(interface_rows)(solved, spike_low, spike_high, upper_gate, got_rows, got_lines)
    interfaces = thomas(lower_band, main_band, upper_band, target)
    previous = jnp.concatenate([jnp.zeros_like(interfaces[:1]), interfaces[:-1]], axis=0)
    columns = jax.vmap(assemble)(solved, spike_low, spike_high, previous, interfaces)
    shape_now = columns.shape
    return jnp.moveaxis(columns, 0, 1).reshape(shape_now[1], blocks * level_count, shape_now[3], shape_now[4])

def reference(fields, diffusivity, offsets, coupling, inverse):
    selector = (offsets[:, None] == jnp.arange(inverse.shape[0], dtype=jnp.int32)[None, :]).astype(jnp.float32)

    def slab_at(start_level, level_count):
        centre = lax.dynamic_slice_in_dim(fields, start_level, level_count, 1)
        heat_slab = lax.dynamic_slice_in_dim(diffusivity, start_level, level_count, 0)
        return tendency(centre, jnp.roll(centre, -1, axis=2), jnp.roll(centre, 1, axis=2), heat_slab)
    return solve_columns(slab_at, inverse, coupling, selector, fields.shape[1])
```

```python
import functools

import jax
import jax.numpy as jnp
from jax import lax
from jax.experimental import pallas as pl
from jax.experimental.pallas import tpu as pltpu
from jax.sharding import PartitionSpec as P

MESH = pl.DeviceIdType.MESH
CHUNKS = 4
PAD = 48
LINES = 32
MSG = 24


def depth_order(n):
    half = n // 2
    steps = sorted(range(half), key=lambda s: -min(s, half - s))
    return [(s, c) for s in steps for c in (0, 1) if (s, c) != (0, 0)]


def solve_kernel(
    n_h, n_d,
    fields, diff, offs, coup, inv,
    sol, back, low, high,
    fbuf, dbuf, offv, cvec, kvec, wv, iv, acc, delta,
    hsend, hrecv, cmsg, crecv, m1, r1, m2,
    load_sem, small_sem, hs_sem, hr_sem, cs_sem, cr_sem, s1_sem, r1_sem, s2_sem, r2_sem,
):
    f32 = jnp.float32
    levels = fields.shape[1]
    per = levels // CHUNKS
    me_h = lax.axis_index("horiz")
    me = lax.axis_index("depth")
    east = lax.rem(me_h + 1, n_h)
    west = lax.rem(me_h + n_h - 1, n_h)

    small = [
        pltpu.make_async_copy(offs, offv, small_sem.at[0]),
        pltpu.make_async_copy(coup, cvec, small_sem.at[1]),
        pltpu.make_async_copy(inv, kvec, small_sem.at[2]),
    ]
    for copy in small:
        copy.start()

    def chunk_copies(c):
        lev = pl.ds(c * per, per)
        out = []
        for h in range(2):
            lane = pl.ds(h * 128, 128)
            for f in range(3):
                out.append(pltpu.make_async_copy(
                    fields.at[f, lev, :, lane],
                    fbuf.at[lev, h * 3 + f, pl.ds(8, LINES), :],
                    load_sem.at[c, h * 3 + f]))
            out.append(pltpu.make_async_copy(
                diff.at[lev, :, lane], dbuf.at[lev, h], load_sem.at[c, 6 + h]))
        return out

    for c in range(CHUNKS):
        for copy in chunk_copies(c):
            copy.start()

    barrier = pltpu.get_barrier_semaphore()
    for to in (east, west):
        pl.semaphore_signal(barrier, inc=1, device_id=(to, me), device_id_type=MESH)
    z, core = me // 2, lax.rem(me, 2)

    def peer_at(step, flip):
        zz = lax.rem(z + step, n_d // 2)
        cc = core if flip == 0 else 1 - core
        return zz * 2 + cc

    order = depth_order(n_d)
    for step, flip in order:
        pl.semaphore_signal(barrier, inc=1, device_id=(me_h, peer_at(step, flip)), device_id_type=MESH)

    f2 = fbuf.reshape(levels * 6 * PAD, 128)
    f2[pl.ds(7, levels * 6, stride=PAD), :] = jnp.zeros((levels * 6, 128), f32)
    f2[pl.ds(40, levels * 6, stride=PAD), :] = jnp.zeros((levels * 6, 128), f32)
    for e in range(2):
        hrecv[e, 0:8, :] = jnp.zeros((8, 128), f32)
        hrecv[e, 200:208, :] = jnp.zeros((8, 128), f32)
    acc[...] = jnp.zeros(acc.shape, f32)

    for copy in small:
        copy.wait()
    sub = lax.broadcasted_iota(jnp.int32, (8, 128), 0)
    lane8 = lax.broadcasted_iota(jnp.int32, (8, 128), 1)
    offset_of = []
    for g in range(4):
        v = jnp.full((8, 128), offv[8 * g], jnp.int32)
        for i in range(1, 8):
            v = jnp.where(sub == i, offv[8 * g + i], v)
        offset_of.append(v)
    masks = [[offset_of[g] == o for o in range(3)] for g in range(4)]

    couple = cvec[...]
    first_row = kvec[:, 0, :]
    last_row = kvec[:, levels - 2, :]
    c_low = jnp.broadcast_to(couple[:, 0:1], (4, levels))
    c_high = jnp.broadcast_to(couple[:, levels - 1:levels], (4, levels))
    gate = jnp.where(me > 0, 1.0, 0.0).astype(f32)
    table_low = first_row * (c_low * gate)
    table_high = last_row * c_high

    def column(table, k):
        return jnp.broadcast_to(table[:, k:k + 1], (4, 128))

    def spread(table4, g):
        rows = [jnp.broadcast_to(table4[o:o + 1, :], (8, 128)) for o in range(4)]
        m = masks[g]
        return jnp.where(m[0], rows[0], jnp.where(m[1], rows[1], jnp.where(m[2], rows[2], rows[3])))

    highs = []
    lows = []
    for k in range(levels):
        lo = column(table_low, k)
        hi = column(table_high, k) if k < levels - 1 else jnp.ones((4, 128), f32)
        if k == levels - 1:
            lo = jnp.zeros((4, 128), f32)
        lows.append(lo)
        highs.append(hi)
        for g in range(4):
            low[k, 8 * g:8 * g + 8, :] = spread(lo, g)
            high[k, 8 * g:8 * g + 8, :] = spread(hi, g)

    c_low4 = jnp.broadcast_to(couple[:, 0:1], (4, 128))
    c_high4 = jnp.broadcast_to(couple[:, levels - 1:levels], (4, 128))
    alpha = c_high4 - c_high4 * highs[levels - 2]
    beta = c_low4 - c_low4 * lows[0]
    cross = c_high4 * lows[levels - 2]
    lane4 = lax.broadcasted_iota(jnp.int32, (4, 128), 1)
    packed = jnp.where(lane4 < 32, alpha, jnp.where(lane4 < 64, beta, cross))
    cmsg[0:4, :] = packed
    cmsg[4:8, :] = packed

    lane = lane8
    is_last = lane == 127
    is_first = lane == 0

    def arrived(c):
        for copy in chunk_copies(c):
            copy.wait()

    def forcing_chunk(c):
        for g in range(4):
            r0 = 8 + 8 * g
            sums = [acc[w, q, 8 * g:8 * g + 8, :] for w in range(2) for q in range(6)]
            for l in range(per):
                k = c * per + l
                hi = high[k, 8 * g:8 * g + 8, :]
                lo = low[k, 8 * g:8 * g + 8, :]
                mid = [fbuf[k, q, r0:r0 + 8, :] for q in range(6)]
                es = [fbuf[k, q, r0 + 1:r0 + 9, :] for q in range(6)]
                ws = [fbuf[k, q, r0 - 1:r0 + 7, :] for q in range(6)]
                up = [pltpu.roll(mid[q], 127, 1) for q in range(6)]
                dn = [pltpu.roll(mid[q], 1, 1) for q in range(6)]
                for h in range(2):
                    d = dbuf[k, h, 8 * g:8 * g + 8, :]
                    keep = 1.0 - 4.0 * d
                    q = [h * 3 + f for f in range(3)]
                    qo = [(1 - h) * 3 + f for f in range(3)]
                    north = [jnp.where(is_last, up[qo[f]], up[q[f]]) for f in range(3)]
                    south = [jnp.where(is_first, dn[qo[f]], dn[q[f]]) for f in range(3)]
                    base = [
                        mid[q[f]] * keep + d * ((es[q[f]] + ws[q[f]]) + (north[f] + south[f]))
                        for f in range(3)
                    ]
                    out = [
                        base[0] - 0.25 * (es[q[2]] - ws[q[2]]),
                        base[1] - 0.25 * (north[2] - south[2]),
                        base[2] - 0.25 * ((es[q[0]] - ws[q[0]]) + (north[1] - south[1])),
                    ]
                    for f in range(3):
                        sol[k, q[f], 8 * g:8 * g + 8, :] = out[f]
                        sums[q[f]] = sums[q[f]] + hi * out[f]
                        sums[6 + q[f]] = sums[6 + q[f]] + lo * out[f]
            for w in range(2):
                for q in range(6):
                    acc[w, q, 8 * g:8 * g + 8, :] = sums[w * 6 + q]

    def chunk_step(c, carry):
        arrived(c)
        forcing_chunk(c)
        return carry

    lax.fori_loop(0, CHUNKS - 1, chunk_step, 0)
    arrived(CHUNKS - 1)

    pl.semaphore_wait(barrier, 2 + len(order))
    hsend[0] = f2[pl.ds(39, levels * 6, stride=PAD), :]
    hsend[1] = f2[pl.ds(8, levels * 6, stride=PAD), :]
    coef_copies = []
    for j, (step, flip) in enumerate(order):
        peer = peer_at(step, flip)
        coef_copies.append(pltpu.make_async_remote_copy(
            src_ref=cmsg, dst_ref=crecv.at[me], send_sem=cs_sem.at[j], recv_sem=cr_sem.at[me],
            device_id=(me_h, peer), device_id_type=MESH))
    halo = []
    for e, to in ((0, east), (1, west)):
        halo.append(pltpu.make_async_remote_copy(
            src_ref=hsend.at[e], dst_ref=hrecv.at[e, pl.ds(8, levels * 6), :],
            send_sem=hs_sem.at[e], recv_sem=hr_sem.at[e],
            device_id=(to, me), device_id_type=MESH))
    for copy in halo:
        copy.start()
    for copy in coef_copies:
        copy.start()
    forcing_chunk(CHUNKS - 1)

    m1r = m1.reshape(n_d * MSG, 128)

    def row_of(f, which, slot, h):
        return f * 8 + which * 4 + slot * 2 + h

    for g in range(4):
        p0, slot = 8 * (g % 2), g // 2
        for w in range(2):
            for h in range(2):
                for f in range(3):
                    m1r[pl.ds(p0 * MSG + row_of(f, w, slot, h), 8, stride=MSG), :] = acc[
                        w, h * 3 + f, 8 * g:8 * g + 8, :]

    def message(j, peer):
        return pltpu.make_async_remote_copy(
            src_ref=m1.at[peer], dst_ref=r1.at[me], send_sem=s1_sem.at[j], recv_sem=r1_sem.at[me],
            device_id=(me_h, peer), device_id_type=MESH)

    def ends(peer):
        return jnp.logical_or(peer == 0, peer == n_d - 1)

    for j, (step, flip) in enumerate(order):
        peer = peer_at(step, flip)

        @pl.when(jnp.logical_not(ends(peer)))
        def _():
            message(j, peer).start()

    shift_high = pltpu.roll(jnp.concatenate([table_high, jnp.zeros((4, 128 - levels), f32)], axis=1), 1, 1)
    pad_high = jnp.concatenate([table_high, jnp.ones((4, 128 - levels), f32)], axis=1)
    ratio = shift_high / jnp.where(pad_high == 0.0, 1.0, pad_high)
    pad_couple = jnp.concatenate([couple, jnp.ones((4, 128 - levels), f32)], axis=1)
    pivot = pltpu.roll(ratio / pad_couple, 127, 1)
    for k in range(levels - 1):
        wk = column(ratio, k)
        ik = column(pivot, k) if k < levels - 2 else column(last_row, levels - 2)
        for g in range(4):
            wv[k, 8 * g:8 * g + 8, :] = spread(wk, g)
            iv[k, 8 * g:8 * g + 8, :] = spread(ik, g)

    def down(k, carry):
        out = []
        for g in range(4):
            w = wv[k, 8 * g:8 * g + 8, :]
            for q in range(6):
                y = sol[k, q, 8 * g:8 * g + 8, :] + w * carry[g * 6 + q]
                sol[k, q, 8 * g:8 * g + 8, :] = y
                out.append(y)
        return tuple(out)

    start = tuple(sol[0, q, 8 * g:8 * g + 8, :] for g in range(4) for q in range(6))
    lax.fori_loop(1, levels - 1, down, start)

    def rise(i, carry):
        k = levels - 2 - i
        out = []
        for g in range(4):
            piv = iv[k, 8 * g:8 * g + 8, :]
            w = wv[k + 1, 8 * g:8 * g + 8, :]
            for q in range(6):
                x = piv * sol[k, q, 8 * g:8 * g + 8, :] + w * carry[g * 6 + q]
                sol[k, q, 8 * g:8 * g + 8, :] = x
                out.append(x)
        return tuple(out)

    wv[levels - 1] = jnp.zeros((LINES, 128), f32)
    zero = jnp.zeros((8, 128), f32)
    lax.fori_loop(0, levels - 1, rise, (zero,) * 24)
    for q in range(6):
        sol[levels - 1, q] = jnp.zeros((LINES, 128), f32)

    for copy in halo:
        copy.wait()
    third = lax.rem(sub, 3)
    m_first = jnp.where(jnp.logical_and(third == 0, sub < 6), 0.25, 0.0).astype(f32)
    m_third = jnp.where(jnp.logical_and(third == 2, sub < 6), 0.25, 0.0).astype(f32)
    edge_line = (0, LINES - 1)
    for e in range(2):
        sign = 1.0 if e == 0 else -1.0
        line = edge_line[e]
        sum_a = jnp.zeros((8, 128), f32)
        sum_b = jnp.zeros((8, 128), f32)
        for k in range(levels):
            r = 8 + 6 * k
            here = hrecv[e, r:r + 8, :]
            above = hrecv[e, r + 2:r + 10, :] if r + 10 <= 208 else here
            below = hrecv[e, r - 2:r + 6, :]
            d0 = jnp.broadcast_to(dbuf[k, 0, line:line + 1, :], (8, 128))
            d1 = jnp.broadcast_to(dbuf[k, 1, line:line + 1, :], (8, 128))
            d = jnp.where(sub < 3, d0, d1)
            change = d * here + sign * (m_first * above + m_third * below)
            delta[e, k] = change
            hi = jnp.broadcast_to(high[k, line:line + 1, :], (8, 128))
            lo = jnp.broadcast_to(low[k, line:line + 1, :], (8, 128))
            sum_a = sum_a + hi * change
            sum_b = sum_b + lo * change
        p, slot = (0, 0) if e == 0 else (n_d - 1, 1)
        for w, total in enumerate((sum_a, sum_b)):
            for h in range(2):
                rows = pl.ds(p * MSG + row_of(0, w, slot, h), 3, stride=8)
                m1r[rows, :] = m1r[rows, :] + total[3 * h:3 * h + 3, :]
    for j, (step, flip) in enumerate(order):
        peer = peer_at(step, flip)

        @pl.when(ends(peer))
        def _():
            message(j, peer).start()

    r1[me] = m1[me]

    sol2 = sol.reshape(levels * 6 * LINES, 128)
    for e in range(2):
        line = edge_line[e]
        prev = delta[e, 0]
        for k in range(1, levels - 1):
            w = jnp.broadcast_to(wv[k, line:line + 1, :], (8, 128))
            prev = delta[e, k] + w * prev
            delta[e, k] = prev
        x = jnp.zeros((8, 128), f32)
        for k in range(levels - 2, -1, -1):
            piv = jnp.broadcast_to(iv[k, line:line + 1, :], (8, 128))
            x = piv * delta[e, k] + (jnp.broadcast_to(wv[k + 1, line:line + 1, :], (8, 128)) * x if k < levels - 2 else 0.0)
            rows = pl.ds(k * 6 * LINES + line, 6, stride=LINES)
            sol2[rows, :] = sol2[rows, :] + x[0:6, :]

    crecv[me] = cmsg[...]
    for j, (step, flip) in enumerate(order):
        coef_copies[j].wait_send()
    for step, flip in order:
        peer = peer_at(step, flip)
        pltpu.make_async_remote_copy(
            src_ref=cmsg, dst_ref=crecv.at[peer], send_sem=cs_sem.at[0], recv_sem=cr_sem.at[peer],
            device_id=(me_h, peer), device_id_type=MESH).wait_recv()
    o0 = offv[me]
    o1 = offv[me + n_d]
    second = lax.rem(sub // 2, 2) == 1
    alphas, betas, crosses = [], [], []
    for r in range(n_d):
        both = jnp.where(
            second,
            jnp.broadcast_to(crecv[r, pl.ds(o1, 1), :], (8, 128)),
            jnp.broadcast_to(crecv[r, pl.ds(o0, 1), :], (8, 128)))
        alphas.append(jnp.broadcast_to(both[:, 0:1], (8, 128)))
        betas.append(jnp.broadcast_to(both[:, 32:33], (8, 128)))
        crosses.append(jnp.broadcast_to(both[:, 64:65], (8, 128)))
    pivots, steps = [], []
    for r in range(n_d):
        main = 1.0 + alphas[r]
        if r + 1 < n_d:
            main = main + betas[r + 1]
        if r > 0:
            q = crosses[r] * pivots[r - 1]
            steps.append(q)
            main = main - crosses[r] * q
        else:
            steps.append(None)
        pivots.append(1.0 / main)

    for j, (step, flip) in enumerate(order):
        message(j, peer_at(step, flip)).wait_send()
    for step, flip in order:
        peer = peer_at(step, flip)
        pltpu.make_async_remote_copy(
            src_ref=m1.at[0], dst_ref=r1.at[peer], send_sem=s1_sem.at[0], recv_sem=r1_sem.at[peer],
            device_id=(me_h, peer), device_id_type=MESH).wait_recv()
    top = sub < 4
    for f in range(3):
        got = [r1[r, 8 * f:8 * f + 8, :] for r in range(n_d)]
        value = []
        for r in range(n_d):
            t = got[r] + pltpu.roll(got[r + 1], 4, 0) if r + 1 < n_d else got[r]
            t = jnp.where(top, t, pltpu.roll(t, 4, 0))
            if r > 0:
                t = t + steps[r] * value[r - 1]
            value.append(t)
        s = [None] * n_d
        s[n_d - 1] = value[n_d - 1] * pivots[n_d - 1]
        for r in range(n_d - 2, -1, -1):
            s[r] = value[r] * pivots[r] + steps[r + 1] * s[r + 1]
        for r in range(n_d):
            before = s[r - 1] if r > 0 else jnp.zeros((8, 128), f32)
            m2[r, 8 * f:8 * f + 8, :] = jnp.where(top, before, s[r])

    def answer(j, peer):
        return pltpu.make_async_remote_copy(
            src_ref=m2.at[peer], dst_ref=back.at[me], send_sem=s2_sem.at[j], recv_sem=r2_sem.at[me],
            device_id=(me_h, peer), device_id_type=MESH)

    for j, (step, flip) in enumerate(order):
        answer(j, peer_at(step, flip)).start()
    back[me] = m2[me]
    for j, (step, flip) in enumerate(order):
        answer(j, peer_at(step, flip)).wait_send()
    for step, flip in order:
        peer = peer_at(step, flip)
        pltpu.make_async_remote_copy(
            src_ref=m2.at[0], dst_ref=back.at[peer], send_sem=s2_sem.at[0], recv_sem=r2_sem.at[peer],
            device_id=(me_h, peer), device_id_type=MESH).wait_recv()


def write_kernel(n_d, sol, back, low, high, out, stage, ends, sem):
    levels = sol.shape[0]
    per = levels // CHUNKS
    backr = back.reshape(n_d * MSG, 128)
    for g in range(4):
        p0, slot = 8 * (g % 2), g // 2
        for w in range(2):
            for h in range(2):
                for f in range(3):
                    row = p0 * MSG + f * 8 + w * 4 + slot * 2 + h
                    ends[w, h * 3 + f, 8 * g:8 * g + 8, :] = backr[pl.ds(row, 8, stride=MSG), :]

    def copies(c):
        lev = pl.ds(c * per, per)
        return [
            pltpu.make_async_copy(
                stage.at[lev, h * 3 + f], out.at[f, lev, :, pl.ds(h * 128, 128)], sem.at[c, h * 3 + f])
            for h in range(2) for f in range(3)
        ]

    def chunk(c, carry):
        for g in range(4):
            rows = slice(8 * g, 8 * g + 8)
            prev = [ends[0, q, rows, :] for q in range(6)]
            here = [ends[1, q, rows, :] for q in range(6)]
            for l in range(per):
                k = c * per + l
                lo = low[k, rows, :]
                hi = high[k, rows, :]
                for q in range(6):
                    stage[k, q, rows, :] = sol[k, q, rows, :] + (lo * prev[q] + hi * here[q])
        for copy in copies(c):
            copy.start()
        return carry

    lax.fori_loop(0, CHUNKS, chunk, 0)
    for c in range(CHUNKS):
        for copy in copies(c):
            copy.wait()


def body(n_h, n_d, fields, diffusivity, offsets, coupling, inverse):
    f32 = jnp.float32
    levels = fields.shape[1]
    any_spec = pl.BlockSpec(memory_space=pltpu.HBM)
    vmem_spec = pl.BlockSpec(memory_space=pltpu.VMEM)
    V = lambda *shape: pltpu.VMEM(shape, f32)
    dma = lambda *shape: pltpu.SemaphoreType.DMA(shape)
    sol, back, low, high = pl.pallas_call(
        functools.partial(solve_kernel, n_h, n_d),
        out_shape=(
            V(levels, 6, LINES, 128),
            V(n_d, MSG, 128),
            V(levels, LINES, 128),
            V(levels, LINES, 128),
        ),
        in_specs=[any_spec] * 5,
        out_specs=(vmem_spec,) * 4,
        scratch_shapes=[
            V(levels, 6, PAD, 128),
            V(levels, 2, LINES, 128),
            pltpu.SMEM((LINES,), jnp.int32),
            V(4, levels),
            V(4, levels, levels),
            V(levels, LINES, 128),
            V(levels, LINES, 128),
            V(2, 6, LINES, 128),
            V(2, levels, 8, 128),
            V(2, levels * 6, 128),
            V(2, levels * 6 + 16, 128),
            V(8, 128),
            V(n_d, 8, 128),
            V(n_d, MSG, 128),
            V(n_d, MSG, 128),
            V(n_d, MSG, 128),
            dma(CHUNKS, 8),
            dma(3),
            dma(2),
            dma(2),
            dma(n_d),
            dma(n_d),
            dma(n_d),
            dma(n_d),
            dma(n_d),
            dma(n_d),
        ],
        compiler_params=pltpu.CompilerParams(
            collective_id=0, has_side_effects=True, vmem_limit_bytes=48 * 1024 * 1024),
        name="columns",
    )(fields, diffusivity, offsets, coupling, inverse)
    return pl.pallas_call(
        functools.partial(write_kernel, n_d),
        out_shape=jax.ShapeDtypeStruct(fields.shape, f32),
        in_specs=[vmem_spec] * 4,
        out_specs=any_spec,
        scratch_shapes=[
            V(levels, 6, LINES, 128),
            V(2, 6, LINES, 128),
            dma(CHUNKS, 6),
        ],
        compiler_params=pltpu.CompilerParams(vmem_limit_bytes=48 * 1024 * 1024),
        name="assemble",
    )(sol, back, low, high)


def solution(mesh):
    return jax.shard_map(
        functools.partial(body, mesh.shape["horiz"], mesh.shape["depth"]),
        mesh=mesh,
        in_specs=(
            P(None, "depth", "horiz", None),
            P("depth", "horiz", None),
            P("horiz"),
            P(None, "depth"),
            P(None, "depth", None),
        ),
        out_specs=P(None, "depth", "horiz", None),
        check_vma=False,
    )
```

```python
import functools

import jax
import jax.numpy as jnp
from jax import lax
from jax.experimental import pallas as pl
from jax.experimental.pallas import tpu as pltpu
from jax.sharding import PartitionSpec as P

MESH = pl.DeviceIdType.MESH
CHUNKS = 4
PAD = 48
LINES = 32
GROUPS = LINES // 8
UNITS = GROUPS * 6
HALF = UNITS // 2


def depth_order(n):
    half = n // 2
    steps = sorted(range(half), key=lambda s: -min(s, half - s))
    return [(s, c) for s in steps for c in (0, 1) if (s, c) != (0, 0)]


def columns_kernel(
    n_h, n_d,
    fields, diff, offs, coup, inv,
    sol, back, low, high,
    fbuf, dbuf, offv, cvec, kvec, offl, wv, iv, delta,
    hsend, hrecv, cmsg, crecv, m1, r1, m2, em, er, comp, ucoef,
    edge_sem, load_sem, small_sem, hs_sem, hr_sem, cs_sem, cr_sem, s1_sem, r1_sem, s2_sem, r2_sem,
    es_sem, er_sem,
):
    f32 = jnp.float32
    levels = fields.shape[1]
    per = levels // CHUNKS
    me_h = lax.axis_index("horiz")
    me = lax.axis_index("depth")
    east = lax.rem(me_h + 1, n_h)
    west = lax.rem(me_h + n_h - 1, n_h)
    z, core = me // 2, lax.rem(me, 2)
    order = depth_order(n_d)
    quads = n_d // 4

    def peer_at(step, flip):
        return lax.rem(z + step, n_d // 2) * 2 + (core if flip == 0 else 1 - core)

    def to_depth(peer):
        return (me_h, peer)

    def remote(src, dst, send, recv, to):
        return pltpu.make_async_remote_copy(
            src_ref=src, dst_ref=dst, send_sem=send, recv_sem=recv, device_id=to, device_id_type=MESH)

    barrier = pltpu.get_barrier_semaphore()
    for to in (east, west):
        pl.semaphore_signal(barrier, inc=1, device_id=(to, me), device_id_type=MESH)
    for step, flip in order:
        pl.semaphore_signal(barrier, inc=1, device_id=to_depth(peer_at(step, flip)), device_id_type=MESH)

    small = [
        pltpu.make_async_copy(offs, offv, small_sem.at[0]),
        pltpu.make_async_copy(coup, cvec, small_sem.at[1]),
        pltpu.make_async_copy(inv, kvec, small_sem.at[2]),
    ]
    outer = []
    for i, first in enumerate((0, LINES - 8)):
        for h in range(2):
            for f in range(3):
                outer.append(pltpu.make_async_copy(
                    fields.at[f, :, pl.ds(first, 8), pl.ds(h * 128, 128)],
                    fbuf.at[:, h * 3 + f, pl.ds(8 + first, 8), :],
                    edge_sem.at[i, h * 3 + f]))

    def chunk_copies(c):
        lev = pl.ds(c * per, per)
        out = []
        for h in range(2):
            lane = pl.ds(h * 128, 128)
            for f in range(3):
                out.append(pltpu.make_async_copy(
                    fields.at[f, lev, pl.ds(8, LINES - 16), lane],
                    fbuf.at[lev, h * 3 + f, pl.ds(16, LINES - 16), :],
                    load_sem.at[c, h * 3 + f]))
            out.append(pltpu.make_async_copy(
                diff.at[lev, :, lane], dbuf.at[lev, h], load_sem.at[c, 6 + h]))
        return out

    for copy in small + outer:
        copy.start()
    for c in range(CHUNKS):
        for copy in chunk_copies(c):
            copy.start()

    f2 = fbuf.reshape(levels * 6 * PAD, 128)
    f2[pl.ds(7, levels * 6, stride=PAD), :] = jnp.zeros((levels * 6, 128), f32)
    f2[pl.ds(40, levels * 6, stride=PAD), :] = jnp.zeros((levels * 6, 128), f32)
    for e in range(2):
        hrecv[e, 0:8, :] = jnp.zeros((8, 128), f32)
        hrecv[e, 200:208, :] = jnp.zeros((8, 128), f32)
    m1[...] = jnp.zeros(m1.shape, f32)

    for copy in small:
        copy.wait()
    sub = lax.broadcasted_iota(jnp.int32, (8, 128), 0)
    lane = lax.broadcasted_iota(jnp.int32, (8, 128), 1)
    masks = []
    for g in range(GROUPS):
        v = jnp.full((8, 128), offv[8 * g], jnp.int32)
        for i in range(1, 8):
            v = jnp.where(sub == i, offv[8 * g + i], v)
        offl[g] = v
        masks.append([v == o for o in range(3)])

    def widen(x):
        return jnp.concatenate([x, jnp.zeros((4, 128 - levels), f32)], axis=1)

    couple = cvec[...]
    first_row = kvec[:, 0, :]
    last_row = kvec[:, levels - 2, :]
    c_low = couple[:, 0:1]
    c_high = couple[:, levels - 1:levels]
    gate = jnp.where(me > 0, 1.0, 0.0).astype(f32)
    table_low = first_row * (jnp.broadcast_to(c_low, (4, levels)) * gate)
    table_high = last_row * jnp.broadcast_to(c_high, (4, levels))
    lane4 = lax.broadcasted_iota(jnp.int32, (4, 128), 1)

    def pick(rows, m):
        return jnp.where(m[0], rows[0], jnp.where(m[1], rows[1], jnp.where(m[2], rows[2], rows[3])))

    def by_line(table):
        rows = [jnp.broadcast_to(table[o:o + 1, :], (8, 128)) for o in range(4)]
        return [pick(rows, masks[g]) for g in range(GROUPS)]

    def fill(ref, table, count):
        lines = by_line(table)
        for k in range(count):
            for g in range(GROUPS):
                ref[k, 8 * g:8 * g + 8, :] = jnp.broadcast_to(lines[g][:, k:k + 1], (8, 128))

    wide_high = widen(table_high)
    fill(low, jnp.where(lane4 == levels - 1, 0.0, widen(table_low)), levels)
    fill(high, jnp.where(lane4 == levels - 1, 1.0, wide_high), levels)

    c_low4 = jnp.broadcast_to(c_low, (4, 128))
    c_high4 = jnp.broadcast_to(c_high, (4, 128))
    alpha = c_high4 - c_high4 * jnp.broadcast_to(table_high[:, levels - 2:levels - 1], (4, 128))
    beta = c_low4 - c_low4 * jnp.broadcast_to(table_low[:, 0:1], (4, 128))
    cross = c_high4 * jnp.broadcast_to(table_low[:, levels - 2:levels - 1], (4, 128))
    packed = jnp.where(lane4 < 32, alpha, jnp.where(lane4 < 64, beta, cross))
    cmsg[0:4, :] = packed
    cmsg[4:8, :] = packed

    for copy in outer:
        copy.wait()
    hsend[0] = f2[pl.ds(39, levels * 6, stride=PAD), :]
    hsend[1] = f2[pl.ds(8, levels * 6, stride=PAD), :]
    pl.semaphore_wait(barrier, 2 + len(order))
    halo = [
        remote(hsend.at[e], hrecv.at[e, pl.ds(8, levels * 6), :], hs_sem.at[e], hr_sem.at[e], (to, me))
        for e, to in ((0, east), (1, west))
    ]
    for copy in halo:
        copy.start()

    def coef_copy(j, peer):
        return remote(cmsg, crecv.at[me], cs_sem.at[j], cr_sem.at[me], to_depth(peer))

    for j, (step, flip) in enumerate(order):
        coef_copy(j, peer_at(step, flip)).start()

    is_last = lane == 127
    is_first = lane == 0

    def forcing(c, g):
        r0 = 8 + 8 * g
        rows = slice(8 * g, 8 * g + 8)
        sums = [m1[g * 6 + q, 8 * w:8 * w + 8, :] for w in range(2) for q in range(6)]
        for l in range(per):
            k = c * per + l
            hi = high[k, rows, :]
            lo = low[k, rows, :]
            mid = [fbuf[k, q, r0:r0 + 8, :] for q in range(6)]
            es = [fbuf[k, q, r0 + 1:r0 + 9, :] for q in range(6)]
            ws = [fbuf[k, q, r0 - 1:r0 + 7, :] for q in range(6)]
            up = [pltpu.roll(mid[q], 127, 1) for q in range(6)]
            dn = [pltpu.roll(mid[q], 1, 1) for q in range(6)]
            for h in range(2):
                d = dbuf[k, h, rows, :]
                keep = 1.0 - 4.0 * d
                q = [h * 3 + f for f in range(3)]
                qo = [(1 - h) * 3 + f for f in range(3)]
                north = [jnp.where(is_last, up[qo[f]], up[q[f]]) for f in range(3)]
                south = [jnp.where(is_first, dn[qo[f]], dn[q[f]]) for f in range(3)]
                base = [
                    mid[q[f]] * keep + d * ((es[q[f]] + ws[q[f]]) + (north[f] + south[f]))
                    for f in range(3)
                ]
                out = [
                    base[0] - 0.25 * (es[q[2]] - ws[q[2]]),
                    base[1] - 0.25 * (north[2] - south[2]),
                    base[2] - 0.25 * ((es[q[0]] - ws[q[0]]) + (north[1] - south[1])),
                ]
                for f in range(3):
                    sol[k, q[f], rows, :] = out[f]
                    sums[q[f]] = sums[q[f]] + hi * out[f]
                    sums[6 + q[f]] = sums[6 + q[f]] + lo * out[f]
        for w in range(2):
            for q in range(6):
                m1[g * 6 + q, 8 * w:8 * w + 8, :] = sums[w * 6 + q]

    def solver_of(slot, quad, m):
        return quad * 4 + m + slot, slot * HALF + quad * 3 + m

    def targets(slot):
        for i, dq in enumerate((2, 1, 3, 0)):
            quad = lax.rem(me // 4 + dq, quads)
            for m in range(3):
                peer, unit = solver_of(slot, quad, m)
                yield slot * HALF + i * 3 + m, peer, unit

    def target_copy(slot, j, peer, unit):
        return remote(m1.at[unit], r1.at[slot, me], s1_sem.at[j], r1_sem.at[slot, me], to_depth(peer))

    for slot in range(2):
        def step_chunk(c, carry):
            if slot == 0:
                for copy in chunk_copies(c):
                    copy.wait()
            for g in range(2 * slot, 2 * slot + 2):
                forcing(c, g)
            return carry

        lax.fori_loop(0, CHUNKS, step_chunk, 0)
        for j, peer, unit in targets(slot):
            @pl.when(peer != me)
            def _():
                target_copy(slot, j, peer, unit).start()

            @pl.when(peer == me)
            def _():
                r1[slot, me] = m1[unit]

    shift_high = pltpu.roll(wide_high, 1, 1)
    inner = jnp.logical_and(lane4 > 0, lane4 < levels - 1)
    ratio = jnp.where(inner, shift_high / jnp.where(inner, wide_high, 1.0), 0.0)
    inner_c = jnp.where(inner, widen(couple), 1.0)
    pivot = pltpu.roll(ratio / inner_c, 127, 1)
    pivot = jnp.where(lane4 == levels - 2, widen(last_row), pivot)
    fill(wv, ratio, levels)
    fill(iv, pivot, levels - 1)

    def down(k, carry):
        out = []
        for g in range(GROUPS):
            rows = slice(8 * g, 8 * g + 8)
            w = wv[k, rows, :]
            for q in range(6):
                y = sol[k, q, rows, :] + w * carry[g * 6 + q]
                sol[k, q, rows, :] = y
                out.append(y)
        return tuple(out)

    def rise(i, carry):
        k = levels - 2 - i
        out = []
        for g in range(GROUPS):
            rows = slice(8 * g, 8 * g + 8)
            piv = iv[k, rows, :]
            w = wv[k + 1, rows, :]
            for q in range(6):
                x = piv * sol[k, q, rows, :] + w * carry[g * 6 + q]
                sol[k, q, rows, :] = x
                out.append(x)
        return tuple(out)

    zero = jnp.zeros((8, 128), f32)
    lax.fori_loop(1, levels - 1, down,
                  tuple(sol[0, q, 8 * g:8 * g + 8, :] for g in range(GROUPS) for q in range(6)))
    lax.fori_loop(0, levels - 1, rise, (zero,) * UNITS)
    for q in range(6):
        sol[levels - 1, q] = jnp.zeros((LINES, 128), f32)

    crecv[me] = cmsg[...]
    for step, flip in order:
        peer = peer_at(step, flip)
        remote(cmsg, crecv.at[peer], cs_sem.at[0], cr_sem.at[peer], to_depth(peer)).wait_recv()
    alphas, betas, crosses = [], [], []
    for r in range(n_d):
        tile = crecv[r]
        alphas.append(jnp.broadcast_to(tile[:, 0:1], (8, 128)))
        betas.append(jnp.broadcast_to(tile[:, 32:33], (8, 128)))
        crosses.append(jnp.broadcast_to(tile[:, 64:65], (8, 128)))
    mains = [1.0 + alphas[r] + (betas[r + 1] if r + 1 < n_d else 0.0) for r in range(n_d)]
    before = None
    for r in range(n_d):
        q = crosses[r] * before if r > 0 else zero
        main = mains[r] - crosses[r] * q if r > 0 else mains[r]
        before = 1.0 / main
        comp[0, r] = q
        comp[1, r] = before
        comp[4, r] = crosses[r]
    after = None
    for r in range(n_d - 1, -1, -1):
        q = crosses[r + 1] * after if r + 1 < n_d else zero
        main = mains[r] - crosses[r + 1] * q if r + 1 < n_d else mains[r]
        after = 1.0 / main
        comp[2, r] = q
        comp[3, r] = main

    for copy in halo:
        copy.wait_recv()
    third = lax.rem(sub, 3)
    m_first = jnp.where(jnp.logical_and(third == 0, sub < 6), 0.25, 0.0).astype(f32)
    m_third = jnp.where(jnp.logical_and(third == 2, sub < 6), 0.25, 0.0).astype(f32)
    edge_line = (0, LINES - 1)
    edge_off = [offv[0], offv[LINES - 1]]
    me_low = jnp.maximum(me - 1, 0)

    def one(ref, line):
        return jnp.broadcast_to(ref[line:line + 1, :], (8, 128))

    def edge_comp(i, r, e):
        return jnp.broadcast_to(comp[i, r, pl.ds(edge_off[e], 1), :], (8, 128))

    edge_sums = []
    for e in range(2):
        sign = 1.0 if e == 0 else -1.0
        line = edge_line[e]
        sum_a = [zero, zero]
        sum_b = [zero, zero]
        for k in range(levels):
            r = 8 + 6 * k
            here = hrecv[e, r:r + 8, :]
            above = hrecv[e, r + 2:r + 10, :]
            below = hrecv[e, r - 2:r + 6, :]
            d = jnp.where(sub < 3, one(dbuf.at[k, 0], line), one(dbuf.at[k, 1], line))
            change = d * here + sign * (m_first * above + m_third * below)
            delta[e, k] = change
            sum_a[k % 2] = sum_a[k % 2] + one(high.at[k], line) * change
            sum_b[k % 2] = sum_b[k % 2] + one(low.at[k], line) * change
        sum_a = sum_a[0] + sum_a[1]
        sum_b = sum_b[0] + sum_b[1]
        edge_sums.append((sum_a, sum_b))
        em[0, 8 * e:8 * e + 8, :] = sum_a + edge_comp(0, me, e) * sum_b
        em[1, 8 * e:8 * e + 8, :] = sum_b + edge_comp(2, me_low, e) * sum_a

    def edge_copy(j, peer):
        side = jnp.where(peer > me, 0, 1)
        return remote(em.at[side], er.at[me], es_sem.at[j], er_sem.at[me], to_depth(peer))

    for j, (step, flip) in enumerate(order):
        edge_copy(j, peer_at(step, flip)).start()

    quad, place = me // 4, lax.rem(me, 4)
    has = [place != 3, place != 0]
    units = [quad * 3 + jnp.minimum(place, 2), HALF + quad * 3 + jnp.maximum(place - 1, 0)]

    for slot in range(2):
        @pl.when(has[slot])
        def _():
            v = offl[units[slot] // 6]
            m = [v == o for o in range(3)]
            for i in range(2):
                for r in range(n_d):
                    ucoef[slot, i, r] = pick([one(comp.at[i, r], o) for o in range(4)], m)

    def answer(slot, j, peer):
        return remote(m2.at[slot, peer], back.at[units[slot]], s2_sem.at[slot, j],
                      r2_sem.at[units[slot]], to_depth(peer))

    for slot in range(2):
        @pl.when(has[slot])
        def _():
            for step, flip in order:
                peer = peer_at(step, flip)
                remote(m1.at[0], r1.at[slot, peer], s1_sem.at[0], r1_sem.at[slot, peer],
                       to_depth(peer)).wait_recv()
            value = None
            values = []
            for r in range(n_d):
                t = r1[slot, r, 0:8, :]
                if r + 1 < n_d:
                    t = t + r1[slot, r + 1, 8:16, :]
                value = t if r == 0 else t + ucoef[slot, 0, r] * value
                values.append(value)
            s = values[n_d - 1] * ucoef[slot, 1, n_d - 1]
            for r in range(n_d - 1, -1, -1):
                m2[slot, r, 8:16, :] = s
                if r + 1 < n_d:
                    m2[slot, r + 1, 0:8, :] = s
                if r > 0:
                    s = values[r - 1] * ucoef[slot, 1, r - 1] + ucoef[slot, 0, r] * s
            m2[slot, 0, 0:8, :] = zero
            for j, (step, flip) in enumerate(order):
                answer(slot, j, peer_at(step, flip)).start()
            back[units[slot]] = m2[slot, me]

    sol2 = sol.reshape(levels * 6 * LINES, 128)
    for e in range(2):
        line = edge_line[e]
        prev = delta[e, 0]
        for k in range(1, levels - 1):
            prev = delta[e, k] + one(wv.at[k], line) * prev
            delta[e, k] = prev
        x = zero
        for k in range(levels - 2, -1, -1):
            x = one(iv.at[k], line) * delta[e, k] + one(wv.at[k + 1], line) * x
            rows = pl.ds(k * 6 * LINES + line, 6, stride=LINES)
            sol2[rows, :] = sol2[rows, :] + x[0:6, :]

    for step, flip in order:
        peer = peer_at(step, flip)
        remote(em.at[0], er.at[peer], es_sem.at[0], er_sem.at[peer], to_depth(peer)).wait_recv()
    edge_values = []
    for e in range(2):
        v = zero
        w = zero
        rows = slice(8 * e, 8 * e + 8)
        for r in range(n_d):
            v = jnp.where(r < me, er[r, rows, :] + edge_comp(0, r, e) * v, v)
        for r in range(n_d - 1, 0, -1):
            w = jnp.where(r > me, er[r, rows, :] + edge_comp(2, r - 1, e) * w, w)
        v = v + edge_sums[e][1]
        w = w + edge_sums[e][0]
        q_me = edge_comp(0, me, e)
        u_me = edge_comp(4, me, e)
        s_here = (w + q_me * v) / (edge_comp(3, me, e) - u_me * q_me)
        s_before = (v + u_me * s_here) * edge_comp(1, me_low, e)
        edge_values.append((jnp.where(me > 0, s_before, 0.0), s_here))

    for slot in range(2):
        for unit in range(slot * HALF, (slot + 1) * HALF):
            i = unit - slot * HALF
            peer, _ = solver_of(slot, i // 3, i % 3)

            @pl.when(me != peer)
            def _():
                remote(m2.at[slot, 0], back.at[unit], s2_sem.at[slot, 0], r2_sem.at[unit],
                       to_depth(peer)).wait_recv()
    back2 = back.reshape((UNITS + 2) * 16, 128)
    for e in range(2):
        unit0 = 0 if e == 0 else UNITS - 6
        for w in range(2):
            rows = pl.ds(unit0 * 16 + 8 * w + 7 * e, 6, stride=16)
            back2[rows, :] = back2[rows, :] + edge_values[e][w][0:6, :]
    for copy in halo:
        copy.wait_send()
    for j, (step, flip) in enumerate(order):
        peer = peer_at(step, flip)
        coef_copy(j, peer).wait_send()
        edge_copy(j, peer).wait_send()
    for slot in range(2):
        for j, peer, unit in targets(slot):
            @pl.when(peer != me)
            def _():
                target_copy(slot, j, peer, unit).wait_send()

        @pl.when(has[slot])
        def _():
            for j, (step, flip) in enumerate(order):
                answer(slot, j, peer_at(step, flip)).wait_send()


def assemble_kernel(sol, back, low, high, out, stage, sem):
    levels = sol.shape[0]
    per = levels // CHUNKS

    def copies(c):
        lev = pl.ds(c * per, per)
        return [
            pltpu.make_async_copy(
                stage.at[lev, h * 3 + f], out.at[f, lev, :, pl.ds(h * 128, 128)], sem.at[c, h * 3 + f])
            for h in range(2) for f in range(3)
        ]

    def chunk(c, carry):
        for g in range(GROUPS):
            rows = slice(8 * g, 8 * g + 8)
            prev = [back[g * 6 + q, 0:8, :] for q in range(6)]
            here = [back[g * 6 + q, 8:16, :] for q in range(6)]
            for l in range(per):
                k = c * per + l
                lo = low[k, rows, :]
                hi = high[k, rows, :]
                for q in range(6):
                    stage[k, q, rows, :] = sol[k, q, rows, :] + (lo * prev[q] + hi * here[q])
        for copy in copies(c):
            copy.start()
        return carry

    lax.fori_loop(0, CHUNKS, chunk, 0)
    for c in range(CHUNKS):
        for copy in copies(c):
            copy.wait()


def body(n_h, n_d, fields, diffusivity, offsets, coupling, inverse):
    f32 = jnp.float32
    levels = fields.shape[1]
    hbm_spec = pl.BlockSpec(memory_space=pltpu.HBM)
    vmem_spec = pl.BlockSpec(memory_space=pltpu.VMEM)
    V = lambda *shape: pltpu.VMEM(shape, f32)
    dma = lambda *shape: pltpu.SemaphoreType.DMA(shape)
    sol, back, low, high = pl.pallas_call(
        functools.partial(columns_kernel, n_h, n_d),
        out_shape=(
            V(levels, 6, LINES, 128),
            V(UNITS + 2, 16, 128),
            V(levels, LINES, 128),
            V(levels, LINES, 128),
        ),
        in_specs=[hbm_spec] * 5,
        out_specs=(vmem_spec,) * 4,
        scratch_shapes=[
            V(levels, 6, PAD, 128),
            V(levels, 2, LINES, 128),
            pltpu.SMEM((LINES,), jnp.int32),
            V(4, levels),
            V(4, levels, levels),
            pltpu.VMEM((GROUPS, 8, 128), jnp.int32),
            V(levels, LINES, 128),
            V(levels, LINES, 128),
            V(2, levels, 8, 128),
            V(2, levels * 6, 128),
            V(2, levels * 6 + 16, 128),
            V(8, 128),
            V(n_d, 8, 128),
            V(UNITS, 16, 128),
            V(2, n_d, 16, 128),
            V(2, n_d, 16, 128),
            V(2, 16, 128),
            V(n_d, 16, 128),
            V(5, n_d, 8, 128),
            V(2, 2, n_d, 8, 128),
            dma(2, 6),
            dma(CHUNKS, 8),
            dma(3),
            dma(2),
            dma(2),
            dma(n_d),
            dma(n_d),
            dma(UNITS),
            dma(2, n_d),
            dma(2, n_d),
            dma(UNITS),
            dma(n_d),
            dma(n_d),
        ],
        compiler_params=pltpu.CompilerParams(
            collective_id=0, has_side_effects=True, vmem_limit_bytes=48 * 1024 * 1024),
        name="columns",
    )(*(pltpu.with_memory_space_constraint(x, pltpu.HBM)
        for x in (fields, diffusivity, offsets, coupling, inverse)))
    return pl.pallas_call(
        assemble_kernel,
        out_shape=jax.ShapeDtypeStruct(fields.shape, f32),
        in_specs=[vmem_spec] * 4,
        out_specs=hbm_spec,
        scratch_shapes=[
            V(levels, 6, LINES, 128),
            dma(CHUNKS, 6),
        ],
        compiler_params=pltpu.CompilerParams(vmem_limit_bytes=48 * 1024 * 1024),
        name="assemble",
    )(sol, back, low, high)


def solution(mesh):
    return jax.shard_map(
        functools.partial(body, mesh.shape["horiz"], mesh.shape["depth"]),
        mesh=mesh,
        in_specs=(
            P(None, "depth", "horiz", None),
            P("depth", "horiz", None),
            P("horiz"),
            P(None, "depth"),
            P(None, "depth", None),
        ),
        out_specs=P(None, "depth", "horiz", None),
        check_vma=False,
    )
```

```python
import functools

import jax
import jax.numpy as jnp
from jax import lax
from jax.experimental import pallas as pl
from jax.experimental.pallas import tpu as pltpu
from jax.sharding import PartitionSpec as P

MESH = pl.DeviceIdType.MESH
CHUNKS = 4
PAD = 48
LINES = 32
GROUPS = LINES // 8
UNITS = GROUPS * 6
HALF = UNITS // 2


def far_first(chips):
    return sorted(range(1, chips), key=lambda s: -min(s, chips - s))


def columns_kernel(
    n_h, n_d,
    fields, diff, offs, coup, inv,
    sol, back, low, high,
    fbuf, dbuf, offv, cvec, kvec, offl, wv, iv, delta,
    hsend, hrecv, cmsg, cpart, chip, crecv, m1, other, chip_rows, middle, r1, m2, got, pass_on,
    esum, epart, em, er, comp, ucoef, lcoef,
    edge_sem, load_sem, small_sem, hs_sem, hr_sem, pair_send, pair_recv, cs_sem, cr_sem,
    s1_sem, r1_sem, s2_sem, r2_sem, es_sem, er_sem,
):
    f32 = jnp.float32
    levels = fields.shape[1]
    per = levels // CHUNKS
    me_h = lax.axis_index("horiz")
    me = lax.axis_index("depth")
    east = lax.rem(me_h + 1, n_h)
    west = lax.rem(me_h + n_h - 1, n_h)
    z, core = me // 2, lax.rem(me, 2)
    chips = n_d // 2
    steps = far_first(chips)
    on_low = core == 0

    def chip_at(step):
        return lax.rem(z + step, chips)

    def same_core(zz):
        return (me_h, zz * 2 + core)

    partner = (me_h, z * 2 + 1 - core)

    def remote(src, dst, send, recv, to):
        return pltpu.make_async_remote_copy(
            src_ref=src, dst_ref=dst, send_sem=send, recv_sem=recv, device_id=to, device_id_type=MESH)

    barrier = pltpu.get_barrier_semaphore()
    meets = [(east, me), (west, me), partner] + [same_core(chip_at(step)) for step in steps]
    for to in meets:
        pl.semaphore_signal(barrier, inc=1, device_id=to, device_id_type=MESH)

    small = [
        pltpu.make_async_copy(offs, offv, small_sem.at[0]),
        pltpu.make_async_copy(coup, cvec, small_sem.at[1]),
        pltpu.make_async_copy(inv, kvec, small_sem.at[2]),
    ]
    outer = []
    for i, first in enumerate((0, LINES - 8)):
        for h in range(2):
            for f in range(3):
                outer.append(pltpu.make_async_copy(
                    fields.at[f, :, pl.ds(first, 8), pl.ds(h * 128, 128)],
                    fbuf.at[:, h * 3 + f, pl.ds(8 + first, 8), :],
                    edge_sem.at[i, h * 3 + f]))

    def chunk_copies(c):
        lev = pl.ds(c * per, per)
        out = []
        for h in range(2):
            lane = pl.ds(h * 128, 128)
            for f in range(3):
                out.append(pltpu.make_async_copy(
                    fields.at[f, lev, pl.ds(8, LINES - 16), lane],
                    fbuf.at[lev, h * 3 + f, pl.ds(16, LINES - 16), :],
                    load_sem.at[c, h * 3 + f]))
            out.append(pltpu.make_async_copy(
                diff.at[lev, :, lane], dbuf.at[lev, h], load_sem.at[c, 6 + h]))
        return out

    for copy in small + outer:
        copy.start()
    for c in range(CHUNKS):
        for copy in chunk_copies(c):
            copy.start()

    f2 = fbuf.reshape(levels * 6 * PAD, 128)
    f2[pl.ds(7, levels * 6, stride=PAD), :] = jnp.zeros((levels * 6, 128), f32)
    f2[pl.ds(40, levels * 6, stride=PAD), :] = jnp.zeros((levels * 6, 128), f32)
    for e in range(2):
        hrecv[e, 0:8, :] = jnp.zeros((8, 128), f32)
        hrecv[e, 200:208, :] = jnp.zeros((8, 128), f32)
    m1[...] = jnp.zeros(m1.shape, f32)

    for copy in small:
        copy.wait()
    sub = lax.broadcasted_iota(jnp.int32, (8, 128), 0)
    lane = lax.broadcasted_iota(jnp.int32, (8, 128), 1)
    masks = []
    for g in range(GROUPS):
        v = jnp.full((8, 128), offv[8 * g], jnp.int32)
        for i in range(1, 8):
            v = jnp.where(sub == i, offv[8 * g + i], v)
        offl[g] = v
        masks.append([v == o for o in range(3)])

    def widen(x):
        return jnp.concatenate([x, jnp.zeros((4, 128 - levels), f32)], axis=1)

    couple = cvec[...]
    first_row = kvec[:, 0, :]
    last_row = kvec[:, levels - 2, :]
    c_low = couple[:, 0:1]
    c_high = couple[:, levels - 1:levels]
    gate = jnp.where(me > 0, 1.0, 0.0).astype(f32)
    table_low = first_row * (jnp.broadcast_to(c_low, (4, levels)) * gate)
    table_high = last_row * jnp.broadcast_to(c_high, (4, levels))
    lane4 = lax.broadcasted_iota(jnp.int32, (4, 128), 1)

    def pick(rows, m):
        return jnp.where(m[0], rows[0], jnp.where(m[1], rows[1], jnp.where(m[2], rows[2], rows[3])))

    def by_line(table):
        rows = [jnp.broadcast_to(table[o:o + 1, :], (8, 128)) for o in range(4)]
        return [pick(rows, masks[g]) for g in range(GROUPS)]

    def fill(ref, table, count):
        lines = by_line(table)
        for k in range(count):
            for g in range(GROUPS):
                ref[k, 8 * g:8 * g + 8, :] = jnp.broadcast_to(lines[g][:, k:k + 1], (8, 128))

    wide_high = widen(table_high)
    fill(low, jnp.where(lane4 == levels - 1, 0.0, widen(table_low)), levels)
    fill(high, jnp.where(lane4 == levels - 1, 1.0, wide_high), levels)

    c_low4 = jnp.broadcast_to(c_low, (4, 128))
    c_high4 = jnp.broadcast_to(c_high, (4, 128))
    alpha = c_high4 - c_high4 * jnp.broadcast_to(table_high[:, levels - 2:levels - 1], (4, 128))
    beta = c_low4 - c_low4 * jnp.broadcast_to(table_low[:, 0:1], (4, 128))
    cross = c_high4 * jnp.broadcast_to(table_low[:, levels - 2:levels - 1], (4, 128))
    packed = jnp.where(lane4 < 32, alpha, jnp.where(lane4 < 64, beta, cross))
    cmsg[0:4, :] = packed
    cmsg[4:8, :] = packed

    for copy in outer:
        copy.wait()
    hsend[0] = f2[pl.ds(39, levels * 6, stride=PAD), :]
    hsend[1] = f2[pl.ds(8, levels * 6, stride=PAD), :]
    is_last = lane == 127
    is_first = lane == 0

    def forcing(c, g):
        r0 = 8 + 8 * g
        rows = slice(8 * g, 8 * g + 8)
        sums = [m1[g * 6 + q, 8 * w:8 * w + 8, :] for w in range(2) for q in range(6)]
        for l in range(per):
            k = c * per + l
            hi = high[k, rows, :]
            lo = low[k, rows, :]
            mid = [fbuf[k, q, r0:r0 + 8, :] for q in range(6)]
            es = [fbuf[k, q, r0 + 1:r0 + 9, :] for q in range(6)]
            ws = [fbuf[k, q, r0 - 1:r0 + 7, :] for q in range(6)]
            up = [pltpu.roll(mid[q], 127, 1) for q in range(6)]
            dn = [pltpu.roll(mid[q], 1, 1) for q in range(6)]
            for h in range(2):
                d = dbuf[k, h, rows, :]
                keep = 1.0 - 4.0 * d
                q = [h * 3 + f for f in range(3)]
                qo = [(1 - h) * 3 + f for f in range(3)]
                north = [jnp.where(is_last, up[qo[f]], up[q[f]]) for f in range(3)]
                south = [jnp.where(is_first, dn[qo[f]], dn[q[f]]) for f in range(3)]
                base = [
                    mid[q[f]] * keep + d * ((es[q[f]] + ws[q[f]]) + (north[f] + south[f]))
                    for f in range(3)
                ]
                out = [
                    base[0] - 0.25 * (es[q[2]] - ws[q[2]]),
                    base[1] - 0.25 * (north[2] - south[2]),
                    base[2] - 0.25 * ((es[q[0]] - ws[q[0]]) + (north[1] - south[1])),
                ]
                for f in range(3):
                    sol[k, q[f], rows, :] = out[f]
                    sums[q[f]] = sums[q[f]] + hi * out[f]
                    sums[6 + q[f]] = sums[6 + q[f]] + lo * out[f]
        for w in range(2):
            for q in range(6):
                m1[g * 6 + q, 8 * w:8 * w + 8, :] = sums[w * 6 + q]

    def slot_forcing(slot, first):
        def step_chunk(c, carry):
            if first:
                for copy in chunk_copies(c):
                    copy.wait()
            for g in range(2 * slot, 2 * slot + 2):
                forcing(c, g)
            return carry

        lax.fori_loop(0, CHUNKS, step_chunk, 0)

    for slot in range(2):
        @pl.when(core == 1 - slot)
        def _():
            slot_forcing(slot, True)

    halo = [
        remote(hsend.at[e], hrecv.at[e, pl.ds(8, levels * 6), :], hs_sem.at[e], hr_sem.at[e], (to, me))
        for e, to in ((0, east), (1, west))
    ]
    pair_coef = remote(cmsg, cpart, pair_send.at[0], pair_recv.at[0], partner)
    pair_rows = remote(m1.at[pl.ds((1 - core) * HALF, HALF)], other, pair_send.at[1], pair_recv.at[1], partner)
    pl.semaphore_wait(barrier, len(meets))
    for copy in (pair_coef, pair_rows, *halo):
        copy.start()
    for slot in range(2):
        @pl.when(core == slot)
        def _():
            slot_forcing(slot, False)

    def splat(tile, at):
        return jnp.broadcast_to(tile[:, at:at + 1], (8, 128))

    pair_coef.wait_recv()
    mine, theirs = cmsg[...], cpart[...]
    tile0 = jnp.where(on_low, mine, theirs)
    tile1 = jnp.where(on_low, theirs, mine)
    alpha0, beta0, cross0 = (splat(tile0, at) for at in (0, 32, 64))
    alpha1, beta1, cross1 = (splat(tile1, at) for at in (0, 32, 64))
    mid_pivot = 1.0 / (1.0 + alpha0 + beta1)
    to_low = cross0 * mid_pivot
    to_high = cross1 * mid_pivot
    chip[...] = jnp.where(
        lane < 32, alpha1 - cross1 * to_high,
        jnp.where(lane < 64, beta0 - cross0 * to_low, cross0 * to_high))
    lcoef[0] = to_low
    lcoef[1] = to_high
    lcoef[2] = mid_pivot

    def coef_copy(j, zz):
        return remote(chip, crecv.at[z], cs_sem.at[j], cr_sem.at[z], same_core(zz))

    for j, step in enumerate(steps):
        coef_copy(j, chip_at(step)).start()

    def one(ref, line):
        return jnp.broadcast_to(ref[line:line + 1, :], (8, 128))

    def group_masks(g):
        v = offl[g]
        return [v == o for o in range(3)]

    own_masks = [group_masks(2 * core + gg) for gg in range(2)]
    own = [
        [pick([one(lcoef.at[i], o) for o in range(4)], own_masks[gg]) for i in range(3)]
        for gg in range(2)
    ]
    pair_rows.wait_recv()
    for i in range(HALF):
        low_k, high_k, _ = own[i // 6]
        a_mine, b_mine = m1[core * HALF + i, 0:8, :], m1[core * HALF + i, 8:16, :]
        a_other, b_other = other[i, 0:8, :], other[i, 8:16, :]
        t = jnp.where(on_low, a_mine, a_other) + jnp.where(on_low, b_other, b_mine)
        middle[i] = t
        chip_rows[i, 0:8, :] = jnp.where(on_low, a_other, a_mine) + high_k * t
        chip_rows[i, 8:16, :] = jnp.where(on_low, b_mine, b_other) + low_k * t

    def solver_of(i, w, m):
        b = (m + core) // 2
        return w * 2 + b, m - b * (2 - core)

    def targets():
        for n, dw in enumerate((2, 1, 3, 0)):
            w = lax.rem(z // 2 + dw, chips // 2)
            for m in range(3):
                zz, j = solver_of(None, w, m)
                yield n * 3 + m, zz, j, w * 3 + m

    def target_copy(n, zz, j, unit):
        return remote(chip_rows.at[unit], r1.at[j, z], s1_sem.at[n], r1_sem.at[j, z], same_core(zz))

    for n, zz, j, unit in targets():
        @pl.when(zz != z)
        def _():
            target_copy(n, zz, j, unit).start()

        @pl.when(zz == z)
        def _():
            r1[j, z] = chip_rows[unit]

    shift_high = pltpu.roll(wide_high, 1, 1)
    inner = jnp.logical_and(lane4 > 0, lane4 < levels - 1)
    ratio = jnp.where(inner, shift_high / jnp.where(inner, wide_high, 1.0), 0.0)
    inner_c = jnp.where(inner, widen(couple), 1.0)
    pivot = pltpu.roll(ratio / inner_c, 127, 1)
    pivot = jnp.where(lane4 == levels - 2, widen(last_row), pivot)
    fill(wv, ratio, levels)
    fill(iv, pivot, levels - 1)

    def down(k, carry):
        out = []
        for g in range(GROUPS):
            rows = slice(8 * g, 8 * g + 8)
            w = wv[k, rows, :]
            for q in range(6):
                y = sol[k, q, rows, :] + w * carry[g * 6 + q]
                sol[k, q, rows, :] = y
                out.append(y)
        return tuple(out)

    def rise(i, carry):
        k = levels - 2 - i
        out = []
        for g in range(GROUPS):
            rows = slice(8 * g, 8 * g + 8)
            piv = iv[k, rows, :]
            w = wv[k + 1, rows, :]
            for q in range(6):
                x = piv * sol[k, q, rows, :] + w * carry[g * 6 + q]
                sol[k, q, rows, :] = x
                out.append(x)
        return tuple(out)

    zero = jnp.zeros((8, 128), f32)
    lax.fori_loop(1, levels - 1, down,
                  tuple(sol[0, q, 8 * g:8 * g + 8, :] for g in range(GROUPS) for q in range(6)))
    lax.fori_loop(0, levels - 1, rise, (zero,) * UNITS)
    for q in range(6):
        sol[levels - 1, q] = jnp.zeros((LINES, 128), f32)

    crecv[z] = chip[...]
    for step in steps:
        zz = chip_at(step)
        remote(chip, crecv.at[zz], cs_sem.at[0], cr_sem.at[zz], same_core(zz)).wait_recv()
    alphas, betas, crosses = [], [], []
    for r in range(chips):
        tile = crecv[r]
        alphas.append(splat(tile, 0))
        betas.append(splat(tile, 32))
        crosses.append(splat(tile, 64))
    mains = [1.0 + alphas[r] + (betas[r + 1] if r + 1 < chips else 0.0) for r in range(chips)]
    before = None
    for r in range(chips):
        q = crosses[r] * before if r > 0 else zero
        main = mains[r] - crosses[r] * q if r > 0 else mains[r]
        before = 1.0 / main
        comp[0, r] = q
        comp[1, r] = before
        comp[4, r] = crosses[r]
    after = None
    for r in range(chips - 1, -1, -1):
        q = crosses[r + 1] * after if r + 1 < chips else zero
        main = mains[r] - crosses[r + 1] * q if r + 1 < chips else mains[r]
        after = 1.0 / main
        comp[2, r] = q
        comp[3, r] = main

    parity = lax.rem(z, 2)
    first_unit = (z // 2) * 3 + parity * (2 - core)
    has = [None, parity == core]
    for j in range(2):
        m = group_masks(2 * core + jnp.minimum(first_unit + j, HALF - 1) // 6)
        for i in range(2):
            for r in range(chips):
                ucoef[j, i, r] = pick([one(comp.at[i, r], o) for o in range(4)], m)

    for copy in halo:
        copy.wait_recv()
    third = lax.rem(sub, 3)
    m_first = jnp.where(jnp.logical_and(third == 0, sub < 6), 0.25, 0.0).astype(f32)
    m_third = jnp.where(jnp.logical_and(third == 2, sub < 6), 0.25, 0.0).astype(f32)
    edge_line = (0, LINES - 1)
    for e in range(2):
        sign = 1.0 if e == 0 else -1.0
        line = edge_line[e]
        sum_a = [zero, zero]
        sum_b = [zero, zero]
        for k in range(levels):
            r = 8 + 6 * k
            here = hrecv[e, r:r + 8, :]
            above = hrecv[e, r + 2:r + 10, :]
            below = hrecv[e, r - 2:r + 6, :]
            d = jnp.where(sub < 3, one(dbuf.at[k, 0], line), one(dbuf.at[k, 1], line))
            change = d * here + sign * (m_first * above + m_third * below)
            delta[e, k] = change
            sum_a[k % 2] = sum_a[k % 2] + one(high.at[k], line) * change
            sum_b[k % 2] = sum_b[k % 2] + one(low.at[k], line) * change
        esum[e, 0:8, :] = sum_a[0] + sum_a[1]
        esum[e, 8:16, :] = sum_b[0] + sum_b[1]
    pair_edge = remote(esum.at[1 - core], epart, pair_send.at[2], pair_recv.at[2], partner)
    pair_edge.start()

    def answer(j, n, zz):
        return remote(m2.at[j, zz], got.at[first_unit + j], s2_sem.at[j, n], r2_sem.at[first_unit + j],
                      same_core(zz))

    def solve_unit(j):
        for step in steps:
            zz = chip_at(step)
            remote(chip_rows.at[0], r1.at[j, zz], s1_sem.at[0], r1_sem.at[j, zz], same_core(zz)).wait_recv()
        values = []
        for r in range(chips):
            t = r1[j, r, 0:8, :]
            if r + 1 < chips:
                t = t + r1[j, r + 1, 8:16, :]
            values.append(t if r == 0 else t + ucoef[j, 0, r] * values[r - 1])
        s = values[chips - 1] * ucoef[j, 1, chips - 1]
        for r in range(chips - 1, -1, -1):
            m2[j, r, 8:16, :] = s
            if r + 1 < chips:
                m2[j, r + 1, 0:8, :] = s
            if r > 0:
                s = values[r - 1] * ucoef[j, 1, r - 1] + ucoef[j, 0, r] * s
        m2[j, 0, 0:8, :] = zero
        for n, step in enumerate(steps):
            answer(j, n, chip_at(step)).start()
        got[first_unit + j] = m2[j, z]

    solve_unit(0)

    @pl.when(has[1])
    def _():
        solve_unit(1)

    edge_off = offv[core * (LINES - 1)]
    z_low = jnp.maximum(z - 1, 0)

    def edge_comp(i, r):
        return jnp.broadcast_to(comp[i, r, pl.ds(edge_off, 1), :], (8, 128))

    def edge_local(i):
        return jnp.broadcast_to(lcoef[i, pl.ds(edge_off, 1), :], (8, 128))

    pair_edge.wait_recv()
    a_mine, b_mine = esum[core, 0:8, :], esum[core, 8:16, :]
    a_other, b_other = epart[0:8, :], epart[8:16, :]
    edge_t = jnp.where(on_low, a_mine, a_other) + jnp.where(on_low, b_other, b_mine)
    edge_a = jnp.where(on_low, a_other, a_mine) + edge_local(1) * edge_t
    edge_b = jnp.where(on_low, b_mine, b_other) + edge_local(0) * edge_t
    em[0] = edge_a + edge_comp(0, z) * edge_b
    em[1] = edge_b + edge_comp(2, z_low) * edge_a

    def edge_copy(n, zz):
        return remote(em.at[jnp.where(zz > z, 0, 1)], er.at[z], es_sem.at[n], er_sem.at[z], same_core(zz))

    for n, step in enumerate(steps):
        edge_copy(n, chip_at(step)).start()

    sol2 = sol.reshape(levels * 6 * LINES, 128)
    for e in range(2):
        line = edge_line[e]
        prev = delta[e, 0]
        for k in range(1, levels - 1):
            prev = delta[e, k] + one(wv.at[k], line) * prev
            delta[e, k] = prev
        x = zero
        for k in range(levels - 2, -1, -1):
            x = one(iv.at[k], line) * delta[e, k] + one(wv.at[k + 1], line) * x
            rows = pl.ds(k * 6 * LINES + line, 6, stride=LINES)
            sol2[rows, :] = sol2[rows, :] + x[0:6, :]

    for step in steps:
        zz = chip_at(step)
        remote(em.at[0], er.at[zz], es_sem.at[0], er_sem.at[zz], same_core(zz)).wait_recv()
    v = zero
    w = zero
    for r in range(chips):
        v = jnp.where(r < z, er[r] + edge_comp(0, r) * v, v)
    for r in range(chips - 1, 0, -1):
        w = jnp.where(r > z, er[r] + edge_comp(2, r - 1) * w, w)
    v = v + edge_b
    w = w + edge_a
    q_here = edge_comp(0, z)
    u_here = edge_comp(4, z)
    edge_high = (w + q_here * v) / (edge_comp(3, z) - u_here * q_here)
    edge_low = jnp.where(z > 0, (v + u_here * edge_high) * edge_comp(1, z_low), 0.0)

    for i in range(HALF):
        @pl.when(w_solver(i, core) != z)
        def _():
            remote(m2.at[0, 0], got.at[i], s2_sem.at[0, 0], r2_sem.at[i], same_core(w_solver(i, core))).wait_recv()
    got2 = got.reshape((HALF + 2) * 16, 128)
    middle2 = middle.reshape((HALF + 2) * 8, 128)
    for e in range(2):
        @pl.when(core == e)
        def _():
            for ref, size, at, add in (
                    (got2, 16, 0, edge_low), (got2, 16, 8, edge_high), (middle2, 8, 0, edge_t)):
                rows = pl.ds(6 * e * size + at + 7 * e, 6, stride=size)
                ref[rows, :] = ref[rows, :] + add[0:6, :]
    for i in range(HALF):
        low_k, high_k, pivot_k = own[i // 6]
        s_low, s_high = got[i, 0:8, :], got[i, 8:16, :]
        s_mid = middle[i] * pivot_k + low_k * s_low + high_k * s_high
        back[core * HALF + i, 0:8, :] = jnp.where(on_low, s_low, s_mid)
        back[core * HALF + i, 8:16, :] = jnp.where(on_low, s_mid, s_high)
        pass_on[i, 0:8, :] = jnp.where(on_low, s_mid, s_low)
        pass_on[i, 8:16, :] = jnp.where(on_low, s_high, s_mid)
    pair_ends = remote(pass_on, back.at[pl.ds(core * HALF, HALF)], pair_send.at[3], pair_recv.at[3], partner)
    pair_ends.start()

    for copy in (*halo, pair_coef, pair_rows, pair_edge):
        copy.wait_send()
    for n, step in enumerate(steps):
        coef_copy(n, chip_at(step)).wait_send()
        edge_copy(n, chip_at(step)).wait_send()
        answer(0, n, chip_at(step)).wait_send()
    for n, zz, j, unit in targets():
        @pl.when(zz != z)
        def _():
            target_copy(n, zz, j, unit).wait_send()

    @pl.when(has[1])
    def _():
        for n, step in enumerate(steps):
            answer(1, n, chip_at(step)).wait_send()
    pair_ends.wait()


def w_solver(i, core):
    return (i // 3) * 2 + (i % 3 + core) // 2


def assemble_kernel(sol, back, low, high, out, stage, sem):
    levels = sol.shape[0]
    per = levels // CHUNKS

    def copies(c):
        lev = pl.ds(c * per, per)
        return [
            pltpu.make_async_copy(
                stage.at[lev, h * 3 + f], out.at[f, lev, :, pl.ds(h * 128, 128)], sem.at[c, h * 3 + f])
            for h in range(2) for f in range(3)
        ]

    def chunk(c, carry):
        for g in range(GROUPS):
            rows = slice(8 * g, 8 * g + 8)
            prev = [back[g * 6 + q, 0:8, :] for q in range(6)]
            here = [back[g * 6 + q, 8:16, :] for q in range(6)]
            for l in range(per):
                k = c * per + l
                lo = low[k, rows, :]
                hi = high[k, rows, :]
                for q in range(6):
                    stage[k, q, rows, :] = sol[k, q, rows, :] + (lo * prev[q] + hi * here[q])
        for copy in copies(c):
            copy.start()
        return carry

    lax.fori_loop(0, CHUNKS, chunk, 0)
    for c in range(CHUNKS):
        for copy in copies(c):
            copy.wait()


def body(n_h, n_d, fields, diffusivity, offsets, coupling, inverse):
    f32 = jnp.float32
    levels = fields.shape[1]
    chips = n_d // 2
    hbm_spec = pl.BlockSpec(memory_space=pltpu.HBM)
    vmem_spec = pl.BlockSpec(memory_space=pltpu.VMEM)
    V = lambda *shape: pltpu.VMEM(shape, f32)
    dma = lambda *shape: pltpu.SemaphoreType.DMA(shape)
    sol, back, low, high = pl.pallas_call(
        functools.partial(columns_kernel, n_h, n_d),
        out_shape=(
            V(levels, 6, LINES, 128),
            V(UNITS, 16, 128),
            V(levels, LINES, 128),
            V(levels, LINES, 128),
        ),
        in_specs=[hbm_spec] * 5,
        out_specs=(vmem_spec,) * 4,
        scratch_shapes=[
            V(levels, 6, PAD, 128),
            V(levels, 2, LINES, 128),
            pltpu.SMEM((LINES,), jnp.int32),
            V(4, levels),
            V(4, levels, levels),
            pltpu.VMEM((GROUPS, 8, 128), jnp.int32),
            V(levels, LINES, 128),
            V(levels, LINES, 128),
            V(2, levels, 8, 128),
            V(2, levels * 6, 128),
            V(2, levels * 6 + 16, 128),
            V(8, 128),
            V(8, 128),
            V(8, 128),
            V(chips, 8, 128),
            V(UNITS, 16, 128),
            V(HALF, 16, 128),
            V(HALF, 16, 128),
            V(HALF + 2, 8, 128),
            V(2, chips, 16, 128),
            V(2, chips, 16, 128),
            V(HALF + 2, 16, 128),
            V(HALF, 16, 128),
            V(2, 16, 128),
            V(16, 128),
            V(2, 8, 128),
            V(chips, 8, 128),
            V(5, chips, 8, 128),
            V(2, 2, chips, 8, 128),
            V(3, 8, 128),
            dma(2, 6),
            dma(CHUNKS, 8),
            dma(3),
            dma(2),
            dma(2),
            dma(4),
            dma(4),
            dma(chips),
            dma(chips),
            dma(HALF),
            dma(2, chips),
            dma(2, chips),
            dma(HALF),
            dma(chips),
            dma(chips),
        ],
        compiler_params=pltpu.CompilerParams(
            collective_id=0, has_side_effects=True, vmem_limit_bytes=48 * 1024 * 1024),
        name="columns",
    )(*(pltpu.with_memory_space_constraint(x, pltpu.HBM)
        for x in (fields, diffusivity, offsets, coupling, inverse)))
    return pl.pallas_call(
        assemble_kernel,
        out_shape=jax.ShapeDtypeStruct(fields.shape, f32),
        in_specs=[vmem_spec] * 4,
        out_specs=hbm_spec,
        scratch_shapes=[
            V(levels, 6, LINES, 128),
            dma(CHUNKS, 6),
        ],
        compiler_params=pltpu.CompilerParams(vmem_limit_bytes=48 * 1024 * 1024),
        name="assemble",
    )(sol, back, low, high)


def solution(mesh):
    return jax.shard_map(
        functools.partial(body, mesh.shape["horiz"], mesh.shape["depth"]),
        mesh=mesh,
        in_specs=(
            P(None, "depth", "horiz", None),
            P("depth", "horiz", None),
            P("horiz"),
            P(None, "depth"),
            P(None, "depth", None),
        ),
        out_specs=P(None, "depth", "horiz", None),
        check_vma=False,
    )
```

```python
import functools

import jax
import jax.numpy as jnp
from jax import lax
from jax.experimental import pallas as pl
from jax.experimental.pallas import tpu as pltpu
from jax.sharding import PartitionSpec as P

MESH = pl.DeviceIdType.MESH
CHUNKS = 4
PAD = 48
LINES = 32
GROUPS = LINES // 8
UNITS = GROUPS * 6
HALF = UNITS // 2


def far_first(chips):
    return sorted(range(1, chips), key=lambda s: -min(s, chips - s))


def columns_kernel(
    n_h, n_d,
    fields, diff, offs, coup, inv,
    sol, back, low, high,
    fbuf, dbuf, offv, cvec, kvec, offl, wv, iv, delta,
    hsend, hrecv, cmsg, cpart, chip, crecv, m1, other, chip_rows, middle, r1, m2, got, pass_on,
    esum, epart, em, er, comp, ucoef, lcoef,
    edge_sem, load_sem, small_sem, hs_sem, hr_sem, pair_send, pair_recv, cs_sem, cr_sem,
    s1_sem, r1_sem, s2_sem, r2_sem, es_sem, er_sem, gate,
):
    f32 = jnp.float32
    levels = fields.shape[1]
    per = levels // CHUNKS
    me_h = lax.axis_index("horiz")
    me = lax.axis_index("depth")
    east = lax.rem(me_h + 1, n_h)
    west = lax.rem(me_h + n_h - 1, n_h)
    z, core = me // 2, lax.rem(me, 2)
    chips = n_d // 2
    steps = far_first(chips)
    on_low = core == 0

    def chip_at(step):
        return lax.rem(z + step, chips)

    def same_core(zz):
        return (me_h, zz * 2 + core)

    partner = (me_h, z * 2 + 1 - core)

    def remote(src, dst, send, recv, to):
        return pltpu.make_async_remote_copy(
            src_ref=src, dst_ref=dst, send_sem=send, recv_sem=recv, device_id=to, device_id_type=MESH)

    barrier = pltpu.get_barrier_semaphore()
    meets = [(east, z * 2), (west, z * 2), partner] + [(me_h, chip_at(step) * 2 + 1) for step in steps]
    for to in meets:
        pl.semaphore_signal(barrier, inc=1, device_id=to, device_id_type=MESH)

    small = [
        pltpu.make_async_copy(offs, offv, small_sem.at[0]),
        pltpu.make_async_copy(coup, cvec, small_sem.at[1]),
        pltpu.make_async_copy(inv, kvec, small_sem.at[2]),
    ]
    outer = []
    for i, first in enumerate((0, LINES - 8)):
        for h in range(2):
            for f in range(3):
                outer.append(pltpu.make_async_copy(
                    fields.at[f, :, pl.ds(first, 8), pl.ds(h * 128, 128)],
                    fbuf.at[:, h * 3 + f, pl.ds(8 + first, 8), :],
                    edge_sem.at[i, h * 3 + f]))

    def chunk_copies(c):
        lev = pl.ds(c * per, per)
        out = []
        for h in range(2):
            lane = pl.ds(h * 128, 128)
            for f in range(3):
                out.append(pltpu.make_async_copy(
                    fields.at[f, lev, pl.ds(8, LINES - 16), lane],
                    fbuf.at[lev, h * 3 + f, pl.ds(16, LINES - 16), :],
                    load_sem.at[c, h * 3 + f]))
            out.append(pltpu.make_async_copy(
                diff.at[lev, :, lane], dbuf.at[lev, h], load_sem.at[c, 6 + h]))
        return out

    for copy in small + outer:
        copy.start()
    for c in range(CHUNKS):
        for copy in chunk_copies(c):
            copy.start()

    f2 = fbuf.reshape(levels * 6 * PAD, 128)
    f2[pl.ds(7, levels * 6, stride=PAD), :] = jnp.zeros((levels * 6, 128), f32)
    f2[pl.ds(40, levels * 6, stride=PAD), :] = jnp.zeros((levels * 6, 128), f32)
    for e in range(2):
        hrecv[e, 0:8, :] = jnp.zeros((8, 128), f32)
        hrecv[e, 200:208, :] = jnp.zeros((8, 128), f32)
    m1[...] = jnp.zeros(m1.shape, f32)

    for copy in small:
        copy.wait()
    sub = lax.broadcasted_iota(jnp.int32, (8, 128), 0)
    lane = lax.broadcasted_iota(jnp.int32, (8, 128), 1)
    masks = []
    for g in range(GROUPS):
        v = jnp.full((8, 128), offv[8 * g], jnp.int32)
        for i in range(1, 8):
            v = jnp.where(sub == i, offv[8 * g + i], v)
        offl[g] = v
        masks.append([v == o for o in range(3)])

    def widen(x):
        return jnp.concatenate([x, jnp.zeros((4, 128 - levels), f32)], axis=1)

    couple = cvec[...]
    first_row = kvec[:, 0, :]
    last_row = kvec[:, levels - 2, :]
    c_low = couple[:, 0:1]
    c_high = couple[:, levels - 1:levels]
    inside = jnp.where(me > 0, 1.0, 0.0).astype(f32)
    table_low = first_row * (jnp.broadcast_to(c_low, (4, levels)) * inside)
    table_high = last_row * jnp.broadcast_to(c_high, (4, levels))
    lane4 = lax.broadcasted_iota(jnp.int32, (4, 128), 1)

    def pick(rows, m):
        return jnp.where(m[0], rows[0], jnp.where(m[1], rows[1], jnp.where(m[2], rows[2], rows[3])))

    def by_line(table):
        rows = [jnp.broadcast_to(table[o:o + 1, :], (8, 128)) for o in range(4)]
        return [pick(rows, masks[g]) for g in range(GROUPS)]

    def fill(ref, table, count):
        lines = by_line(table)
        for k in range(count):
            for g in range(GROUPS):
                ref[k, 8 * g:8 * g + 8, :] = jnp.broadcast_to(lines[g][:, k:k + 1], (8, 128))

    wide_high = widen(table_high)
    fill(low, jnp.where(lane4 == levels - 1, 0.0, widen(table_low)), levels)
    fill(high, jnp.where(lane4 == levels - 1, 1.0, wide_high), levels)

    c_low4 = jnp.broadcast_to(c_low, (4, 128))
    c_high4 = jnp.broadcast_to(c_high, (4, 128))
    alpha = c_high4 - c_high4 * jnp.broadcast_to(table_high[:, levels - 2:levels - 1], (4, 128))
    beta = c_low4 - c_low4 * jnp.broadcast_to(table_low[:, 0:1], (4, 128))
    cross = c_high4 * jnp.broadcast_to(table_low[:, levels - 2:levels - 1], (4, 128))
    packed = jnp.where(lane4 < 32, alpha, jnp.where(lane4 < 64, beta, cross))
    cmsg[0:4, :] = packed
    cmsg[4:8, :] = packed

    for copy in outer:
        copy.wait()
    hsend[0] = f2[pl.ds(39, levels * 6, stride=PAD), :]
    hsend[1] = f2[pl.ds(8, levels * 6, stride=PAD), :]
    is_last = lane == 127
    is_first = lane == 0

    def forcing(c, g):
        r0 = 8 + 8 * g
        rows = slice(8 * g, 8 * g + 8)
        sums = [m1[g * 6 + q, 8 * w:8 * w + 8, :] for w in range(2) for q in range(6)]
        for l in range(per):
            k = c * per + l
            hi = high[k, rows, :]
            lo = low[k, rows, :]
            mid = [fbuf[k, q, r0:r0 + 8, :] for q in range(6)]
            es = [fbuf[k, q, r0 + 1:r0 + 9, :] for q in range(6)]
            ws = [fbuf[k, q, r0 - 1:r0 + 7, :] for q in range(6)]
            up = [pltpu.roll(mid[q], 127, 1) for q in range(6)]
            dn = [pltpu.roll(mid[q], 1, 1) for q in range(6)]
            for h in range(2):
                d = dbuf[k, h, rows, :]
                keep = 1.0 - 4.0 * d
                q = [h * 3 + f for f in range(3)]
                qo = [(1 - h) * 3 + f for f in range(3)]
                north = [jnp.where(is_last, up[qo[f]], up[q[f]]) for f in range(3)]
                south = [jnp.where(is_first, dn[qo[f]], dn[q[f]]) for f in range(3)]
                base = [
                    mid[q[f]] * keep + d * ((es[q[f]] + ws[q[f]]) + (north[f] + south[f]))
                    for f in range(3)
                ]
                out = [
                    base[0] - 0.25 * (es[q[2]] - ws[q[2]]),
                    base[1] - 0.25 * (north[2] - south[2]),
                    base[2] - 0.25 * ((es[q[0]] - ws[q[0]]) + (north[1] - south[1])),
                ]
                for f in range(3):
                    sol[k, q[f], rows, :] = out[f]
                    sums[q[f]] = sums[q[f]] + hi * out[f]
                    sums[6 + q[f]] = sums[6 + q[f]] + lo * out[f]
        for w in range(2):
            for q in range(6):
                m1[g * 6 + q, 8 * w:8 * w + 8, :] = sums[w * 6 + q]

    def slot_forcing(slot, first):
        def step_chunk(c, carry):
            if first:
                for copy in chunk_copies(c):
                    copy.wait()
            for g in range(2 * slot, 2 * slot + 2):
                forcing(c, g)
            return carry

        lax.fori_loop(0, CHUNKS, step_chunk, 0)

    for slot in range(2):
        @pl.when(core == 1 - slot)
        def _():
            slot_forcing(slot, True)

    halo = [
        remote(hsend.at[e], hrecv.at[e, pl.ds(8, levels * 6), :], hs_sem.at[e], hr_sem.at[e], (to, me))
        for e, to in ((0, east), (1, west))
    ]
    pair_coef = remote(cmsg, cpart, pair_send.at[0], pair_recv.at[0], partner)
    pair_rows = remote(m1.at[pl.ds((1 - core) * HALF, HALF)], other, pair_send.at[1], pair_recv.at[1], partner)

    @pl.when(core == 1)
    def _():
        pl.semaphore_wait(barrier, 2 * len(steps) + 1)
        pl.semaphore_signal(gate.at[0], inc=1, device_id=partner, device_id_type=MESH)

    @pl.when(core == 0)
    def _():
        pl.semaphore_wait(gate.at[0], 1)

    for copy in (pair_coef, pair_rows):
        copy.start()
    for slot in range(2):
        @pl.when(core == slot)
        def _():
            slot_forcing(slot, False)

    def splat(tile, at):
        return jnp.broadcast_to(tile[:, at:at + 1], (8, 128))

    pair_coef.wait_recv()
    mine, theirs = cmsg[...], cpart[...]
    tile0 = jnp.where(on_low, mine, theirs)
    tile1 = jnp.where(on_low, theirs, mine)
    alpha0, beta0, cross0 = (splat(tile0, at) for at in (0, 32, 64))
    alpha1, beta1, cross1 = (splat(tile1, at) for at in (0, 32, 64))
    mid_pivot = 1.0 / (1.0 + alpha0 + beta1)
    to_low = cross0 * mid_pivot
    to_high = cross1 * mid_pivot
    chip[...] = jnp.where(
        lane < 32, alpha1 - cross1 * to_high,
        jnp.where(lane < 64, beta0 - cross0 * to_low, cross0 * to_high))
    lcoef[0] = to_low
    lcoef[1] = to_high
    lcoef[2] = mid_pivot

    def coef_copy(j, zz):
        return remote(chip, crecv.at[z], cs_sem.at[j], cr_sem.at[z], same_core(zz))

    for j, step in enumerate(steps):
        coef_copy(j, chip_at(step)).start()

    def one(ref, line):
        return jnp.broadcast_to(ref[line:line + 1, :], (8, 128))

    def group_masks(g):
        v = offl[g]
        return [v == o for o in range(3)]

    own_masks = [group_masks(2 * core + gg) for gg in range(2)]
    own = [
        [pick([one(lcoef.at[i], o) for o in range(4)], own_masks[gg]) for i in range(3)]
        for gg in range(2)
    ]
    pair_rows.wait_recv()
    for i in range(HALF):
        low_k, high_k, _ = own[i // 6]
        a_mine, b_mine = m1[core * HALF + i, 0:8, :], m1[core * HALF + i, 8:16, :]
        a_other, b_other = other[i, 0:8, :], other[i, 8:16, :]
        t = jnp.where(on_low, a_mine, a_other) + jnp.where(on_low, b_other, b_mine)
        middle[i] = t
        chip_rows[i, 0:8, :] = jnp.where(on_low, a_other, a_mine) + high_k * t
        chip_rows[i, 8:16, :] = jnp.where(on_low, b_mine, b_other) + low_k * t

    def solver_of(i, w, m):
        b = (m + core) // 2
        return w * 2 + b, m - b * (2 - core)

    def targets():
        for n, dw in enumerate((2, 1, 3, 0)):
            w = lax.rem(z // 2 + dw, chips // 2)
            for m in range(3):
                zz, j = solver_of(None, w, m)
                yield n * 3 + m, zz, j, w * 3 + m

    def target_copy(n, zz, j, unit):
        return remote(chip_rows.at[unit], r1.at[j, z], s1_sem.at[n], r1_sem.at[j, z], same_core(zz))

    for n, zz, j, unit in targets():
        @pl.when(zz != z)
        def _():
            target_copy(n, zz, j, unit).start()

        @pl.when(zz == z)
        def _():
            r1[j, z] = chip_rows[unit]

    @pl.when(core == 0)
    def _():
        pl.semaphore_wait(barrier, 5)
        pl.semaphore_signal(gate.at[1], inc=1, device_id=partner, device_id_type=MESH)

    @pl.when(core == 1)
    def _():
        pl.semaphore_wait(gate.at[1], 1)

    for copy in halo:
        copy.start()

    shift_high = pltpu.roll(wide_high, 1, 1)
    inner = jnp.logical_and(lane4 > 0, lane4 < levels - 1)
    ratio = jnp.where(inner, shift_high / jnp.where(inner, wide_high, 1.0), 0.0)
    inner_c = jnp.where(inner, widen(couple), 1.0)
    pivot = pltpu.roll(ratio / inner_c, 127, 1)
    pivot = jnp.where(lane4 == levels - 2, widen(last_row), pivot)
    fill(wv, ratio, levels)
    fill(iv, pivot, levels - 1)

    def down(k, carry):
        out = []
        for g in range(GROUPS):
            rows = slice(8 * g, 8 * g + 8)
            w = wv[k, rows, :]
            for q in range(6):
                y = sol[k, q, rows, :] + w * carry[g * 6 + q]
                sol[k, q, rows, :] = y
                out.append(y)
        return tuple(out)

    def rise(i, carry):
        k = levels - 2 - i
        out = []
        for g in range(GROUPS):
            rows = slice(8 * g, 8 * g + 8)
            piv = iv[k, rows, :]
            w = wv[k + 1, rows, :]
            for q in range(6):
                x = piv * sol[k, q, rows, :] + w * carry[g * 6 + q]
                sol[k, q, rows, :] = x
                out.append(x)
        return tuple(out)

    zero = jnp.zeros((8, 128), f32)
    lax.fori_loop(1, levels - 1, down,
                  tuple(sol[0, q, 8 * g:8 * g + 8, :] for g in range(GROUPS) for q in range(6)))
    lax.fori_loop(0, levels - 1, rise, (zero,) * UNITS)
    for q in range(6):
        sol[levels - 1, q] = jnp.zeros((LINES, 128), f32)

    crecv[z] = chip[...]
    for step in steps:
        zz = chip_at(step)
        remote(chip, crecv.at[zz], cs_sem.at[0], cr_sem.at[zz], same_core(zz)).wait_recv()
    alphas, betas, crosses = [], [], []
    for r in range(chips):
        tile = crecv[r]
        alphas.append(splat(tile, 0))
        betas.append(splat(tile, 32))
        crosses.append(splat(tile, 64))
    mains = [1.0 + alphas[r] + (betas[r + 1] if r + 1 < chips else 0.0) for r in range(chips)]
    before = None
    for r in range(chips):
        q = crosses[r] * before if r > 0 else zero
        main = mains[r] - crosses[r] * q if r > 0 else mains[r]
        before = 1.0 / main
        comp[0, r] = q
        comp[1, r] = before
        comp[4, r] = crosses[r]
    after = None
    for r in range(chips - 1, -1, -1):
        q = crosses[r + 1] * after if r + 1 < chips else zero
        main = mains[r] - crosses[r + 1] * q if r + 1 < chips else mains[r]
        after = 1.0 / main
        comp[2, r] = q
        comp[3, r] = main

    parity = lax.rem(z, 2)
    first_unit = (z // 2) * 3 + parity * (2 - core)
    has = [None, parity == core]
    for j in range(2):
        m = group_masks(2 * core + jnp.minimum(first_unit + j, HALF - 1) // 6)
        for i in range(2):
            for r in range(chips):
                ucoef[j, i, r] = pick([one(comp.at[i, r], o) for o in range(4)], m)

    for copy in halo:
        copy.wait_recv()
    third = lax.rem(sub, 3)
    m_first = jnp.where(jnp.logical_and(third == 0, sub < 6), 0.25, 0.0).astype(f32)
    m_third = jnp.where(jnp.logical_and(third == 2, sub < 6), 0.25, 0.0).astype(f32)
    edge_line = (0, LINES - 1)
    for e in range(2):
        sign = 1.0 if e == 0 else -1.0
        line = edge_line[e]
        sum_a = [zero, zero]
        sum_b = [zero, zero]
        for k in range(levels):
            r = 8 + 6 * k
            here = hrecv[e, r:r + 8, :]
            above = hrecv[e, r + 2:r + 10, :]
            below = hrecv[e, r - 2:r + 6, :]
            d = jnp.where(sub < 3, one(dbuf.at[k, 0], line), one(dbuf.at[k, 1], line))
            change = d * here + sign * (m_first * above + m_third * below)
            delta[e, k] = change
            sum_a[k % 2] = sum_a[k % 2] + one(high.at[k], line) * change
            sum_b[k % 2] = sum_b[k % 2] + one(low.at[k], line) * change
        esum[e, 0:8, :] = sum_a[0] + sum_a[1]
        esum[e, 8:16, :] = sum_b[0] + sum_b[1]
    pair_edge = remote(esum.at[1 - core], epart, pair_send.at[2], pair_recv.at[2], partner)
    pair_edge.start()

    def answer(j, n, zz):
        return remote(m2.at[j, zz], got.at[first_unit + j], s2_sem.at[j, n], r2_sem.at[first_unit + j],
                      same_core(zz))

    def solve_unit(j):
        for step in steps:
            zz = chip_at(step)
            remote(chip_rows.at[0], r1.at[j, zz], s1_sem.at[0], r1_sem.at[j, zz], same_core(zz)).wait_recv()
        values = []
        for r in range(chips):
            t = r1[j, r, 0:8, :]
            if r + 1 < chips:
                t = t + r1[j, r + 1, 8:16, :]
            values.append(t if r == 0 else t + ucoef[j, 0, r] * values[r - 1])
        s = values[chips - 1] * ucoef[j, 1, chips - 1]
        for r in range(chips - 1, -1, -1):
            m2[j, r, 8:16, :] = s
            if r + 1 < chips:
                m2[j, r + 1, 0:8, :] = s
            if r > 0:
                s = values[r - 1] * ucoef[j, 1, r - 1] + ucoef[j, 0, r] * s
        m2[j, 0, 0:8, :] = zero
        for n, step in enumerate(steps):
            answer(j, n, chip_at(step)).start()
        got[first_unit + j] = m2[j, z]

    solve_unit(0)

    @pl.when(has[1])
    def _():
        solve_unit(1)

    edge_off = offv[core * (LINES - 1)]
    z_low = jnp.maximum(z - 1, 0)

    def edge_comp(i, r):
        return jnp.broadcast_to(comp[i, r, pl.ds(edge_off, 1), :], (8, 128))

    def edge_local(i):
        return jnp.broadcast_to(lcoef[i, pl.ds(edge_off, 1), :], (8, 128))

    pair_edge.wait_recv()
    a_mine, b_mine = esum[core, 0:8, :], esum[core, 8:16, :]
    a_other, b_other = epart[0:8, :], epart[8:16, :]
    edge_t = jnp.where(on_low, a_mine, a_other) + jnp.where(on_low, b_other, b_mine)
    edge_a = jnp.where(on_low, a_other, a_mine) + edge_local(1) * edge_t
    edge_b = jnp.where(on_low, b_mine, b_other) + edge_local(0) * edge_t
    em[0] = edge_a + edge_comp(0, z) * edge_b
    em[1] = edge_b + edge_comp(2, z_low) * edge_a

    def edge_copy(n, zz):
        return remote(em.at[jnp.where(zz > z, 0, 1)], er.at[z], es_sem.at[n], er_sem.at[z], same_core(zz))

    for n, step in enumerate(steps):
        edge_copy(n, chip_at(step)).start()

    sol2 = sol.reshape(levels * 6 * LINES, 128)
    for e in range(2):
        line = edge_line[e]
        prev = delta[e, 0]
        for k in range(1, levels - 1):
            prev = delta[e, k] + one(wv.at[k], line) * prev
            delta[e, k] = prev
        x = zero
        for k in range(levels - 2, -1, -1):
            x = one(iv.at[k], line) * delta[e, k] + one(wv.at[k + 1], line) * x
            rows = pl.ds(k * 6 * LINES + line, 6, stride=LINES)
            sol2[rows, :] = sol2[rows, :] + x[0:6, :]

    for step in steps:
        zz = chip_at(step)
        remote(em.at[0], er.at[zz], es_sem.at[0], er_sem.at[zz], same_core(zz)).wait_recv()
    v = zero
    w = zero
    for r in range(chips):
        v = jnp.where(r < z, er[r] + edge_comp(0, r) * v, v)
    for r in range(chips - 1, 0, -1):
        w = jnp.where(r > z, er[r] + edge_comp(2, r - 1) * w, w)
    v = v + edge_b
    w = w + edge_a
    q_here = edge_comp(0, z)
    u_here = edge_comp(4, z)
    edge_high = (w + q_here * v) / (edge_comp(3, z) - u_here * q_here)
    edge_low = jnp.where(z > 0, (v + u_here * edge_high) * edge_comp(1, z_low), 0.0)

    for i in range(HALF):
        @pl.when(w_solver(i, core) != z)
        def _():
            remote(m2.at[0, 0], got.at[i], s2_sem.at[0, 0], r2_sem.at[i], same_core(w_solver(i, core))).wait_recv()
    got2 = got.reshape((HALF + 2) * 16, 128)
    middle2 = middle.reshape((HALF + 2) * 8, 128)
    for e in range(2):
        @pl.when(core == e)
        def _():
            for ref, size, at, add in (
                    (got2, 16, 0, edge_low), (got2, 16, 8, edge_high), (middle2, 8, 0, edge_t)):
                rows = pl.ds(6 * e * size + at + 7 * e, 6, stride=size)
                ref[rows, :] = ref[rows, :] + add[0:6, :]
    for i in range(HALF):
        low_k, high_k, pivot_k = own[i // 6]
        s_low, s_high = got[i, 0:8, :], got[i, 8:16, :]
        s_mid = middle[i] * pivot_k + low_k * s_low + high_k * s_high
        back[core * HALF + i, 0:8, :] = jnp.where(on_low, s_low, s_mid)
        back[core * HALF + i, 8:16, :] = jnp.where(on_low, s_mid, s_high)
        pass_on[i, 0:8, :] = jnp.where(on_low, s_mid, s_low)
        pass_on[i, 8:16, :] = jnp.where(on_low, s_high, s_mid)
    pair_ends = remote(pass_on, back.at[pl.ds(core * HALF, HALF)], pair_send.at[3], pair_recv.at[3], partner)
    pair_ends.start()

    for copy in (*halo, pair_coef, pair_rows, pair_edge):
        copy.wait_send()
    for n, step in enumerate(steps):
        coef_copy(n, chip_at(step)).wait_send()
        edge_copy(n, chip_at(step)).wait_send()
        answer(0, n, chip_at(step)).wait_send()
    for n, zz, j, unit in targets():
        @pl.when(zz != z)
        def _():
            target_copy(n, zz, j, unit).wait_send()

    @pl.when(has[1])
    def _():
        for n, step in enumerate(steps):
            answer(1, n, chip_at(step)).wait_send()
    pair_ends.wait()


def w_solver(i, core):
    return (i // 3) * 2 + (i % 3 + core) // 2


def assemble_kernel(sol, back, low, high, out, stage, sem):
    levels = sol.shape[0]
    per = levels // CHUNKS

    def copies(c):
        lev = pl.ds(c * per, per)
        return [
            pltpu.make_async_copy(
                stage.at[lev, h * 3 + f], out.at[f, lev, :, pl.ds(h * 128, 128)], sem.at[c, h * 3 + f])
            for h in range(2) for f in range(3)
        ]

    def chunk(c, carry):
        for g in range(GROUPS):
            rows = slice(8 * g, 8 * g + 8)
            prev = [back[g * 6 + q, 0:8, :] for q in range(6)]
            here = [back[g * 6 + q, 8:16, :] for q in range(6)]
            for l in range(per):
                k = c * per + l
                lo = low[k, rows, :]
                hi = high[k, rows, :]
                for q in range(6):
                    stage[k, q, rows, :] = sol[k, q, rows, :] + (lo * prev[q] + hi * here[q])
        for copy in copies(c):
            copy.start()
        return carry

    lax.fori_loop(0, CHUNKS, chunk, 0)
    for c in range(CHUNKS):
        for copy in copies(c):
            copy.wait()


def body(n_h, n_d, fields, diffusivity, offsets, coupling, inverse):
    f32 = jnp.float32
    levels = fields.shape[1]
    chips = n_d // 2
    hbm_spec = pl.BlockSpec(memory_space=pltpu.HBM)
    vmem_spec = pl.BlockSpec(memory_space=pltpu.VMEM)
    V = lambda *shape: pltpu.VMEM(shape, f32)
    dma = lambda *shape: pltpu.SemaphoreType.DMA(shape)
    sol, back, low, high = pl.pallas_call(
        functools.partial(columns_kernel, n_h, n_d),
        out_shape=(
            V(levels, 6, LINES, 128),
            V(UNITS, 16, 128),
            V(levels, LINES, 128),
            V(levels, LINES, 128),
        ),
        in_specs=[hbm_spec] * 5,
        out_specs=(vmem_spec,) * 4,
        scratch_shapes=[
            V(levels, 6, PAD, 128),
            V(levels, 2, LINES, 128),
            pltpu.SMEM((LINES,), jnp.int32),
            V(4, levels),
            V(4, levels, levels),
            pltpu.VMEM((GROUPS, 8, 128), jnp.int32),
            V(levels, LINES, 128),
            V(levels, LINES, 128),
            V(2, levels, 8, 128),
            V(2, levels * 6, 128),
            V(2, levels * 6 + 16, 128),
            V(8, 128),
            V(8, 128),
            V(8, 128),
            V(chips, 8, 128),
            V(UNITS, 16, 128),
            V(HALF, 16, 128),
            V(HALF, 16, 128),
            V(HALF + 2, 8, 128),
            V(2, chips, 16, 128),
            V(2, chips, 16, 128),
            V(HALF + 2, 16, 128),
            V(HALF, 16, 128),
            V(2, 16, 128),
            V(16, 128),
            V(2, 8, 128),
            V(chips, 8, 128),
            V(5, chips, 8, 128),
            V(2, 2, chips, 8, 128),
            V(3, 8, 128),
            dma(2, 6),
            dma(CHUNKS, 8),
            dma(3),
            dma(2),
            dma(2),
            dma(4),
            dma(4),
            dma(chips),
            dma(chips),
            dma(HALF),
            dma(2, chips),
            dma(2, chips),
            dma(HALF),
            dma(chips),
            dma(chips),
            pltpu.SemaphoreType.REGULAR((2,)),
        ],
        compiler_params=pltpu.CompilerParams(
            collective_id=0, has_side_effects=True, vmem_limit_bytes=48 * 1024 * 1024),
        name="columns",
    )(*(pltpu.with_memory_space_constraint(x, pltpu.HBM)
        for x in (fields, diffusivity, offsets, coupling, inverse)))
    return pl.pallas_call(
        assemble_kernel,
        out_shape=jax.ShapeDtypeStruct(fields.shape, f32),
        in_specs=[vmem_spec] * 4,
        out_specs=hbm_spec,
        scratch_shapes=[
            V(levels, 6, LINES, 128),
            dma(CHUNKS, 6),
        ],
        compiler_params=pltpu.CompilerParams(vmem_limit_bytes=48 * 1024 * 1024),
        name="assemble",
    )(sol, back, low, high)


def solution(mesh):
    return jax.shard_map(
        functools.partial(body, mesh.shape["horiz"], mesh.shape["depth"]),
        mesh=mesh,
        in_specs=(
            P(None, "depth", "horiz", None),
            P("depth", "horiz", None),
            P("horiz"),
            P(None, "depth"),
            P(None, "depth", None),
        ),
        out_specs=P(None, "depth", "horiz", None),
        check_vma=False,
    )
```

```python
import functools

import jax
import jax.numpy as jnp
from jax import lax
from jax.experimental import pallas as pl
from jax.experimental.pallas import tpu as pltpu
from jax.sharding import PartitionSpec as P

MESH = pl.DeviceIdType.MESH
CHUNKS = 4
PAD = 48
LINES = 32
GROUPS = LINES // 8
UNITS = GROUPS * 6
HALF = UNITS // 2


def far_first(chips):
    return sorted(range(1, chips), key=lambda s: -min(s, chips - s))


def columns_kernel(
    n_h, n_d,
    fields, diff, offs, coup, inv,
    sol, back, low, high,
    fbuf, dbuf, offv, cvec, kvec, offl, wv, iv, delta,
    hsend, hrecv, cmsg, cpart, chip, crecv, m1, other, chip_rows, middle, r1, m2, got, pass_on,
    esum, epart, em, er, comp, ucoef, lcoef,
    edge_sem, load_sem, small_sem, hs_sem, hr_sem, pair_send, pair_recv, cs_sem, cr_sem,
    s1_sem, r1_sem, s2_sem, r2_sem, es_sem, er_sem, gate,
):
    f32 = jnp.float32
    levels = fields.shape[1]
    per = levels // CHUNKS
    me_h = lax.axis_index("horiz")
    me = lax.axis_index("depth")
    east = lax.rem(me_h + 1, n_h)
    west = lax.rem(me_h + n_h - 1, n_h)
    z, core = me // 2, lax.rem(me, 2)
    chips = n_d // 2
    steps = far_first(chips)
    on_low = core == 0

    def chip_at(step):
        return lax.rem(z + step, chips)

    def same_core(zz):
        return (me_h, zz * 2 + core)

    partner = (me_h, z * 2 + 1 - core)

    def remote(src, dst, send, recv, to):
        return pltpu.make_async_remote_copy(
            src_ref=src, dst_ref=dst, send_sem=send, recv_sem=recv, device_id=to, device_id_type=MESH)

    barrier = pltpu.get_barrier_semaphore()
    meets = [(east, z * 2), (west, z * 2), partner] + [(me_h, chip_at(step) * 2 + 1) for step in steps]
    for to in meets:
        pl.semaphore_signal(barrier, inc=1, device_id=to, device_id_type=MESH)

    small = [
        pltpu.make_async_copy(offs, offv, small_sem.at[0]),
        pltpu.make_async_copy(coup, cvec, small_sem.at[1]),
        pltpu.make_async_copy(inv, kvec, small_sem.at[2]),
    ]
    outer = []
    for i, first in enumerate((0, LINES - 8)):
        for h in range(2):
            for f in range(3):
                outer.append(pltpu.make_async_copy(
                    fields.at[f, :, pl.ds(first, 8), pl.ds(h * 128, 128)],
                    fbuf.at[:, h * 3 + f, pl.ds(8 + first, 8), :],
                    edge_sem.at[i, h * 3 + f]))

    def chunk_copies(c):
        lev = pl.ds(c * per, per)
        out = []
        for h in range(2):
            lane = pl.ds(h * 128, 128)
            for f in range(3):
                out.append(pltpu.make_async_copy(
                    fields.at[f, lev, pl.ds(8, LINES - 16), lane],
                    fbuf.at[lev, h * 3 + f, pl.ds(16, LINES - 16), :],
                    load_sem.at[c, h * 3 + f]))
            out.append(pltpu.make_async_copy(
                diff.at[lev, :, lane], dbuf.at[lev, h], load_sem.at[c, 6 + h]))
        return out

    for copy in small + outer:
        copy.start()
    for c in range(CHUNKS):
        for copy in chunk_copies(c):
            copy.start()

    f2 = fbuf.reshape(levels * 6 * PAD, 128)
    f2[pl.ds(7, levels * 6, stride=PAD), :] = jnp.zeros((levels * 6, 128), f32)
    f2[pl.ds(40, levels * 6, stride=PAD), :] = jnp.zeros((levels * 6, 128), f32)
    for e in range(2):
        hrecv[e, 0:8, :] = jnp.zeros((8, 128), f32)
        hrecv[e, 200:208, :] = jnp.zeros((8, 128), f32)
    m1[...] = jnp.zeros(m1.shape, f32)

    for copy in small:
        copy.wait()
    sub = lax.broadcasted_iota(jnp.int32, (8, 128), 0)
    lane = lax.broadcasted_iota(jnp.int32, (8, 128), 1)
    masks = []
    for g in range(GROUPS):
        v = jnp.full((8, 128), offv[8 * g], jnp.int32)
        for i in range(1, 8):
            v = jnp.where(sub == i, offv[8 * g + i], v)
        offl[g] = v
        masks.append([v == o for o in range(3)])

    def widen(x):
        return jnp.concatenate([x, jnp.zeros((4, 128 - levels), f32)], axis=1)

    couple = cvec[...]
    first_row = kvec[:, 0, :]
    last_row = kvec[:, levels - 2, :]
    c_low = couple[:, 0:1]
    c_high = couple[:, levels - 1:levels]
    inside = jnp.where(me > 0, 1.0, 0.0).astype(f32)
    table_low = first_row * (jnp.broadcast_to(c_low, (4, levels)) * inside)
    table_high = last_row * jnp.broadcast_to(c_high, (4, levels))
    lane4 = lax.broadcasted_iota(jnp.int32, (4, 128), 1)

    def pick(rows, m):
        return jnp.where(m[0], rows[0], jnp.where(m[1], rows[1], jnp.where(m[2], rows[2], rows[3])))

    def by_line(table):
        rows = [jnp.broadcast_to(table[o:o + 1, :], (8, 128)) for o in range(4)]
        return [pick(rows, masks[g]) for g in range(GROUPS)]

    def fill(ref, table, count):
        lines = by_line(table)
        for k in range(count):
            for g in range(GROUPS):
                ref[k, 8 * g:8 * g + 8, :] = jnp.broadcast_to(lines[g][:, k:k + 1], (8, 128))

    wide_high = widen(table_high)
    fill(low, jnp.where(lane4 == levels - 1, 0.0, widen(table_low)), levels)
    fill(high, jnp.where(lane4 == levels - 1, 1.0, wide_high), levels)

    c_low4 = jnp.broadcast_to(c_low, (4, 128))
    c_high4 = jnp.broadcast_to(c_high, (4, 128))
    alpha = c_high4 - c_high4 * jnp.broadcast_to(table_high[:, levels - 2:levels - 1], (4, 128))
    beta = c_low4 - c_low4 * jnp.broadcast_to(table_low[:, 0:1], (4, 128))
    cross = c_high4 * jnp.broadcast_to(table_low[:, levels - 2:levels - 1], (4, 128))
    packed = jnp.where(lane4 < 32, alpha, jnp.where(lane4 < 64, beta, cross))
    cmsg[0:4, :] = packed
    cmsg[4:8, :] = packed

    for copy in outer:
        copy.wait()
    hsend[0] = f2[pl.ds(39, levels * 6, stride=PAD), :]
    hsend[1] = f2[pl.ds(8, levels * 6, stride=PAD), :]
    halo = [
        remote(hsend.at[e], hrecv.at[e, pl.ds(8, levels * 6), :], hs_sem.at[e], hr_sem.at[e], (to, me))
        for e, to in ((0, east), (1, west))
    ]

    waits_late = lax.rem(me_h, 4) == 0

    def send_halo():
        @pl.when(core == 0)
        def _():
            pl.semaphore_wait(barrier, 5)
            pl.semaphore_signal(gate.at[1], inc=1, device_id=partner, device_id_type=MESH)

        @pl.when(core == 1)
        def _():
            pl.semaphore_wait(gate.at[1], 1)

        for copy in halo:
            copy.start()

    @pl.when(jnp.logical_not(waits_late))
    def _():
        send_halo()

    is_last = lane == 127
    is_first = lane == 0

    def forcing(c, g):
        r0 = 8 + 8 * g
        rows = slice(8 * g, 8 * g + 8)
        sums = [m1[g * 6 + q, 8 * w:8 * w + 8, :] for w in range(2) for q in range(6)]
        for l in range(per):
            k = c * per + l
            hi = high[k, rows, :]
            lo = low[k, rows, :]
            mid = [fbuf[k, q, r0:r0 + 8, :] for q in range(6)]
            es = [fbuf[k, q, r0 + 1:r0 + 9, :] for q in range(6)]
            ws = [fbuf[k, q, r0 - 1:r0 + 7, :] for q in range(6)]
            up = [pltpu.roll(mid[q], 127, 1) for q in range(6)]
            dn = [pltpu.roll(mid[q], 1, 1) for q in range(6)]
            for h in range(2):
                d = dbuf[k, h, rows, :]
                keep = 1.0 - 4.0 * d
                q = [h * 3 + f for f in range(3)]
                qo = [(1 - h) * 3 + f for f in range(3)]
                north = [jnp.where(is_last, up[qo[f]], up[q[f]]) for f in range(3)]
                south = [jnp.where(is_first, dn[qo[f]], dn[q[f]]) for f in range(3)]
                base = [
                    mid[q[f]] * keep + d * ((es[q[f]] + ws[q[f]]) + (north[f] + south[f]))
                    for f in range(3)
                ]
                out = [
                    base[0] - 0.25 * (es[q[2]] - ws[q[2]]),
                    base[1] - 0.25 * (north[2] - south[2]),
                    base[2] - 0.25 * ((es[q[0]] - ws[q[0]]) + (north[1] - south[1])),
                ]
                for f in range(3):
                    sol[k, q[f], rows, :] = out[f]
                    sums[q[f]] = sums[q[f]] + hi * out[f]
                    sums[6 + q[f]] = sums[6 + q[f]] + lo * out[f]
        for w in range(2):
            for q in range(6):
                m1[g * 6 + q, 8 * w:8 * w + 8, :] = sums[w * 6 + q]

    def slot_forcing(slot, first):
        def step_chunk(c, carry):
            if first:
                for copy in chunk_copies(c):
                    copy.wait()
            for g in range(2 * slot, 2 * slot + 2):
                forcing(c, g)
            return carry

        lax.fori_loop(0, CHUNKS, step_chunk, 0)

    for slot in range(2):
        @pl.when(core == 1 - slot)
        def _():
            slot_forcing(slot, True)

    pair_coef = remote(cmsg, cpart, pair_send.at[0], pair_recv.at[0], partner)
    pair_rows = remote(m1.at[pl.ds((1 - core) * HALF, HALF)], other, pair_send.at[1], pair_recv.at[1], partner)

    @pl.when(core == 1)
    def _():
        pl.semaphore_wait(barrier, 2 * len(steps) + 1)
        pl.semaphore_signal(gate.at[0], inc=1, device_id=partner, device_id_type=MESH)

    @pl.when(core == 0)
    def _():
        pl.semaphore_wait(gate.at[0], 1)

    for copy in (pair_coef, pair_rows):
        copy.start()
    for slot in range(2):
        @pl.when(core == slot)
        def _():
            slot_forcing(slot, False)

    def splat(tile, at):
        return jnp.broadcast_to(tile[:, at:at + 1], (8, 128))

    pair_coef.wait_recv()
    mine, theirs = cmsg[...], cpart[...]
    tile0 = jnp.where(on_low, mine, theirs)
    tile1 = jnp.where(on_low, theirs, mine)
    alpha0, beta0, cross0 = (splat(tile0, at) for at in (0, 32, 64))
    alpha1, beta1, cross1 = (splat(tile1, at) for at in (0, 32, 64))
    mid_pivot = 1.0 / (1.0 + alpha0 + beta1)
    to_low = cross0 * mid_pivot
    to_high = cross1 * mid_pivot
    chip[...] = jnp.where(
        lane < 32, alpha1 - cross1 * to_high,
        jnp.where(lane < 64, beta0 - cross0 * to_low, cross0 * to_high))
    lcoef[0] = to_low
    lcoef[1] = to_high
    lcoef[2] = mid_pivot

    def coef_copy(j, zz):
        return remote(chip, crecv.at[z], cs_sem.at[j], cr_sem.at[z], same_core(zz))

    for j, step in enumerate(steps):
        coef_copy(j, chip_at(step)).start()

    def one(ref, line):
        return jnp.broadcast_to(ref[line:line + 1, :], (8, 128))

    def group_masks(g):
        v = offl[g]
        return [v == o for o in range(3)]

    own_masks = [group_masks(2 * core + gg) for gg in range(2)]
    own = [
        [pick([one(lcoef.at[i], o) for o in range(4)], own_masks[gg]) for i in range(3)]
        for gg in range(2)
    ]
    pair_rows.wait_recv()
    for i in range(HALF):
        low_k, high_k, _ = own[i // 6]
        a_mine, b_mine = m1[core * HALF + i, 0:8, :], m1[core * HALF + i, 8:16, :]
        a_other, b_other = other[i, 0:8, :], other[i, 8:16, :]
        t = jnp.where(on_low, a_mine, a_other) + jnp.where(on_low, b_other, b_mine)
        middle[i] = t
        chip_rows[i, 0:8, :] = jnp.where(on_low, a_other, a_mine) + high_k * t
        chip_rows[i, 8:16, :] = jnp.where(on_low, b_mine, b_other) + low_k * t

    def solver_of(i, w, m):
        b = (m + core) // 2
        return w * 2 + b, m - b * (2 - core)

    def targets():
        for n, dw in enumerate((2, 1, 3, 0)):
            w = lax.rem(z // 2 + dw, chips // 2)
            for m in range(3):
                zz, j = solver_of(None, w, m)
                yield n * 3 + m, zz, j, w * 3 + m

    def target_copy(n, zz, j, unit):
        return remote(chip_rows.at[unit], r1.at[j, z], s1_sem.at[n], r1_sem.at[j, z], same_core(zz))

    for n, zz, j, unit in targets():
        @pl.when(zz != z)
        def _():
            target_copy(n, zz, j, unit).start()

        @pl.when(zz == z)
        def _():
            r1[j, z] = chip_rows[unit]

    @pl.when(waits_late)
    def _():
        send_halo()

    shift_high = pltpu.roll(wide_high, 1, 1)
    inner = jnp.logical_and(lane4 > 0, lane4 < levels - 1)
    ratio = jnp.where(inner, shift_high / jnp.where(inner, wide_high, 1.0), 0.0)
    inner_c = jnp.where(inner, widen(couple), 1.0)
    pivot = pltpu.roll(ratio / inner_c, 127, 1)
    pivot = jnp.where(lane4 == levels - 2, widen(last_row), pivot)
    fill(wv, ratio, levels)
    fill(iv, pivot, levels - 1)

    def down(k, carry):
        out = []
        for g in range(GROUPS):
            rows = slice(8 * g, 8 * g + 8)
            w = wv[k, rows, :]
            for q in range(6):
                y = sol[k, q, rows, :] + w * carry[g * 6 + q]
                sol[k, q, rows, :] = y
                out.append(y)
        return tuple(out)

    def rise(i, carry):
        k = levels - 2 - i
        out = []
        for g in range(GROUPS):
            rows = slice(8 * g, 8 * g + 8)
            piv = iv[k, rows, :]
            w = wv[k + 1, rows, :]
            for q in range(6):
                x = piv * sol[k, q, rows, :] + w * carry[g * 6 + q]
                sol[k, q, rows, :] = x
                out.append(x)
        return tuple(out)

    zero = jnp.zeros((8, 128), f32)
    lax.fori_loop(1, levels - 1, down,
                  tuple(sol[0, q, 8 * g:8 * g + 8, :] for g in range(GROUPS) for q in range(6)))
    lax.fori_loop(0, levels - 1, rise, (zero,) * UNITS)
    for q in range(6):
        sol[levels - 1, q] = jnp.zeros((LINES, 128), f32)

    crecv[z] = chip[...]
    for step in steps:
        zz = chip_at(step)
        remote(chip, crecv.at[zz], cs_sem.at[0], cr_sem.at[zz], same_core(zz)).wait_recv()
    alphas, betas, crosses = [], [], []
    for r in range(chips):
        tile = crecv[r]
        alphas.append(splat(tile, 0))
        betas.append(splat(tile, 32))
        crosses.append(splat(tile, 64))
    mains = [1.0 + alphas[r] + (betas[r + 1] if r + 1 < chips else 0.0) for r in range(chips)]
    before = None
    for r in range(chips):
        q = crosses[r] * before if r > 0 else zero
        main = mains[r] - crosses[r] * q if r > 0 else mains[r]
        before = 1.0 / main
        comp[0, r] = q
        comp[1, r] = before
        comp[4, r] = crosses[r]
    after = None
    for r in range(chips - 1, -1, -1):
        q = crosses[r + 1] * after if r + 1 < chips else zero
        main = mains[r] - crosses[r + 1] * q if r + 1 < chips else mains[r]
        after = 1.0 / main
        comp[2, r] = q
        comp[3, r] = main

    parity = lax.rem(z, 2)
    first_unit = (z // 2) * 3 + parity * (2 - core)
    has = [None, parity == core]
    for j in range(2):
        m = group_masks(2 * core + jnp.minimum(first_unit + j, HALF - 1) // 6)
        for i in range(2):
            for r in range(chips):
                ucoef[j, i, r] = pick([one(comp.at[i, r], o) for o in range(4)], m)

    third = lax.rem(sub, 3)
    m_first = jnp.where(jnp.logical_and(third == 0, sub < 6), 0.25, 0.0).astype(f32)
    m_third = jnp.where(jnp.logical_and(third == 2, sub < 6), 0.25, 0.0).astype(f32)
    edge_line = (0, LINES - 1)
    pair_edge = remote(esum.at[1 - core], epart, pair_send.at[2], pair_recv.at[2], partner)

    def halo_sums():
        for copy in halo:
            copy.wait_recv()
        for e in range(2):
            sign = 1.0 if e == 0 else -1.0
            line = edge_line[e]
            sum_a = [zero, zero]
            sum_b = [zero, zero]
            for k in range(levels):
                r = 8 + 6 * k
                here = hrecv[e, r:r + 8, :]
                above = hrecv[e, r + 2:r + 10, :]
                below = hrecv[e, r - 2:r + 6, :]
                d = jnp.where(sub < 3, one(dbuf.at[k, 0], line), one(dbuf.at[k, 1], line))
                change = d * here + sign * (m_first * above + m_third * below)
                delta[e, k] = change
                sum_a[k % 2] = sum_a[k % 2] + one(high.at[k], line) * change
                sum_b[k % 2] = sum_b[k % 2] + one(low.at[k], line) * change
            esum[e, 0:8, :] = sum_a[0] + sum_a[1]
            esum[e, 8:16, :] = sum_b[0] + sum_b[1]
        pair_edge.start()

    @pl.when(me_h != 0)
    def _():
        halo_sums()

    def answer(j, n, zz):
        return remote(m2.at[j, zz], got.at[first_unit + j], s2_sem.at[j, n], r2_sem.at[first_unit + j],
                      same_core(zz))

    def solve_unit(j):
        for step in steps:
            zz = chip_at(step)
            remote(chip_rows.at[0], r1.at[j, zz], s1_sem.at[0], r1_sem.at[j, zz], same_core(zz)).wait_recv()
        values = []
        for r in range(chips):
            t = r1[j, r, 0:8, :]
            if r + 1 < chips:
                t = t + r1[j, r + 1, 8:16, :]
            values.append(t if r == 0 else t + ucoef[j, 0, r] * values[r - 1])
        s = values[chips - 1] * ucoef[j, 1, chips - 1]
        for r in range(chips - 1, -1, -1):
            m2[j, r, 8:16, :] = s
            if r + 1 < chips:
                m2[j, r + 1, 0:8, :] = s
            if r > 0:
                s = values[r - 1] * ucoef[j, 1, r - 1] + ucoef[j, 0, r] * s
        m2[j, 0, 0:8, :] = zero
        for n, step in enumerate(steps):
            answer(j, n, chip_at(step)).start()
        got[first_unit + j] = m2[j, z]

    solve_unit(0)

    @pl.when(has[1])
    def _():
        solve_unit(1)

    @pl.when(me_h == 0)
    def _():
        halo_sums()

    edge_off = offv[core * (LINES - 1)]
    z_low = jnp.maximum(z - 1, 0)

    def edge_comp(i, r):
        return jnp.broadcast_to(comp[i, r, pl.ds(edge_off, 1), :], (8, 128))

    def edge_local(i):
        return jnp.broadcast_to(lcoef[i, pl.ds(edge_off, 1), :], (8, 128))

    pair_edge.wait_recv()
    a_mine, b_mine = esum[core, 0:8, :], esum[core, 8:16, :]
    a_other, b_other = epart[0:8, :], epart[8:16, :]
    edge_t = jnp.where(on_low, a_mine, a_other) + jnp.where(on_low, b_other, b_mine)
    edge_a = jnp.where(on_low, a_other, a_mine) + edge_local(1) * edge_t
    edge_b = jnp.where(on_low, b_mine, b_other) + edge_local(0) * edge_t
    em[0] = edge_a + edge_comp(0, z) * edge_b
    em[1] = edge_b + edge_comp(2, z_low) * edge_a

    def edge_copy(n, zz):
        return remote(em.at[jnp.where(zz > z, 0, 1)], er.at[z], es_sem.at[n], er_sem.at[z], same_core(zz))

    for n, step in enumerate(steps):
        edge_copy(n, chip_at(step)).start()

    sol2 = sol.reshape(levels * 6 * LINES, 128)
    for e in range(2):
        line = edge_line[e]
        prev = delta[e, 0]
        for k in range(1, levels - 1):
            prev = delta[e, k] + one(wv.at[k], line) * prev
            delta[e, k] = prev
        x = zero
        for k in range(levels - 2, -1, -1):
            x = one(iv.at[k], line) * delta[e, k] + one(wv.at[k + 1], line) * x
            rows = pl.ds(k * 6 * LINES + line, 6, stride=LINES)
            sol2[rows, :] = sol2[rows, :] + x[0:6, :]

    for step in steps:
        zz = chip_at(step)
        remote(em.at[0], er.at[zz], es_sem.at[0], er_sem.at[zz], same_core(zz)).wait_recv()
    v = zero
    w = zero
    for r in range(chips):
        v = jnp.where(r < z, er[r] + edge_comp(0, r) * v, v)
    for r in range(chips - 1, 0, -1):
        w = jnp.where(r > z, er[r] + edge_comp(2, r - 1) * w, w)
    v = v + edge_b
    w = w + edge_a
    q_here = edge_comp(0, z)
    u_here = edge_comp(4, z)
    edge_high = (w + q_here * v) / (edge_comp(3, z) - u_here * q_here)
    edge_low = jnp.where(z > 0, (v + u_here * edge_high) * edge_comp(1, z_low), 0.0)

    for i in range(HALF):
        @pl.when(w_solver(i, core) != z)
        def _():
            remote(m2.at[0, 0], got.at[i], s2_sem.at[0, 0], r2_sem.at[i], same_core(w_solver(i, core))).wait_recv()
    got2 = got.reshape((HALF + 2) * 16, 128)
    middle2 = middle.reshape((HALF + 2) * 8, 128)
    for e in range(2):
        @pl.when(core == e)
        def _():
            for ref, size, at, add in (
                    (got2, 16, 0, edge_low), (got2, 16, 8, edge_high), (middle2, 8, 0, edge_t)):
                rows = pl.ds(6 * e * size + at + 7 * e, 6, stride=size)
                ref[rows, :] = ref[rows, :] + add[0:6, :]
    for i in range(HALF):
        low_k, high_k, pivot_k = own[i // 6]
        s_low, s_high = got[i, 0:8, :], got[i, 8:16, :]
        s_mid = middle[i] * pivot_k + low_k * s_low + high_k * s_high
        back[core * HALF + i, 0:8, :] = jnp.where(on_low, s_low, s_mid)
        back[core * HALF + i, 8:16, :] = jnp.where(on_low, s_mid, s_high)
        pass_on[i, 0:8, :] = jnp.where(on_low, s_mid, s_low)
        pass_on[i, 8:16, :] = jnp.where(on_low, s_high, s_mid)
    pair_ends = remote(pass_on, back.at[pl.ds(core * HALF, HALF)], pair_send.at[3], pair_recv.at[3], partner)
    pair_ends.start()

    for copy in (*halo, pair_coef, pair_rows, pair_edge):
        copy.wait_send()
    for n, step in enumerate(steps):
        coef_copy(n, chip_at(step)).wait_send()
        edge_copy(n, chip_at(step)).wait_send()
        answer(0, n, chip_at(step)).wait_send()
    for n, zz, j, unit in targets():
        @pl.when(zz != z)
        def _():
            target_copy(n, zz, j, unit).wait_send()

    @pl.when(has[1])
    def _():
        for n, step in enumerate(steps):
            answer(1, n, chip_at(step)).wait_send()
    pair_ends.wait()


def w_solver(i, core):
    return (i // 3) * 2 + (i % 3 + core) // 2


def assemble_kernel(sol, back, low, high, out, stage, sem):
    levels = sol.shape[0]
    per = levels // CHUNKS

    def copies(c):
        lev = pl.ds(c * per, per)
        return [
            pltpu.make_async_copy(
                stage.at[lev, h * 3 + f], out.at[f, lev, :, pl.ds(h * 128, 128)], sem.at[c, h * 3 + f])
            for h in range(2) for f in range(3)
        ]

    def chunk(c, carry):
        for g in range(GROUPS):
            rows = slice(8 * g, 8 * g + 8)
            prev = [back[g * 6 + q, 0:8, :] for q in range(6)]
            here = [back[g * 6 + q, 8:16, :] for q in range(6)]
            for l in range(per):
                k = c * per + l
                lo = low[k, rows, :]
                hi = high[k, rows, :]
                for q in range(6):
                    stage[k, q, rows, :] = sol[k, q, rows, :] + (lo * prev[q] + hi * here[q])
        for copy in copies(c):
            copy.start()
        return carry

    lax.fori_loop(0, CHUNKS, chunk, 0)
    for c in range(CHUNKS):
        for copy in copies(c):
            copy.wait()


def body(n_h, n_d, fields, diffusivity, offsets, coupling, inverse):
    f32 = jnp.float32
    levels = fields.shape[1]
    chips = n_d // 2
    hbm_spec = pl.BlockSpec(memory_space=pltpu.HBM)
    vmem_spec = pl.BlockSpec(memory_space=pltpu.VMEM)
    V = lambda *shape: pltpu.VMEM(shape, f32)
    dma = lambda *shape: pltpu.SemaphoreType.DMA(shape)
    sol, back, low, high = pl.pallas_call(
        functools.partial(columns_kernel, n_h, n_d),
        out_shape=(
            V(levels, 6, LINES, 128),
            V(UNITS, 16, 128),
            V(levels, LINES, 128),
            V(levels, LINES, 128),
        ),
        in_specs=[hbm_spec] * 5,
        out_specs=(vmem_spec,) * 4,
        scratch_shapes=[
            V(levels, 6, PAD, 128),
            V(levels, 2, LINES, 128),
            pltpu.SMEM((LINES,), jnp.int32),
            V(4, levels),
            V(4, levels, levels),
            pltpu.VMEM((GROUPS, 8, 128), jnp.int32),
            V(levels, LINES, 128),
            V(levels, LINES, 128),
            V(2, levels, 8, 128),
            V(2, levels * 6, 128),
            V(2, levels * 6 + 16, 128),
            V(8, 128),
            V(8, 128),
            V(8, 128),
            V(chips, 8, 128),
            V(UNITS, 16, 128),
            V(HALF, 16, 128),
            V(HALF, 16, 128),
            V(HALF + 2, 8, 128),
            V(2, chips, 16, 128),
            V(2, chips, 16, 128),
            V(HALF + 2, 16, 128),
            V(HALF, 16, 128),
            V(2, 16, 128),
            V(16, 128),
            V(2, 8, 128),
            V(chips, 8, 128),
            V(5, chips, 8, 128),
            V(2, 2, chips, 8, 128),
            V(3, 8, 128),
            dma(2, 6),
            dma(CHUNKS, 8),
            dma(3),
            dma(2),
            dma(2),
            dma(4),
            dma(4),
            dma(chips),
            dma(chips),
            dma(HALF),
            dma(2, chips),
            dma(2, chips),
            dma(HALF),
            dma(chips),
            dma(chips),
            pltpu.SemaphoreType.REGULAR((2,)),
        ],
        compiler_params=pltpu.CompilerParams(
            collective_id=0, has_side_effects=True, vmem_limit_bytes=48 * 1024 * 1024),
        name="columns",
    )(*(pltpu.with_memory_space_constraint(x, pltpu.HBM)
        for x in (fields, diffusivity, offsets, coupling, inverse)))
    return pl.pallas_call(
        assemble_kernel,
        out_shape=jax.ShapeDtypeStruct(fields.shape, f32),
        in_specs=[vmem_spec] * 4,
        out_specs=hbm_spec,
        scratch_shapes=[
            V(levels, 6, LINES, 128),
            dma(CHUNKS, 6),
        ],
        compiler_params=pltpu.CompilerParams(vmem_limit_bytes=48 * 1024 * 1024),
        name="assemble",
    )(sol, back, low, high)


def solution(mesh):
    return jax.shard_map(
        functools.partial(body, mesh.shape["horiz"], mesh.shape["depth"]),
        mesh=mesh,
        in_specs=(
            P(None, "depth", "horiz", None),
            P("depth", "horiz", None),
            P("horiz"),
            P(None, "depth"),
            P(None, "depth", None),
        ),
        out_specs=P(None, "depth", "horiz", None),
        check_vma=False,
    )
```

```python
import functools

import jax
import jax.numpy as jnp
from jax import lax
from jax.experimental import pallas as pl
from jax.experimental.pallas import tpu as pltpu
from jax.sharding import PartitionSpec as P

MESH = pl.DeviceIdType.MESH
CHUNKS = 4
PAD = 48
LINES = 32
GROUPS = LINES // 8
UNITS = GROUPS * 6
HALF = UNITS // 2


def far_first(chips):
    return sorted(range(1, chips), key=lambda s: -min(s, chips - s))


def columns_kernel(
    n_h, n_d,
    fields, diff, offs, coup, inv,
    sol, back, low, high,
    fbuf, dbuf, offv, cvec, kvec, offl, wv, iv, delta,
    hsend, hrecv, cmsg, cpart, chip, crecv, m1, other, chip_rows, middle, r1, m2, got, pass_on,
    esum, epart, em, er, comp, ucoef, lcoef, ends,
    edge_sem, load_sem, small_sem, hs_sem, hr_sem, pair_send, pair_recv, cs_sem, cr_sem,
    s1_sem, r1_sem, s2_sem, r2_sem, es_sem, er_sem, gate,
):
    f32 = jnp.float32
    levels = fields.shape[1]
    per = levels // CHUNKS
    me_h = lax.axis_index("horiz")
    me = lax.axis_index("depth")
    east = lax.rem(me_h + 1, n_h)
    west = lax.rem(me_h + n_h - 1, n_h)
    z, core = me // 2, lax.rem(me, 2)
    chips = n_d // 2
    steps = far_first(chips)
    on_low = core == 0

    def chip_at(step):
        return lax.rem(z + step, chips)

    def same_core(zz):
        return (me_h, zz * 2 + core)

    partner = (me_h, z * 2 + 1 - core)

    def remote(src, dst, send, recv, to):
        return pltpu.make_async_remote_copy(
            src_ref=src, dst_ref=dst, send_sem=send, recv_sem=recv, device_id=to, device_id_type=MESH)

    barrier = pltpu.get_barrier_semaphore()
    meets = [(east, z * 2), (west, z * 2), partner] + [(me_h, chip_at(step) * 2 + 1) for step in steps]
    for to in meets:
        pl.semaphore_signal(barrier, inc=1, device_id=to, device_id_type=MESH)

    small = [
        pltpu.make_async_copy(offs, offv, small_sem.at[0]),
        pltpu.make_async_copy(coup, cvec, small_sem.at[1]),
        pltpu.make_async_copy(inv, kvec, small_sem.at[2]),
    ]
    outer = []
    for i, first in enumerate((0, LINES - 8)):
        for h in range(2):
            for f in range(3):
                outer.append(pltpu.make_async_copy(
                    fields.at[f, :, pl.ds(first, 8), pl.ds(h * 128, 128)],
                    fbuf.at[:, h * 3 + f, pl.ds(8 + first, 8), :],
                    edge_sem.at[i, h * 3 + f]))

    def chunk_copies(c):
        lev = pl.ds(c * per, per)
        out = []
        for h in range(2):
            lane = pl.ds(h * 128, 128)
            for f in range(3):
                out.append(pltpu.make_async_copy(
                    fields.at[f, lev, pl.ds(8, LINES - 16), lane],
                    fbuf.at[lev, h * 3 + f, pl.ds(16, LINES - 16), :],
                    load_sem.at[c, h * 3 + f]))
            out.append(pltpu.make_async_copy(
                diff.at[lev, :, lane], dbuf.at[lev, h], load_sem.at[c, 6 + h]))
        return out

    for copy in small + outer:
        copy.start()
    for c in range(CHUNKS):
        for copy in chunk_copies(c):
            copy.start()

    f2 = fbuf.reshape(levels * 6 * PAD, 128)
    f2[pl.ds(7, levels * 6, stride=PAD), :] = jnp.zeros((levels * 6, 128), f32)
    f2[pl.ds(40, levels * 6, stride=PAD), :] = jnp.zeros((levels * 6, 128), f32)
    for e in range(2):
        hrecv[e, 0:8, :] = jnp.zeros((8, 128), f32)
        hrecv[e, 200:208, :] = jnp.zeros((8, 128), f32)
    m1[...] = jnp.zeros(m1.shape, f32)

    def pack():
        for copy in outer:
            copy.wait()
        hsend[0] = f2[pl.ds(39, levels * 6, stride=PAD), :]
        hsend[1] = f2[pl.ds(8, levels * 6, stride=PAD), :]

    halo = [
        remote(hsend.at[e], hrecv.at[e, pl.ds(8, levels * 6), :], hs_sem.at[e], hr_sem.at[e], (to, me))
        for e, to in ((0, east), (1, west))
    ]

    waits_late = me_h == 0

    def send_halo():
        @pl.when(core == 0)
        def _():
            pl.semaphore_wait(barrier, 5)
            pl.semaphore_signal(gate.at[1], inc=1, device_id=partner, device_id_type=MESH)

        @pl.when(core == 1)
        def _():
            pl.semaphore_wait(gate.at[1], 1)

        for copy in halo:
            copy.start()

    @pl.when(me_h == n_h - 1)
    def _():
        pack()
        send_halo()

    for copy in small:
        copy.wait()
    sub = lax.broadcasted_iota(jnp.int32, (8, 128), 0)
    lane = lax.broadcasted_iota(jnp.int32, (8, 128), 1)
    masks = []
    for g in range(GROUPS):
        v = jnp.full((8, 128), offv[8 * g], jnp.int32)
        for i in range(1, 8):
            v = jnp.where(sub == i, offv[8 * g + i], v)
        offl[g] = v
        masks.append([v == o for o in range(3)])

    def widen(x):
        return jnp.concatenate([x, jnp.zeros((4, 128 - levels), f32)], axis=1)

    couple = cvec[...]
    first_row = kvec[:, 0, :]
    last_row = kvec[:, levels - 2, :]
    c_low = couple[:, 0:1]
    c_high = couple[:, levels - 1:levels]
    inside = jnp.where(me > 0, 1.0, 0.0).astype(f32)
    table_low = first_row * (jnp.broadcast_to(c_low, (4, levels)) * inside)
    table_high = last_row * jnp.broadcast_to(c_high, (4, levels))
    lane4 = lax.broadcasted_iota(jnp.int32, (4, 128), 1)

    def pick(rows, m):
        return jnp.where(m[0], rows[0], jnp.where(m[1], rows[1], jnp.where(m[2], rows[2], rows[3])))

    def by_line(table):
        rows = [jnp.broadcast_to(table[o:o + 1, :], (8, 128)) for o in range(4)]
        return [pick(rows, masks[g]) for g in range(GROUPS)]

    def fill(ref, table, count):
        lines = by_line(table)
        for k in range(count):
            for g in range(GROUPS):
                ref[k, 8 * g:8 * g + 8, :] = jnp.broadcast_to(lines[g][:, k:k + 1], (8, 128))

    wide_high = widen(table_high)
    fill(low, jnp.where(lane4 == levels - 1, 0.0, widen(table_low)), levels)
    fill(high, jnp.where(lane4 == levels - 1, 1.0, wide_high), levels)

    c_low4 = jnp.broadcast_to(c_low, (4, 128))
    c_high4 = jnp.broadcast_to(c_high, (4, 128))
    alpha = c_high4 - c_high4 * jnp.broadcast_to(table_high[:, levels - 2:levels - 1], (4, 128))
    beta = c_low4 - c_low4 * jnp.broadcast_to(table_low[:, 0:1], (4, 128))
    cross = c_high4 * jnp.broadcast_to(table_low[:, levels - 2:levels - 1], (4, 128))
    packed = jnp.where(lane4 < 32, alpha, jnp.where(lane4 < 64, beta, cross))
    cmsg[0:4, :] = packed
    cmsg[4:8, :] = packed

    @pl.when(me_h != n_h - 1)
    def _():
        pack()

    @pl.when(jnp.logical_and(me_h != n_h - 1, jnp.logical_not(waits_late)))
    def _():
        send_halo()

    is_last = lane == 127
    is_first = lane == 0

    def forcing(c, g):
        r0 = 8 + 8 * g
        rows = slice(8 * g, 8 * g + 8)
        sums = [m1[g * 6 + q, 8 * w:8 * w + 8, :] for w in range(2) for q in range(6)]
        for l in range(per):
            k = c * per + l
            hi = high[k, rows, :]
            lo = low[k, rows, :]
            mid = [fbuf[k, q, r0:r0 + 8, :] for q in range(6)]
            es = [fbuf[k, q, r0 + 1:r0 + 9, :] for q in range(6)]
            ws = [fbuf[k, q, r0 - 1:r0 + 7, :] for q in range(6)]
            up = [pltpu.roll(mid[q], 127, 1) for q in range(6)]
            dn = [pltpu.roll(mid[q], 1, 1) for q in range(6)]
            for h in range(2):
                d = dbuf[k, h, rows, :]
                keep = 1.0 - 4.0 * d
                q = [h * 3 + f for f in range(3)]
                qo = [(1 - h) * 3 + f for f in range(3)]
                north = [jnp.where(is_last, up[qo[f]], up[q[f]]) for f in range(3)]
                south = [jnp.where(is_first, dn[qo[f]], dn[q[f]]) for f in range(3)]
                base = [
                    mid[q[f]] * keep + d * ((es[q[f]] + ws[q[f]]) + (north[f] + south[f]))
                    for f in range(3)
                ]
                out = [
                    base[0] - 0.25 * (es[q[2]] - ws[q[2]]),
                    base[1] - 0.25 * (north[2] - south[2]),
                    base[2] - 0.25 * ((es[q[0]] - ws[q[0]]) + (north[1] - south[1])),
                ]
                for f in range(3):
                    sol[k, q[f], rows, :] = out[f]
                    sums[q[f]] = sums[q[f]] + hi * out[f]
                    sums[6 + q[f]] = sums[6 + q[f]] + lo * out[f]
        for w in range(2):
            for q in range(6):
                m1[g * 6 + q, 8 * w:8 * w + 8, :] = sums[w * 6 + q]

    def slot_forcing(slot, first):
        def step_chunk(c, carry):
            if first:
                for copy in chunk_copies(c):
                    copy.wait()
            for g in range(2 * slot, 2 * slot + 2):
                forcing(c, g)
            return carry

        lax.fori_loop(0, CHUNKS, step_chunk, 0)

    for slot in range(2):
        @pl.when(core == 1 - slot)
        def _():
            slot_forcing(slot, True)

    pair_coef = remote(cmsg, cpart, pair_send.at[0], pair_recv.at[0], partner)
    pair_rows = remote(m1.at[pl.ds((1 - core) * HALF, HALF)], other, pair_send.at[1], pair_recv.at[1], partner)

    @pl.when(core == 1)
    def _():
        pl.semaphore_wait(barrier, 2 * len(steps) + 1)
        pl.semaphore_signal(gate.at[0], inc=1, device_id=partner, device_id_type=MESH)

    @pl.when(core == 0)
    def _():
        pl.semaphore_wait(gate.at[0], 1)

    for copy in (pair_coef, pair_rows):
        copy.start()
    for slot in range(2):
        @pl.when(core == slot)
        def _():
            slot_forcing(slot, False)

    def splat(tile, at):
        return jnp.broadcast_to(tile[:, at:at + 1], (8, 128))

    pair_coef.wait_recv()
    mine, theirs = cmsg[...], cpart[...]
    tile0 = jnp.where(on_low, mine, theirs)
    tile1 = jnp.where(on_low, theirs, mine)
    alpha0, beta0, cross0 = (splat(tile0, at) for at in (0, 32, 64))
    alpha1, beta1, cross1 = (splat(tile1, at) for at in (0, 32, 64))
    mid_pivot = 1.0 / (1.0 + alpha0 + beta1)
    to_low = cross0 * mid_pivot
    to_high = cross1 * mid_pivot
    chip[...] = jnp.where(
        lane < 32, alpha1 - cross1 * to_high,
        jnp.where(lane < 64, beta0 - cross0 * to_low, cross0 * to_high))
    lcoef[0] = to_low
    lcoef[1] = to_high
    lcoef[2] = mid_pivot

    def coef_copy(j, zz):
        return remote(chip, crecv.at[z], cs_sem.at[j], cr_sem.at[z], same_core(zz))

    for j, step in enumerate(steps):
        coef_copy(j, chip_at(step)).start()

    def one(ref, line):
        return jnp.broadcast_to(ref[line:line + 1, :], (8, 128))

    def group_masks(g):
        v = offl[g]
        return [v == o for o in range(3)]

    own_masks = [group_masks(2 * core + gg) for gg in range(2)]
    own = [
        [pick([one(lcoef.at[i], o) for o in range(4)], own_masks[gg]) for i in range(3)]
        for gg in range(2)
    ]
    pair_rows.wait_recv()
    for i in range(HALF):
        low_k, high_k, _ = own[i // 6]
        a_mine, b_mine = m1[core * HALF + i, 0:8, :], m1[core * HALF + i, 8:16, :]
        a_other, b_other = other[i, 0:8, :], other[i, 8:16, :]
        t = jnp.where(on_low, a_mine, a_other) + jnp.where(on_low, b_other, b_mine)
        middle[i] = t
        chip_rows[i, 0:8, :] = jnp.where(on_low, a_other, a_mine) + high_k * t
        chip_rows[i, 8:16, :] = jnp.where(on_low, b_mine, b_other) + low_k * t

    def solver_of(i, w, m):
        b = (m + core) // 2
        return w * 2 + b, m - b * (2 - core)

    def targets():
        for n, dw in enumerate((2, 1, 3, 0)):
            w = lax.rem(z // 2 + dw, chips // 2)
            for m in range(3):
                zz, j = solver_of(None, w, m)
                yield n * 3 + m, zz, j, w * 3 + m

    def target_copy(n, zz, j, unit):
        return remote(chip_rows.at[unit], r1.at[j, z], s1_sem.at[n], r1_sem.at[j, z], same_core(zz))

    for n, zz, j, unit in targets():
        @pl.when(zz != z)
        def _():
            target_copy(n, zz, j, unit).start()

        @pl.when(zz == z)
        def _():
            r1[j, z] = chip_rows[unit]

    @pl.when(waits_late)
    def _():
        send_halo()

    shift_high = pltpu.roll(wide_high, 1, 1)
    inner = jnp.logical_and(lane4 > 0, lane4 < levels - 1)
    ratio = jnp.where(inner, shift_high / jnp.where(inner, wide_high, 1.0), 0.0)
    inner_c = jnp.where(inner, widen(couple), 1.0)
    pivot = pltpu.roll(ratio / inner_c, 127, 1)
    pivot = jnp.where(lane4 == levels - 2, widen(last_row), pivot)
    fill(wv, ratio, levels)
    fill(iv, pivot, levels - 1)

    def down(k, carry):
        out = []
        for g in range(GROUPS):
            rows = slice(8 * g, 8 * g + 8)
            w = wv[k, rows, :]
            for q in range(6):
                y = sol[k, q, rows, :] + w * carry[g * 6 + q]
                sol[k, q, rows, :] = y
                out.append(y)
        return tuple(out)

    def rise(i, carry):
        k = levels - 2 - i
        out = []
        for g in range(GROUPS):
            rows = slice(8 * g, 8 * g + 8)
            piv = iv[k, rows, :]
            w = wv[k + 1, rows, :]
            for q in range(6):
                x = piv * sol[k, q, rows, :] + w * carry[g * 6 + q]
                sol[k, q, rows, :] = x
                out.append(x)
        return tuple(out)

    zero = jnp.zeros((8, 128), f32)
    lax.fori_loop(1, levels - 1, down,
                  tuple(sol[0, q, 8 * g:8 * g + 8, :] for g in range(GROUPS) for q in range(6)))
    lax.fori_loop(0, levels - 1, rise, (zero,) * UNITS)
    for q in range(6):
        sol[levels - 1, q] = jnp.zeros((LINES, 128), f32)

    third = lax.rem(sub, 3)
    m_first = jnp.where(jnp.logical_and(third == 0, sub < 6), 0.25, 0.0).astype(f32)
    m_third = jnp.where(jnp.logical_and(third == 2, sub < 6), 0.25, 0.0).astype(f32)
    edge_line = (0, LINES - 1)
    pair_edge = remote(esum.at[1 - core], epart, pair_send.at[2], pair_recv.at[2], partner)

    def halo_sums():
        for copy in halo:
            copy.wait_recv()
        for e in range(2):
            sign = 1.0 if e == 0 else -1.0
            line = edge_line[e]
            sum_a = [zero, zero]
            sum_b = [zero, zero]
            for k in range(levels):
                r = 8 + 6 * k
                here = hrecv[e, r:r + 8, :]
                above = hrecv[e, r + 2:r + 10, :]
                below = hrecv[e, r - 2:r + 6, :]
                d = jnp.where(sub < 3, one(dbuf.at[k, 0], line), one(dbuf.at[k, 1], line))
                change = d * here + sign * (m_first * above + m_third * below)
                delta[e, k] = change
                sum_a[k % 2] = sum_a[k % 2] + one(high.at[k], line) * change
                sum_b[k % 2] = sum_b[k % 2] + one(low.at[k], line) * change
            esum[e, 0:8, :] = sum_a[0] + sum_a[1]
            esum[e, 8:16, :] = sum_b[0] + sum_b[1]
        pair_edge.start()

    @pl.when(me_h > 1)
    def _():
        halo_sums()

    crecv[z] = chip[...]
    for step in steps:
        zz = chip_at(step)
        remote(chip, crecv.at[zz], cs_sem.at[0], cr_sem.at[zz], same_core(zz)).wait_recv()
    alphas, betas, crosses = [], [], []
    for r in range(chips):
        tile = crecv[r]
        alphas.append(splat(tile, 0))
        betas.append(splat(tile, 32))
        crosses.append(splat(tile, 64))
    mains = [1.0 + alphas[r] + (betas[r + 1] if r + 1 < chips else 0.0) for r in range(chips)]
    before = None
    for r in range(chips):
        q = crosses[r] * before if r > 0 else zero
        main = mains[r] - crosses[r] * q if r > 0 else mains[r]
        before = 1.0 / main
        comp[0, r] = q
        comp[1, r] = before
        comp[4, r] = crosses[r]
    after = None
    for r in range(chips - 1, -1, -1):
        q = crosses[r + 1] * after if r + 1 < chips else zero
        main = mains[r] - crosses[r + 1] * q if r + 1 < chips else mains[r]
        after = 1.0 / main
        comp[2, r] = q
        comp[3, r] = main

    parity = lax.rem(z, 2)
    first_unit = (z // 2) * 3 + parity * (2 - core)
    has = [None, parity == core]
    for j in range(2):
        m = group_masks(2 * core + jnp.minimum(first_unit + j, HALF - 1) // 6)
        for i in range(2):
            for r in range(chips):
                ucoef[j, i, r] = pick([one(comp.at[i, r], o) for o in range(4)], m)

    edge_off = offv[core * (LINES - 1)]
    z_low = jnp.maximum(z - 1, 0)

    def edge_comp(i, r):
        return jnp.broadcast_to(comp[i, r, pl.ds(edge_off, 1), :], (8, 128))

    def edge_local(i):
        return jnp.broadcast_to(lcoef[i, pl.ds(edge_off, 1), :], (8, 128))

    def edge_copy(n, zz):
        return remote(em.at[jnp.where(zz > z, 0, 1)], er.at[z], es_sem.at[n], er_sem.at[z], same_core(zz))

    def edge_send():
        pair_edge.wait_recv()
        a_mine, b_mine = esum[core, 0:8, :], esum[core, 8:16, :]
        a_other, b_other = epart[0:8, :], epart[8:16, :]
        edge_t = jnp.where(on_low, a_mine, a_other) + jnp.where(on_low, b_other, b_mine)
        edge_a = jnp.where(on_low, a_other, a_mine) + edge_local(1) * edge_t
        edge_b = jnp.where(on_low, b_mine, b_other) + edge_local(0) * edge_t
        ends[0] = edge_t
        ends[1] = edge_a
        ends[2] = edge_b
        em[0] = edge_a + edge_comp(0, z) * edge_b
        em[1] = edge_b + edge_comp(2, z_low) * edge_a
        for n, step in enumerate(steps):
            edge_copy(n, chip_at(step)).start()

    @pl.when(me_h > 1)
    def _():
        edge_send()

    def answer(j, n, zz):
        return remote(m2.at[j, zz], got.at[first_unit + j], s2_sem.at[j, n], r2_sem.at[first_unit + j],
                      same_core(zz))

    def solve_unit(j):
        for step in steps:
            zz = chip_at(step)
            remote(chip_rows.at[0], r1.at[j, zz], s1_sem.at[0], r1_sem.at[j, zz], same_core(zz)).wait_recv()
        values = []
        for r in range(chips):
            t = r1[j, r, 0:8, :]
            if r + 1 < chips:
                t = t + r1[j, r + 1, 8:16, :]
            values.append(t if r == 0 else t + ucoef[j, 0, r] * values[r - 1])
        s = values[chips - 1] * ucoef[j, 1, chips - 1]
        for r in range(chips - 1, -1, -1):
            m2[j, r, 8:16, :] = s
            if r + 1 < chips:
                m2[j, r + 1, 0:8, :] = s
            if r > 0:
                s = values[r - 1] * ucoef[j, 1, r - 1] + ucoef[j, 0, r] * s
        m2[j, 0, 0:8, :] = zero
        for n, step in enumerate(steps):
            answer(j, n, chip_at(step)).start()
        got[first_unit + j] = m2[j, z]

    solve_unit(0)

    @pl.when(has[1])
    def _():
        solve_unit(1)

    @pl.when(me_h <= 1)
    def _():
        halo_sums()
        edge_send()

    sol2 = sol.reshape(levels * 6 * LINES, 128)
    for e in range(2):
        line = edge_line[e]
        prev = delta[e, 0]
        for k in range(1, levels - 1):
            prev = delta[e, k] + one(wv.at[k], line) * prev
            delta[e, k] = prev
        x = zero
        for k in range(levels - 2, -1, -1):
            x = one(iv.at[k], line) * delta[e, k] + one(wv.at[k + 1], line) * x
            rows = pl.ds(k * 6 * LINES + line, 6, stride=LINES)
            sol2[rows, :] = sol2[rows, :] + x[0:6, :]

    for step in steps:
        zz = chip_at(step)
        remote(em.at[0], er.at[zz], es_sem.at[0], er_sem.at[zz], same_core(zz)).wait_recv()
    v = zero
    w = zero
    for r in range(chips):
        v = jnp.where(r < z, er[r] + edge_comp(0, r) * v, v)
    for r in range(chips - 1, 0, -1):
        w = jnp.where(r > z, er[r] + edge_comp(2, r - 1) * w, w)
    edge_t = ends[0]
    v = v + ends[2]
    w = w + ends[1]
    q_here = edge_comp(0, z)
    u_here = edge_comp(4, z)
    edge_high = (w + q_here * v) / (edge_comp(3, z) - u_here * q_here)
    edge_low = jnp.where(z > 0, (v + u_here * edge_high) * edge_comp(1, z_low), 0.0)

    for i in range(HALF):
        @pl.when(w_solver(i, core) != z)
        def _():
            remote(m2.at[0, 0], got.at[i], s2_sem.at[0, 0], r2_sem.at[i], same_core(w_solver(i, core))).wait_recv()
    got2 = got.reshape((HALF + 2) * 16, 128)
    middle2 = middle.reshape((HALF + 2) * 8, 128)
    for e in range(2):
        @pl.when(core == e)
        def _():
            for ref, size, at, add in (
                    (got2, 16, 0, edge_low), (got2, 16, 8, edge_high), (middle2, 8, 0, edge_t)):
                rows = pl.ds(6 * e * size + at + 7 * e, 6, stride=size)
                ref[rows, :] = ref[rows, :] + add[0:6, :]
    for i in range(HALF):
        low_k, high_k, pivot_k = own[i // 6]
        s_low, s_high = got[i, 0:8, :], got[i, 8:16, :]
        s_mid = middle[i] * pivot_k + low_k * s_low + high_k * s_high
        back[core * HALF + i, 0:8, :] = jnp.where(on_low, s_low, s_mid)
        back[core * HALF + i, 8:16, :] = jnp.where(on_low, s_mid, s_high)
        pass_on[i, 0:8, :] = jnp.where(on_low, s_mid, s_low)
        pass_on[i, 8:16, :] = jnp.where(on_low, s_high, s_mid)
    pair_ends = remote(pass_on, back.at[pl.ds(core * HALF, HALF)], pair_send.at[3], pair_recv.at[3], partner)
    pair_ends.start()

    for copy in (*halo, pair_coef, pair_rows, pair_edge):
        copy.wait_send()
    for n, step in enumerate(steps):
        coef_copy(n, chip_at(step)).wait_send()
        edge_copy(n, chip_at(step)).wait_send()
        answer(0, n, chip_at(step)).wait_send()
    for n, zz, j, unit in targets():
        @pl.when(zz != z)
        def _():
            target_copy(n, zz, j, unit).wait_send()

    @pl.when(has[1])
    def _():
        for n, step in enumerate(steps):
            answer(1, n, chip_at(step)).wait_send()
    pair_ends.wait()


def w_solver(i, core):
    return (i // 3) * 2 + (i % 3 + core) // 2


def assemble_kernel(sol, back, low, high, out, stage, sem):
    levels = sol.shape[0]
    per = levels // CHUNKS

    def copies(c):
        lev = pl.ds(c * per, per)
        return [
            pltpu.make_async_copy(
                stage.at[f, lev], out.at[f, lev], sem.at[c, f])
            for f in range(3)
        ]

    def chunk(c, carry):
        for g in range(GROUPS):
            rows = slice(8 * g, 8 * g + 8)
            prev = [back[g * 6 + q, 0:8, :] for q in range(6)]
            here = [back[g * 6 + q, 8:16, :] for q in range(6)]
            for l in range(per):
                k = c * per + l
                lo = low[k, rows, :]
                hi = high[k, rows, :]
                for q in range(6):
                    h, f = q // 3, q % 3
                    stage[f, k, rows, 128 * h:128 * h + 128] = sol[k, q, rows, :] + (lo * prev[q] + hi * here[q])
        for copy in copies(c):
            copy.start()
        return carry

    lax.fori_loop(0, CHUNKS, chunk, 0)
    for c in range(CHUNKS):
        for copy in copies(c):
            copy.wait()


def body(n_h, n_d, fields, diffusivity, offsets, coupling, inverse):
    f32 = jnp.float32
    levels = fields.shape[1]
    chips = n_d // 2
    hbm_spec = pl.BlockSpec(memory_space=pltpu.HBM)
    vmem_spec = pl.BlockSpec(memory_space=pltpu.VMEM)
    V = lambda *shape: pltpu.VMEM(shape, f32)
    dma = lambda *shape: pltpu.SemaphoreType.DMA(shape)
    sol, back, low, high = pl.pallas_call(
        functools.partial(columns_kernel, n_h, n_d),
        out_shape=(
            V(levels, 6, LINES, 128),
            V(UNITS, 16, 128),
            V(levels, LINES, 128),
            V(levels, LINES, 128),
        ),
        in_specs=[hbm_spec] * 5,
        out_specs=(vmem_spec,) * 4,
        scratch_shapes=[
            V(levels, 6, PAD, 128),
            V(levels, 2, LINES, 128),
            pltpu.SMEM((LINES,), jnp.int32),
            V(4, levels),
            V(4, levels, levels),
            pltpu.VMEM((GROUPS, 8, 128), jnp.int32),
            V(levels, LINES, 128),
            V(levels, LINES, 128),
            V(2, levels, 8, 128),
            V(2, levels * 6, 128),
            V(2, levels * 6 + 16, 128),
            V(8, 128),
            V(8, 128),
            V(8, 128),
            V(chips, 8, 128),
            V(UNITS, 16, 128),
            V(HALF, 16, 128),
            V(HALF, 16, 128),
            V(HALF + 2, 8, 128),
            V(2, chips, 16, 128),
            V(2, chips, 16, 128),
            V(HALF + 2, 16, 128),
            V(HALF, 16, 128),
            V(2, 16, 128),
            V(16, 128),
            V(2, 8, 128),
            V(chips, 8, 128),
            V(5, chips, 8, 128),
            V(2, 2, chips, 8, 128),
            V(3, 8, 128),
            V(3, 8, 128),
            dma(2, 6),
            dma(CHUNKS, 8),
            dma(3),
            dma(2),
            dma(2),
            dma(4),
            dma(4),
            dma(chips),
            dma(chips),
            dma(HALF),
            dma(2, chips),
            dma(2, chips),
            dma(HALF),
            dma(chips),
            dma(chips),
            pltpu.SemaphoreType.REGULAR((2,)),
        ],
        compiler_params=pltpu.CompilerParams(
            collective_id=0, has_side_effects=True, vmem_limit_bytes=48 * 1024 * 1024),
        name="columns",
    )(*(pltpu.with_memory_space_constraint(x, pltpu.HBM)
        for x in (fields, diffusivity, offsets, coupling, inverse)))
    return pl.pallas_call(
        assemble_kernel,
        out_shape=jax.ShapeDtypeStruct(fields.shape, f32),
        in_specs=[vmem_spec] * 4,
        out_specs=hbm_spec,
        scratch_shapes=[
            V(3, levels, LINES, 256),
            dma(CHUNKS, 3),
        ],
        compiler_params=pltpu.CompilerParams(vmem_limit_bytes=48 * 1024 * 1024),
        name="assemble",
    )(sol, back, low, high)


def solution(mesh):
    return jax.shard_map(
        functools.partial(body, mesh.shape["horiz"], mesh.shape["depth"]),
        mesh=mesh,
        in_specs=(
            P(None, "depth", "horiz", None),
            P("depth", "horiz", None),
            P("horiz"),
            P(None, "depth"),
            P(None, "depth", None),
        ),
        out_specs=P(None, "depth", "horiz", None),
        check_vma=False,
    )
```

```python
import functools

import jax
import jax.numpy as jnp
from jax import lax
from jax.experimental import pallas as pl
from jax.experimental.pallas import tpu as pltpu
from jax.sharding import PartitionSpec as P

MESH = pl.DeviceIdType.MESH
CHUNKS = 4
PAD = 48
LINES = 32
GROUPS = LINES // 8
UNITS = GROUPS * 6
HALF = UNITS // 2


def far_first(chips):
    return sorted(range(1, chips), key=lambda s: -min(s, chips - s))


def columns_kernel(
    n_h, n_d,
    fields, diff, offs, coup, inv,
    sol, back, low, high,
    fbuf, dbuf, offv, cvec, kvec, offl, wv, iv, delta,
    hsend, hrecv, cmsg, cpart, chip, crecv, m1, other, chip_rows, middle, r1, m2, got, pass_on,
    esum, epart, em, er, comp, ucoef, lcoef, ends, edge_out, edge_in,
    edge_sem, load_sem, small_sem, hs_sem, hr_sem, pair_send, pair_recv, cs_sem, cr_sem,
    s1_sem, r1_sem, s2_sem, r2_sem, es_sem, er_sem, gate,
):
    f32 = jnp.float32
    levels = fields.shape[1]
    per = levels // CHUNKS
    me_h = lax.axis_index("horiz")
    me = lax.axis_index("depth")
    east = lax.rem(me_h + 1, n_h)
    west = lax.rem(me_h + n_h - 1, n_h)
    z, core = me // 2, lax.rem(me, 2)
    chips = n_d // 2
    steps = far_first(chips)
    on_low = core == 0

    def chip_at(step):
        return lax.rem(z + step, chips)

    def same_core(zz):
        return (me_h, zz * 2 + core)

    partner = (me_h, z * 2 + 1 - core)

    def remote(src, dst, send, recv, to):
        return pltpu.make_async_remote_copy(
            src_ref=src, dst_ref=dst, send_sem=send, recv_sem=recv, device_id=to, device_id_type=MESH)

    barrier = pltpu.get_barrier_semaphore()
    meets = [(east, z * 2), (west, z * 2), partner] + [(me_h, chip_at(step) * 2 + 1) for step in steps]
    for to in meets:
        pl.semaphore_signal(barrier, inc=1, device_id=to, device_id_type=MESH)

    small = [
        pltpu.make_async_copy(offs, offv, small_sem.at[0]),
        pltpu.make_async_copy(coup, cvec, small_sem.at[1]),
        pltpu.make_async_copy(inv, kvec, small_sem.at[2]),
    ]
    outer = []
    for i, first in enumerate((LINES - 8, 0)):
        for h in range(2):
            for f in range(3):
                outer.append(pltpu.make_async_copy(
                    fields.at[f, :, pl.ds(first, 8), pl.ds(h * 128, 128)],
                    fbuf.at[:, h * 3 + f, pl.ds(8 + first, 8), :],
                    edge_sem.at[i, h * 3 + f]))

    def chunk_copies(c):
        lev = pl.ds(c * per, per)
        out = []
        for h in range(2):
            lane = pl.ds(h * 128, 128)
            for f in range(3):
                out.append(pltpu.make_async_copy(
                    fields.at[f, lev, pl.ds(8, LINES - 16), lane],
                    fbuf.at[lev, h * 3 + f, pl.ds(16, LINES - 16), :],
                    load_sem.at[c, h * 3 + f]))
            out.append(pltpu.make_async_copy(
                diff.at[lev, :, lane], dbuf.at[lev, h], load_sem.at[c, 6 + h]))
        return out

    for copy in small + outer:
        copy.start()
    for c in range(CHUNKS):
        for copy in chunk_copies(c):
            copy.start()

    f2 = fbuf.reshape(levels * 6 * PAD, 128)
    f2[pl.ds(7, levels * 6, stride=PAD), :] = jnp.zeros((levels * 6, 128), f32)
    f2[pl.ds(40, levels * 6, stride=PAD), :] = jnp.zeros((levels * 6, 128), f32)
    for e in range(2):
        hrecv[e, 0:8, :] = jnp.zeros((8, 128), f32)
        hrecv[e, 200:208, :] = jnp.zeros((8, 128), f32)
    m1[...] = jnp.zeros(m1.shape, f32)

    def pack(e):
        for copy in outer[6 * e:6 * e + 6]:
            copy.wait()
        hsend[e] = f2[pl.ds(8 if e else 39, levels * 6, stride=PAD), :]

    halo = [
        remote(hsend.at[e], hrecv.at[e, pl.ds(8, levels * 6), :], hs_sem.at[e], hr_sem.at[e], (to, me))
        for e, to in ((0, east), (1, west))
    ]

    waits_late = me_h == 0

    def meet_neighbours():
        @pl.when(core == 0)
        def _():
            pl.semaphore_wait(barrier, 5)
            pl.semaphore_signal(gate.at[1], inc=1, device_id=partner, device_id_type=MESH)

        @pl.when(core == 1)
        def _():
            pl.semaphore_wait(gate.at[1], 1)

    @pl.when(me_h == n_h - 1)
    def _():
        meet_neighbours()
        for e in range(2):
            pack(e)
            halo[e].start()

    for copy in small:
        copy.wait()
    sub = lax.broadcasted_iota(jnp.int32, (8, 128), 0)
    lane = lax.broadcasted_iota(jnp.int32, (8, 128), 1)
    masks = []
    for g in range(GROUPS):
        v = jnp.full((8, 128), offv[8 * g], jnp.int32)
        for i in range(1, 8):
            v = jnp.where(sub == i, offv[8 * g + i], v)
        offl[g] = v
        masks.append([v == o for o in range(3)])

    def widen(x):
        return jnp.concatenate([x, jnp.zeros((4, 128 - levels), f32)], axis=1)

    couple = cvec[...]
    first_row = kvec[:, 0, :]
    last_row = kvec[:, levels - 2, :]
    c_low = couple[:, 0:1]
    c_high = couple[:, levels - 1:levels]
    inside = jnp.where(me > 0, 1.0, 0.0).astype(f32)
    table_low = first_row * (jnp.broadcast_to(c_low, (4, levels)) * inside)
    table_high = last_row * jnp.broadcast_to(c_high, (4, levels))
    lane4 = lax.broadcasted_iota(jnp.int32, (4, 128), 1)

    def pick(rows, m):
        return jnp.where(m[0], rows[0], jnp.where(m[1], rows[1], jnp.where(m[2], rows[2], rows[3])))

    def by_line(table):
        rows = [jnp.broadcast_to(table[o:o + 1, :], (8, 128)) for o in range(4)]
        return [pick(rows, masks[g]) for g in range(GROUPS)]

    def fill(ref, table, count):
        lines = by_line(table)
        for k in range(count):
            for g in range(GROUPS):
                ref[k, 8 * g:8 * g + 8, :] = jnp.broadcast_to(lines[g][:, k:k + 1], (8, 128))

    wide_high = widen(table_high)
    fill(low, jnp.where(lane4 == levels - 1, 0.0, widen(table_low)), levels)
    fill(high, jnp.where(lane4 == levels - 1, 1.0, wide_high), levels)

    c_low4 = jnp.broadcast_to(c_low, (4, 128))
    c_high4 = jnp.broadcast_to(c_high, (4, 128))
    alpha = c_high4 - c_high4 * jnp.broadcast_to(table_high[:, levels - 2:levels - 1], (4, 128))
    beta = c_low4 - c_low4 * jnp.broadcast_to(table_low[:, 0:1], (4, 128))
    cross = c_high4 * jnp.broadcast_to(table_low[:, levels - 2:levels - 1], (4, 128))
    packed = jnp.where(lane4 < 32, alpha, jnp.where(lane4 < 64, beta, cross))
    cmsg[0:4, :] = packed
    cmsg[4:8, :] = packed

    @pl.when(me_h != n_h - 1)
    def _():
        for e in range(2):
            pack(e)

    def send_halo():
        meet_neighbours()
        for copy in halo:
            copy.start()

    @pl.when(jnp.logical_and(me_h != n_h - 1, jnp.logical_not(waits_late)))
    def _():
        send_halo()

    is_last = lane == 127
    is_first = lane == 0

    def forcing(c, g):
        r0 = 8 + 8 * g
        rows = slice(8 * g, 8 * g + 8)
        sums = [m1[g * 6 + q, 8 * w:8 * w + 8, :] for w in range(2) for q in range(6)]
        for l in range(per):
            k = c * per + l
            hi = high[k, rows, :]
            lo = low[k, rows, :]
            mid = [fbuf[k, q, r0:r0 + 8, :] for q in range(6)]
            es = [fbuf[k, q, r0 + 1:r0 + 9, :] for q in range(6)]
            ws = [fbuf[k, q, r0 - 1:r0 + 7, :] for q in range(6)]
            up = [pltpu.roll(mid[q], 127, 1) for q in range(6)]
            dn = [pltpu.roll(mid[q], 1, 1) for q in range(6)]
            for h in range(2):
                d = dbuf[k, h, rows, :]
                keep = 1.0 - 4.0 * d
                q = [h * 3 + f for f in range(3)]
                qo = [(1 - h) * 3 + f for f in range(3)]
                north = [jnp.where(is_last, up[qo[f]], up[q[f]]) for f in range(3)]
                south = [jnp.where(is_first, dn[qo[f]], dn[q[f]]) for f in range(3)]
                base = [
                    mid[q[f]] * keep + d * ((es[q[f]] + ws[q[f]]) + (north[f] + south[f]))
                    for f in range(3)
                ]
                out = [
                    base[0] - 0.25 * (es[q[2]] - ws[q[2]]),
                    base[1] - 0.25 * (north[2] - south[2]),
                    base[2] - 0.25 * ((es[q[0]] - ws[q[0]]) + (north[1] - south[1])),
                ]
                for f in range(3):
                    sol[k, q[f], rows, :] = out[f]
                    sums[q[f]] = sums[q[f]] + hi * out[f]
                    sums[6 + q[f]] = sums[6 + q[f]] + lo * out[f]
        for w in range(2):
            for q in range(6):
                m1[g * 6 + q, 8 * w:8 * w + 8, :] = sums[w * 6 + q]

    def slot_forcing(slot, first):
        def step_chunk(c, carry):
            if first:
                for copy in chunk_copies(c):
                    copy.wait()
            for g in range(2 * slot, 2 * slot + 2):
                forcing(c, g)
            return carry

        lax.fori_loop(0, CHUNKS, step_chunk, 0)

    for slot in range(2):
        @pl.when(core == 1 - slot)
        def _():
            slot_forcing(slot, True)

    pair_coef = remote(cmsg, cpart, pair_send.at[0], pair_recv.at[0], partner)
    pair_rows = remote(m1.at[pl.ds((1 - core) * HALF, HALF)], other, pair_send.at[1], pair_recv.at[1], partner)

    @pl.when(core == 1)
    def _():
        pl.semaphore_wait(barrier, 2 * len(steps) + 1)
        pl.semaphore_signal(gate.at[0], inc=1, device_id=partner, device_id_type=MESH)

    @pl.when(core == 0)
    def _():
        pl.semaphore_wait(gate.at[0], 1)

    for copy in (pair_coef, pair_rows):
        copy.start()
    for slot in range(2):
        @pl.when(core == slot)
        def _():
            slot_forcing(slot, False)

    def splat(tile, at):
        return jnp.broadcast_to(tile[:, at:at + 1], (8, 128))

    pair_coef.wait_recv()
    mine, theirs = cmsg[...], cpart[...]
    tile0 = jnp.where(on_low, mine, theirs)
    tile1 = jnp.where(on_low, theirs, mine)
    alpha0, beta0, cross0 = (splat(tile0, at) for at in (0, 32, 64))
    alpha1, beta1, cross1 = (splat(tile1, at) for at in (0, 32, 64))
    mid_pivot = 1.0 / (1.0 + alpha0 + beta1)
    to_low = cross0 * mid_pivot
    to_high = cross1 * mid_pivot
    chip[...] = jnp.where(
        lane < 32, alpha1 - cross1 * to_high,
        jnp.where(lane < 64, beta0 - cross0 * to_low, cross0 * to_high))
    lcoef[0] = to_low
    lcoef[1] = to_high
    lcoef[2] = mid_pivot

    def coef_copy(j, zz):
        return remote(chip, crecv.at[z], cs_sem.at[j], cr_sem.at[z], same_core(zz))

    for j, step in enumerate(steps):
        coef_copy(j, chip_at(step)).start()

    def one(ref, line):
        return jnp.broadcast_to(ref[line:line + 1, :], (8, 128))

    def group_masks(g):
        v = offl[g]
        return [v == o for o in range(3)]

    own_masks = [group_masks(2 * core + gg) for gg in range(2)]
    own = [
        [pick([one(lcoef.at[i], o) for o in range(4)], own_masks[gg]) for i in range(3)]
        for gg in range(2)
    ]
    pair_rows.wait_recv()
    for i in range(HALF):
        low_k, high_k, _ = own[i // 6]
        a_mine, b_mine = m1[core * HALF + i, 0:8, :], m1[core * HALF + i, 8:16, :]
        a_other, b_other = other[i, 0:8, :], other[i, 8:16, :]
        t = jnp.where(on_low, a_mine, a_other) + jnp.where(on_low, b_other, b_mine)
        middle[i] = t
        chip_rows[i, 0:8, :] = jnp.where(on_low, a_other, a_mine) + high_k * t
        chip_rows[i, 8:16, :] = jnp.where(on_low, b_mine, b_other) + low_k * t

    def solver_of(i, w, m):
        b = (m + core) // 2
        return w * 2 + b, m - b * (2 - core)

    def targets():
        for n, dw in enumerate((2, 1, 3, 0)):
            w = lax.rem(z // 2 + dw, chips // 2)
            for m in range(3):
                zz, j = solver_of(None, w, m)
                yield n * 3 + m, zz, j, w * 3 + m

    def target_copy(n, zz, j, unit):
        return remote(chip_rows.at[unit], r1.at[j, z], s1_sem.at[n], r1_sem.at[j, z], same_core(zz))

    for n, zz, j, unit in targets():
        @pl.when(zz != z)
        def _():
            target_copy(n, zz, j, unit).start()

        @pl.when(zz == z)
        def _():
            r1[j, z] = chip_rows[unit]

    @pl.when(waits_late)
    def _():
        send_halo()

    shift_high = pltpu.roll(wide_high, 1, 1)
    inner = jnp.logical_and(lane4 > 0, lane4 < levels - 1)
    ratio = jnp.where(inner, shift_high / jnp.where(inner, wide_high, 1.0), 0.0)
    inner_c = jnp.where(inner, widen(couple), 1.0)
    pivot = pltpu.roll(ratio / inner_c, 127, 1)
    pivot = jnp.where(lane4 == levels - 2, widen(last_row), pivot)
    fill(wv, ratio, levels)
    fill(iv, pivot, levels - 1)

    def down(k, carry):
        out = []
        for g in range(GROUPS):
            rows = slice(8 * g, 8 * g + 8)
            w = wv[k, rows, :]
            for q in range(6):
                y = sol[k, q, rows, :] + w * carry[g * 6 + q]
                sol[k, q, rows, :] = y
                out.append(y)
        return tuple(out)

    def rise(i, carry):
        k = levels - 2 - i
        out = []
        for g in range(GROUPS):
            rows = slice(8 * g, 8 * g + 8)
            piv = iv[k, rows, :]
            w = wv[k + 1, rows, :]
            for q in range(6):
                x = piv * sol[k, q, rows, :] + w * carry[g * 6 + q]
                sol[k, q, rows, :] = x
                out.append(x)
        return tuple(out)

    zero = jnp.zeros((8, 128), f32)
    lax.fori_loop(1, levels - 1, down,
                  tuple(sol[0, q, 8 * g:8 * g + 8, :] for g in range(GROUPS) for q in range(6)))
    lax.fori_loop(0, levels - 1, rise, (zero,) * UNITS)
    for q in range(6):
        sol[levels - 1, q] = jnp.zeros((LINES, 128), f32)

    third = lax.rem(sub, 3)
    m_first = jnp.where(jnp.logical_and(third == 0, sub < 6), 0.25, 0.0).astype(f32)
    m_third = jnp.where(jnp.logical_and(third == 2, sub < 6), 0.25, 0.0).astype(f32)
    edge_line = (0, LINES - 1)
    pair_edge = remote(esum.at[1 - core], epart, pair_send.at[2], pair_recv.at[2], partner)

    def halo_sums():
        for e in (1, 0):
            halo[e].wait_recv()
            sign = 1.0 if e == 0 else -1.0
            line = edge_line[e]
            sum_a = [zero, zero]
            sum_b = [zero, zero]
            for k in range(levels):
                r = 8 + 6 * k
                here = hrecv[e, r:r + 8, :]
                above = hrecv[e, r + 2:r + 10, :]
                below = hrecv[e, r - 2:r + 6, :]
                d = jnp.where(sub < 3, one(dbuf.at[k, 0], line), one(dbuf.at[k, 1], line))
                change = d * here + sign * (m_first * above + m_third * below)
                delta[e, k] = change
                sum_a[k % 2] = sum_a[k % 2] + one(high.at[k], line) * change
                sum_b[k % 2] = sum_b[k % 2] + one(low.at[k], line) * change
            esum[e, 0:8, :] = sum_a[0] + sum_a[1]
            esum[e, 8:16, :] = sum_b[0] + sum_b[1]
        pair_edge.start()

    @pl.when(me_h > 1)
    def _():
        halo_sums()

    crecv[z] = chip[...]
    for step in steps:
        zz = chip_at(step)
        remote(chip, crecv.at[zz], cs_sem.at[0], cr_sem.at[zz], same_core(zz)).wait_recv()
    alphas, betas, crosses = [], [], []
    for r in range(chips):
        tile = crecv[r]
        alphas.append(splat(tile, 0))
        betas.append(splat(tile, 32))
        crosses.append(splat(tile, 64))
    mains = [1.0 + alphas[r] + (betas[r + 1] if r + 1 < chips else 0.0) for r in range(chips)]
    before = None
    for r in range(chips):
        q = crosses[r] * before if r > 0 else zero
        main = mains[r] - crosses[r] * q if r > 0 else mains[r]
        before = 1.0 / main
        comp[0, r] = q
        comp[1, r] = before
        comp[4, r] = crosses[r]
    after = None
    for r in range(chips - 1, -1, -1):
        q = crosses[r + 1] * after if r + 1 < chips else zero
        main = mains[r] - crosses[r + 1] * q if r + 1 < chips else mains[r]
        after = 1.0 / main
        comp[2, r] = q
        comp[3, r] = main

    parity = lax.rem(z, 2)
    first_unit = (z // 2) * 3 + parity * (2 - core)
    has = [None, parity == core]
    for j in range(2):
        m = group_masks(2 * core + jnp.minimum(first_unit + j, HALF - 1) // 6)
        for i in range(2):
            for r in range(chips):
                ucoef[j, i, r] = pick([one(comp.at[i, r], o) for o in range(4)], m)

    edge_off = offv[core * (LINES - 1)]
    z_low = jnp.maximum(z - 1, 0)

    def edge_comp(i, r):
        return jnp.broadcast_to(comp[i, r, pl.ds(edge_off, 1), :], (8, 128))

    def edge_local(i):
        return jnp.broadcast_to(lcoef[i, pl.ds(edge_off, 1), :], (8, 128))

    def edge_copy(n, zz):
        return remote(em.at[jnp.where(zz > z, 0, 1)], er.at[z], es_sem.at[n], er_sem.at[z], same_core(zz))

    def edge_send():
        pair_edge.wait_recv()
        a_mine, b_mine = esum[core, 0:8, :], esum[core, 8:16, :]
        a_other, b_other = epart[0:8, :], epart[8:16, :]
        edge_t = jnp.where(on_low, a_mine, a_other) + jnp.where(on_low, b_other, b_mine)
        edge_a = jnp.where(on_low, a_other, a_mine) + edge_local(1) * edge_t
        edge_b = jnp.where(on_low, b_mine, b_other) + edge_local(0) * edge_t
        ends[0] = edge_t
        ends[1] = edge_a
        ends[2] = edge_b
        em[0] = edge_a + edge_comp(0, z) * edge_b
        em[1] = edge_b + edge_comp(2, z_low) * edge_a
        for n, step in enumerate(steps):
            edge_copy(n, chip_at(step)).start()

    @pl.when(me_h > 1)
    def _():
        edge_send()

    def answer(j, n, zz):
        return remote(m2.at[j, zz], got.at[first_unit + j], s2_sem.at[j, n], r2_sem.at[first_unit + j],
                      same_core(zz))

    def solve_unit(j):
        for step in steps:
            zz = chip_at(step)
            remote(chip_rows.at[0], r1.at[j, zz], s1_sem.at[0], r1_sem.at[j, zz], same_core(zz)).wait_recv()
        values = []
        for r in range(chips):
            t = r1[j, r, 0:8, :]
            if r + 1 < chips:
                t = t + r1[j, r + 1, 8:16, :]
            values.append(t if r == 0 else t + ucoef[j, 0, r] * values[r - 1])
        s = values[chips - 1] * ucoef[j, 1, chips - 1]
        for r in range(chips - 1, -1, -1):
            m2[j, r, 8:16, :] = s
            if r + 1 < chips:
                m2[j, r + 1, 0:8, :] = s
            if r > 0:
                s = values[r - 1] * ucoef[j, 1, r - 1] + ucoef[j, 0, r] * s
        m2[j, 0, 0:8, :] = zero
        for n, step in enumerate(steps):
            answer(j, n, chip_at(step)).start()
        got[first_unit + j] = m2[j, z]

    solve_unit(0)

    @pl.when(has[1])
    def _():
        solve_unit(1)

    @pl.when(me_h <= 1)
    def _():
        halo_sums()
        edge_send()

    sol2 = sol.reshape(levels * 6 * LINES, 128)
    for e in range(2):
        line = edge_line[e]
        prev = delta[e, 0]
        for k in range(1, levels - 1):
            prev = delta[e, k] + one(wv.at[k], line) * prev
            delta[e, k] = prev
        x = zero
        for k in range(levels - 2, -1, -1):
            x = one(iv.at[k], line) * delta[e, k] + one(wv.at[k + 1], line) * x
            rows = pl.ds(k * 6 * LINES + line, 6, stride=LINES)
            sol2[rows, :] = sol2[rows, :] + x[0:6, :]

    for i in range(HALF):
        @pl.when(w_solver(i, core) != z)
        def _():
            remote(m2.at[0, 0], got.at[i], s2_sem.at[0, 0], r2_sem.at[i], same_core(w_solver(i, core))).wait_recv()
    for i in range(HALF):
        low_k, high_k, pivot_k = own[i // 6]
        s_low, s_high = got[i, 0:8, :], got[i, 8:16, :]
        s_mid = middle[i] * pivot_k + low_k * s_low + high_k * s_high
        back[core * HALF + i, 0:8, :] = jnp.where(on_low, s_low, s_mid)
        back[core * HALF + i, 8:16, :] = jnp.where(on_low, s_mid, s_high)
        pass_on[i, 0:8, :] = jnp.where(on_low, s_mid, s_low)
        pass_on[i, 8:16, :] = jnp.where(on_low, s_high, s_mid)
    pair_ends = remote(pass_on, back.at[pl.ds(core * HALF, HALF)], pair_send.at[3], pair_recv.at[3], partner)
    pair_ends.start()

    for step in steps:
        zz = chip_at(step)
        remote(em.at[0], er.at[zz], es_sem.at[0], er_sem.at[zz], same_core(zz)).wait_recv()
    v = zero
    w = zero
    for r in range(chips):
        v = jnp.where(r < z, er[r] + edge_comp(0, r) * v, v)
    for r in range(chips - 1, 0, -1):
        w = jnp.where(r > z, er[r] + edge_comp(2, r - 1) * w, w)
    edge_t = ends[0]
    v = v + ends[2]
    w = w + ends[1]
    q_here = edge_comp(0, z)
    u_here = edge_comp(4, z)
    edge_high = (w + q_here * v) / (edge_comp(3, z) - u_here * q_here)
    edge_low = jnp.where(z > 0, (v + u_here * edge_high) * edge_comp(1, z_low), 0.0)
    edge_mid = edge_local(2) * edge_t + edge_local(0) * edge_low + edge_local(1) * edge_high
    edge_out[0:8, :] = jnp.where(on_low, edge_mid, edge_low)
    edge_out[8:16, :] = jnp.where(on_low, edge_high, edge_mid)
    pair_last = remote(edge_out, edge_in, pair_send.at[4], pair_recv.at[4], partner)
    pair_last.start()
    back2 = back.reshape((UNITS + 2) * 16, 128)

    def add_to_line(e, parts):
        for w in range(2):
            rows = pl.ds(e * (UNITS - 6) * 16 + 8 * w + 7 * e, 6, stride=16)
            back2[rows, :] = back2[rows, :] + parts[w][0:6, :]

    for e in range(2):
        @pl.when(core == e)
        def _():
            add_to_line(e, (edge_low, edge_mid) if e == 0 else (edge_mid, edge_high))

    for copy in (*halo, pair_coef, pair_rows, pair_edge):
        copy.wait_send()
    for n, step in enumerate(steps):
        coef_copy(n, chip_at(step)).wait_send()
        edge_copy(n, chip_at(step)).wait_send()
        answer(0, n, chip_at(step)).wait_send()
    for n, zz, j, unit in targets():
        @pl.when(zz != z)
        def _():
            target_copy(n, zz, j, unit).wait_send()

    @pl.when(has[1])
    def _():
        for n, step in enumerate(steps):
            answer(1, n, chip_at(step)).wait_send()
    pair_ends.wait()
    pair_last.wait()
    for e in range(2):
        @pl.when(core == 1 - e)
        def _():
            add_to_line(e, (edge_in[0:8, :], edge_in[8:16, :]))


def w_solver(i, core):
    return (i // 3) * 2 + (i % 3 + core) // 2


def assemble_kernel(sol, back, low, high, out, stage, sem):
    levels = sol.shape[0]
    per = levels // CHUNKS

    def copies(c):
        lev = pl.ds(c * per, per)
        return [
            pltpu.make_async_copy(
                stage.at[f, lev], out.at[f, lev], sem.at[c, f])
            for f in range(3)
        ]

    def chunk(c, carry):
        for g in range(GROUPS):
            rows = slice(8 * g, 8 * g + 8)
            prev = [back[g * 6 + q, 0:8, :] for q in range(6)]
            here = [back[g * 6 + q, 8:16, :] for q in range(6)]
            for l in range(per):
                k = c * per + l
                lo = low[k, rows, :]
                hi = high[k, rows, :]
                for q in range(6):
                    h, f = q // 3, q % 3
                    stage[f, k, rows, 128 * h:128 * h + 128] = sol[k, q, rows, :] + (lo * prev[q] + hi * here[q])
        for copy in copies(c):
            copy.start()
        return carry

    lax.fori_loop(0, CHUNKS, chunk, 0)
    for c in range(CHUNKS):
        for copy in copies(c):
            copy.wait()


def body(n_h, n_d, fields, diffusivity, offsets, coupling, inverse):
    f32 = jnp.float32
    levels = fields.shape[1]
    chips = n_d // 2
    hbm_spec = pl.BlockSpec(memory_space=pltpu.HBM)
    vmem_spec = pl.BlockSpec(memory_space=pltpu.VMEM)
    V = lambda *shape: pltpu.VMEM(shape, f32)
    dma = lambda *shape: pltpu.SemaphoreType.DMA(shape)
    sol, back, low, high = pl.pallas_call(
        functools.partial(columns_kernel, n_h, n_d),
        out_shape=(
            V(levels, 6, LINES, 128),
            V(UNITS + 2, 16, 128),
            V(levels, LINES, 128),
            V(levels, LINES, 128),
        ),
        in_specs=[hbm_spec] * 5,
        out_specs=(vmem_spec,) * 4,
        scratch_shapes=[
            V(levels, 6, PAD, 128),
            V(levels, 2, LINES, 128),
            pltpu.SMEM((LINES,), jnp.int32),
            V(4, levels),
            V(4, levels, levels),
            pltpu.VMEM((GROUPS, 8, 128), jnp.int32),
            V(levels, LINES, 128),
            V(levels, LINES, 128),
            V(2, levels, 8, 128),
            V(2, levels * 6, 128),
            V(2, levels * 6 + 16, 128),
            V(8, 128),
            V(8, 128),
            V(8, 128),
            V(chips, 8, 128),
            V(UNITS, 16, 128),
            V(HALF, 16, 128),
            V(HALF, 16, 128),
            V(HALF + 2, 8, 128),
            V(2, chips, 16, 128),
            V(2, chips, 16, 128),
            V(HALF + 2, 16, 128),
            V(HALF, 16, 128),
            V(2, 16, 128),
            V(16, 128),
            V(2, 8, 128),
            V(chips, 8, 128),
            V(5, chips, 8, 128),
            V(2, 2, chips, 8, 128),
            V(3, 8, 128),
            V(3, 8, 128),
            V(16, 128),
            V(16, 128),
            dma(2, 6),
            dma(CHUNKS, 8),
            dma(3),
            dma(2),
            dma(2),
            dma(5),
            dma(5),
            dma(chips),
            dma(chips),
            dma(HALF),
            dma(2, chips),
            dma(2, chips),
            dma(HALF),
            dma(chips),
            dma(chips),
            pltpu.SemaphoreType.REGULAR((2,)),
        ],
        compiler_params=pltpu.CompilerParams(
            collective_id=0, has_side_effects=True, vmem_limit_bytes=48 * 1024 * 1024),
        name="columns",
    )(*(pltpu.with_memory_space_constraint(x, pltpu.HBM)
        for x in (fields, diffusivity, offsets, coupling, inverse)))
    return pl.pallas_call(
        assemble_kernel,
        out_shape=jax.ShapeDtypeStruct(fields.shape, f32),
        in_specs=[vmem_spec] * 4,
        out_specs=hbm_spec,
        scratch_shapes=[
            V(3, levels, LINES, 256),
            dma(CHUNKS, 3),
        ],
        compiler_params=pltpu.CompilerParams(vmem_limit_bytes=48 * 1024 * 1024),
        name="assemble",
    )(sol, back, low, high)


def solution(mesh):
    return jax.shard_map(
        functools.partial(body, mesh.shape["horiz"], mesh.shape["depth"]),
        mesh=mesh,
        in_specs=(
            P(None, "depth", "horiz", None),
            P("depth", "horiz", None),
            P("horiz"),
            P(None, "depth"),
            P(None, "depth", None),
        ),
        out_specs=P(None, "depth", "horiz", None),
        check_vma=False,
    )
```

```python
import functools

import jax
import jax.numpy as jnp
from jax import lax
from jax.experimental import pallas as pl
from jax.experimental.pallas import tpu as pltpu
from jax.sharding import PartitionSpec as P

MESH = pl.DeviceIdType.MESH
CHUNKS = 4
PAD = 48
LINES = 32
GROUPS = LINES // 8
UNITS = GROUPS * 6
HALF = UNITS // 2


def far_first(chips):
    return sorted(range(1, chips), key=lambda s: -min(s, chips - s))


def columns_kernel(
    n_h, n_d,
    fields, diff, offs, coup, inv,
    sol, back, low, high,
    fbuf, dbuf, offv, cvec, kvec, offl, wv, iv, delta,
    hsend, hrecv, cmsg, cpart, chip, crecv, m1, other, chip_rows, middle, r1, m2, got, pass_on,
    esum, epart, em, er, comp, ucoef, lcoef, ends, edge_out, edge_in,
    edge_sem, load_sem, small_sem, hs_sem, hr_sem, pair_send, pair_recv, cs_sem, cr_sem,
    s1_sem, r1_sem, s2_sem, r2_sem, es_sem, er_sem, gate,
):
    f32 = jnp.float32
    levels = fields.shape[1]
    per = levels // CHUNKS
    me_h = lax.axis_index("horiz")
    me = lax.axis_index("depth")
    east = lax.rem(me_h + 1, n_h)
    west = lax.rem(me_h + n_h - 1, n_h)
    z, core = me // 2, lax.rem(me, 2)
    chips = n_d // 2
    steps = far_first(chips)
    on_low = core == 0

    def chip_at(step):
        return lax.rem(z + step, chips)

    def same_core(zz):
        return (me_h, zz * 2 + core)

    partner = (me_h, z * 2 + 1 - core)

    def remote(src, dst, send, recv, to):
        return pltpu.make_async_remote_copy(
            src_ref=src, dst_ref=dst, send_sem=send, recv_sem=recv, device_id=to, device_id_type=MESH)

    barrier = pltpu.get_barrier_semaphore()
    meets = [(east, z * 2), (west, z * 2), partner] + [(me_h, chip_at(step) * 2 + 1) for step in steps]
    for to in meets:
        pl.semaphore_signal(barrier, inc=1, device_id=to, device_id_type=MESH)

    small = [
        pltpu.make_async_copy(offs, offv, small_sem.at[0]),
        pltpu.make_async_copy(coup, cvec, small_sem.at[1]),
        pltpu.make_async_copy(inv, kvec, small_sem.at[2]),
    ]
    outer = []
    for i, first in enumerate((LINES - 8, 0)):
        for h in range(2):
            for f in range(3):
                outer.append(pltpu.make_async_copy(
                    fields.at[f, :, pl.ds(first, 8), pl.ds(h * 128, 128)],
                    fbuf.at[:, h * 3 + f, pl.ds(8 + first, 8), :],
                    edge_sem.at[i, h * 3 + f]))

    def chunk_copies(c):
        lev = pl.ds(c * per, per)
        out = []
        for h in range(2):
            lane = pl.ds(h * 128, 128)
            for f in range(3):
                out.append(pltpu.make_async_copy(
                    fields.at[f, lev, pl.ds(8, LINES - 16), lane],
                    fbuf.at[lev, h * 3 + f, pl.ds(16, LINES - 16), :],
                    load_sem.at[c, h * 3 + f]))
            out.append(pltpu.make_async_copy(
                diff.at[lev, :, lane], dbuf.at[lev, h], load_sem.at[c, 6 + h]))
        return out

    for copy in small + outer:
        copy.start()
    for c in range(CHUNKS):
        for copy in chunk_copies(c):
            copy.start()

    f2 = fbuf.reshape(levels * 6 * PAD, 128)
    f2[pl.ds(7, levels * 6, stride=PAD), :] = jnp.zeros((levels * 6, 128), f32)
    f2[pl.ds(40, levels * 6, stride=PAD), :] = jnp.zeros((levels * 6, 128), f32)
    for e in range(2):
        hrecv[e, 0:8, :] = jnp.zeros((8, 128), f32)
        hrecv[e, 200:208, :] = jnp.zeros((8, 128), f32)
    m1[...] = jnp.zeros(m1.shape, f32)

    def pack(e):
        for copy in outer[6 * e:6 * e + 6]:
            copy.wait()
        hsend[e] = f2[pl.ds(8 if e else 39, levels * 6, stride=PAD), :]

    halo = [
        remote(hsend.at[e], hrecv.at[e, pl.ds(8, levels * 6), :], hs_sem.at[e], hr_sem.at[e], (to, me))
        for e, to in ((0, east), (1, west))
    ]

    waits_late = me_h == 0

    def meet_neighbours():
        @pl.when(core == 0)
        def _():
            pl.semaphore_wait(barrier, 5)
            pl.semaphore_signal(gate.at[1], inc=1, device_id=partner, device_id_type=MESH)

        @pl.when(core == 1)
        def _():
            pl.semaphore_wait(gate.at[1], 1)

    @pl.when(me_h == n_h - 1)
    def _():
        meet_neighbours()
        for e in range(2):
            pack(e)
            halo[e].start()

    for copy in small:
        copy.wait()
    sub = lax.broadcasted_iota(jnp.int32, (8, 128), 0)
    lane = lax.broadcasted_iota(jnp.int32, (8, 128), 1)
    masks = []
    for g in range(GROUPS):
        v = jnp.full((8, 128), offv[8 * g], jnp.int32)
        for i in range(1, 8):
            v = jnp.where(sub == i, offv[8 * g + i], v)
        offl[g] = v
        masks.append([v == o for o in range(3)])

    def widen(x):
        return jnp.concatenate([x, jnp.zeros((4, 128 - levels), f32)], axis=1)

    couple = cvec[...]
    first_row = kvec[:, 0, :]
    last_row = kvec[:, levels - 2, :]
    c_low = couple[:, 0:1]
    c_high = couple[:, levels - 1:levels]
    inside = jnp.where(me > 0, 1.0, 0.0).astype(f32)
    table_low = first_row * (jnp.broadcast_to(c_low, (4, levels)) * inside)
    table_high = last_row * jnp.broadcast_to(c_high, (4, levels))
    lane4 = lax.broadcasted_iota(jnp.int32, (4, 128), 1)

    def pick(rows, m):
        return jnp.where(m[0], rows[0], jnp.where(m[1], rows[1], jnp.where(m[2], rows[2], rows[3])))

    def by_line(table):
        rows = [jnp.broadcast_to(table[o:o + 1, :], (8, 128)) for o in range(4)]
        return [pick(rows, masks[g]) for g in range(GROUPS)]

    def fill(ref, table, count):
        lines = by_line(table)
        for k in range(count):
            for g in range(GROUPS):
                ref[k, 8 * g:8 * g + 8, :] = jnp.broadcast_to(lines[g][:, k:k + 1], (8, 128))

    wide_high = widen(table_high)
    fill(low, jnp.where(lane4 == levels - 1, 0.0, widen(table_low)), levels)
    fill(high, jnp.where(lane4 == levels - 1, 1.0, wide_high), levels)

    c_low4 = jnp.broadcast_to(c_low, (4, 128))
    c_high4 = jnp.broadcast_to(c_high, (4, 128))
    alpha = c_high4 - c_high4 * jnp.broadcast_to(table_high[:, levels - 2:levels - 1], (4, 128))
    beta = c_low4 - c_low4 * jnp.broadcast_to(table_low[:, 0:1], (4, 128))
    cross = c_high4 * jnp.broadcast_to(table_low[:, levels - 2:levels - 1], (4, 128))
    packed = jnp.where(lane4 < 32, alpha, jnp.where(lane4 < 64, beta, cross))
    cmsg[0:4, :] = packed
    cmsg[4:8, :] = packed

    @pl.when(me_h != n_h - 1)
    def _():
        for e in range(2):
            pack(e)

    def send_halo():
        meet_neighbours()
        for copy in halo:
            copy.start()

    @pl.when(jnp.logical_and(me_h != n_h - 1, jnp.logical_not(waits_late)))
    def _():
        send_halo()

    is_last = lane == 127
    is_first = lane == 0

    def forcing(c, g):
        r0 = 8 + 8 * g
        rows = slice(8 * g, 8 * g + 8)
        sums = [m1[g * 6 + q, 8 * w:8 * w + 8, :] for w in range(2) for q in range(6)]
        for l in range(per):
            k = c * per + l
            hi = high[k, rows, :]
            lo = low[k, rows, :]
            mid = [fbuf[k, q, r0:r0 + 8, :] for q in range(6)]
            es = [fbuf[k, q, r0 + 1:r0 + 9, :] for q in range(6)]
            ws = [fbuf[k, q, r0 - 1:r0 + 7, :] for q in range(6)]
            up = [pltpu.roll(mid[q], 127, 1) for q in range(6)]
            dn = [pltpu.roll(mid[q], 1, 1) for q in range(6)]
            for h in range(2):
                d = dbuf[k, h, rows, :]
                keep = 1.0 - 4.0 * d
                q = [h * 3 + f for f in range(3)]
                qo = [(1 - h) * 3 + f for f in range(3)]
                north = [jnp.where(is_last, up[qo[f]], up[q[f]]) for f in range(3)]
                south = [jnp.where(is_first, dn[qo[f]], dn[q[f]]) for f in range(3)]
                base = [
                    mid[q[f]] * keep + d * ((es[q[f]] + ws[q[f]]) + (north[f] + south[f]))
                    for f in range(3)
                ]
                out = [
                    base[0] - 0.25 * (es[q[2]] - ws[q[2]]),
                    base[1] - 0.25 * (north[2] - south[2]),
                    base[2] - 0.25 * ((es[q[0]] - ws[q[0]]) + (north[1] - south[1])),
                ]
                for f in range(3):
                    sol[k, q[f], rows, :] = out[f]
                    sums[q[f]] = sums[q[f]] + hi * out[f]
                    sums[6 + q[f]] = sums[6 + q[f]] + lo * out[f]
        for w in range(2):
            for q in range(6):
                m1[g * 6 + q, 8 * w:8 * w + 8, :] = sums[w * 6 + q]

    def slot_forcing(slot, first, start, stop):
        def step_chunk(c, carry):
            if first:
                for copy in chunk_copies(c):
                    copy.wait()
            for g in range(2 * slot, 2 * slot + 2):
                forcing(c, g)
            return carry

        lax.fori_loop(start, stop, step_chunk, 0)

    for slot in range(2):
        @pl.when(core == 1 - slot)
        def _():
            slot_forcing(slot, True, 0, CHUNKS)

    pair_coef = remote(cmsg, cpart, pair_send.at[0], pair_recv.at[0], partner)
    pair_rows = remote(m1.at[pl.ds((1 - core) * HALF, HALF)], other, pair_send.at[1], pair_recv.at[1], partner)

    @pl.when(core == 1)
    def _():
        pl.semaphore_wait(barrier, 2 * len(steps) + 1)
        pl.semaphore_signal(gate.at[0], inc=1, device_id=partner, device_id_type=MESH)

    @pl.when(core == 0)
    def _():
        pl.semaphore_wait(gate.at[0], 1)

    for copy in (pair_coef, pair_rows):
        copy.start()
    def second_half(start, stop):
        for slot in range(2):
            @pl.when(core == slot)
            def _():
                slot_forcing(slot, False, start, stop)

    second_half(0, CHUNKS - 1)

    def splat(tile, at):
        return jnp.broadcast_to(tile[:, at:at + 1], (8, 128))

    pair_coef.wait_recv()
    mine, theirs = cmsg[...], cpart[...]
    tile0 = jnp.where(on_low, mine, theirs)
    tile1 = jnp.where(on_low, theirs, mine)
    alpha0, beta0, cross0 = (splat(tile0, at) for at in (0, 32, 64))
    alpha1, beta1, cross1 = (splat(tile1, at) for at in (0, 32, 64))
    mid_pivot = 1.0 / (1.0 + alpha0 + beta1)
    to_low = cross0 * mid_pivot
    to_high = cross1 * mid_pivot
    chip[...] = jnp.where(
        lane < 32, alpha1 - cross1 * to_high,
        jnp.where(lane < 64, beta0 - cross0 * to_low, cross0 * to_high))
    lcoef[0] = to_low
    lcoef[1] = to_high
    lcoef[2] = mid_pivot

    def coef_copy(j, zz):
        return remote(chip, crecv.at[z], cs_sem.at[j], cr_sem.at[z], same_core(zz))

    for j, step in enumerate(steps):
        coef_copy(j, chip_at(step)).start()

    second_half(CHUNKS - 1, CHUNKS)

    def one(ref, line):
        return jnp.broadcast_to(ref[line:line + 1, :], (8, 128))

    def group_masks(g):
        v = offl[g]
        return [v == o for o in range(3)]

    own_masks = [group_masks(2 * core + gg) for gg in range(2)]
    own = [
        [pick([one(lcoef.at[i], o) for o in range(4)], own_masks[gg]) for i in range(3)]
        for gg in range(2)
    ]
    pair_rows.wait_recv()
    for i in range(HALF):
        low_k, high_k, _ = own[i // 6]
        a_mine, b_mine = m1[core * HALF + i, 0:8, :], m1[core * HALF + i, 8:16, :]
        a_other, b_other = other[i, 0:8, :], other[i, 8:16, :]
        t = jnp.where(on_low, a_mine, a_other) + jnp.where(on_low, b_other, b_mine)
        middle[i] = t
        chip_rows[i, 0:8, :] = jnp.where(on_low, a_other, a_mine) + high_k * t
        chip_rows[i, 8:16, :] = jnp.where(on_low, b_mine, b_other) + low_k * t

    def solver_of(i, w, m):
        b = (m + core) // 2
        return w * 2 + b, m - b * (2 - core)

    def targets():
        for n, dw in enumerate((2, 1, 3, 0)):
            w = lax.rem(z // 2 + dw, chips // 2)
            for m in range(3):
                zz, j = solver_of(None, w, m)
                yield n * 3 + m, zz, j, w * 3 + m

    def target_copy(n, zz, j, unit):
        return remote(chip_rows.at[unit], r1.at[j, z], s1_sem.at[n], r1_sem.at[j, z], same_core(zz))

    for n, zz, j, unit in targets():
        @pl.when(zz != z)
        def _():
            target_copy(n, zz, j, unit).start()

        @pl.when(zz == z)
        def _():
            r1[j, z] = chip_rows[unit]

    @pl.when(waits_late)
    def _():
        send_halo()

    shift_high = pltpu.roll(wide_high, 1, 1)
    inner = jnp.logical_and(lane4 > 0, lane4 < levels - 1)
    ratio = jnp.where(inner, shift_high / jnp.where(inner, wide_high, 1.0), 0.0)
    inner_c = jnp.where(inner, widen(couple), 1.0)
    pivot = pltpu.roll(ratio / inner_c, 127, 1)
    pivot = jnp.where(lane4 == levels - 2, widen(last_row), pivot)
    fill(wv, ratio, levels)
    fill(iv, pivot, levels - 1)

    def down(k, carry):
        out = []
        for g in range(GROUPS):
            rows = slice(8 * g, 8 * g + 8)
            w = wv[k, rows, :]
            for q in range(6):
                y = sol[k, q, rows, :] + w * carry[g * 6 + q]
                sol[k, q, rows, :] = y
                out.append(y)
        return tuple(out)

    def rise(i, carry):
        k = levels - 2 - i
        out = []
        for g in range(GROUPS):
            rows = slice(8 * g, 8 * g + 8)
            piv = iv[k, rows, :]
            w = wv[k + 1, rows, :]
            for q in range(6):
                x = piv * sol[k, q, rows, :] + w * carry[g * 6 + q]
                sol[k, q, rows, :] = x
                out.append(x)
        return tuple(out)

    zero = jnp.zeros((8, 128), f32)
    lax.fori_loop(1, levels - 1, down,
                  tuple(sol[0, q, 8 * g:8 * g + 8, :] for g in range(GROUPS) for q in range(6)))
    lax.fori_loop(0, levels - 1, rise, (zero,) * UNITS)
    for q in range(6):
        sol[levels - 1, q] = jnp.zeros((LINES, 128), f32)

    third = lax.rem(sub, 3)
    m_first = jnp.where(jnp.logical_and(third == 0, sub < 6), 0.25, 0.0).astype(f32)
    m_third = jnp.where(jnp.logical_and(third == 2, sub < 6), 0.25, 0.0).astype(f32)
    edge_line = (0, LINES - 1)
    pair_edge = remote(esum.at[1 - core], epart, pair_send.at[2], pair_recv.at[2], partner)

    def halo_sums():
        for e in (1, 0):
            halo[e].wait_recv()
            sign = 1.0 if e == 0 else -1.0
            line = edge_line[e]
            sum_a = [zero, zero]
            sum_b = [zero, zero]
            for k in range(levels):
                r = 8 + 6 * k
                here = hrecv[e, r:r + 8, :]
                above = hrecv[e, r + 2:r + 10, :]
                below = hrecv[e, r - 2:r + 6, :]
                d = jnp.where(sub < 3, one(dbuf.at[k, 0], line), one(dbuf.at[k, 1], line))
                change = d * here + sign * (m_first * above + m_third * below)
                delta[e, k] = change
                sum_a[k % 2] = sum_a[k % 2] + one(high.at[k], line) * change
                sum_b[k % 2] = sum_b[k % 2] + one(low.at[k], line) * change
            esum[e, 0:8, :] = sum_a[0] + sum_a[1]
            esum[e, 8:16, :] = sum_b[0] + sum_b[1]
        pair_edge.start()

    @pl.when(me_h > 1)
    def _():
        halo_sums()

    crecv[z] = chip[...]
    for step in steps:
        zz = chip_at(step)
        remote(chip, crecv.at[zz], cs_sem.at[0], cr_sem.at[zz], same_core(zz)).wait_recv()
    alphas, betas, crosses = [], [], []
    for r in range(chips):
        tile = crecv[r]
        alphas.append(splat(tile, 0))
        betas.append(splat(tile, 32))
        crosses.append(splat(tile, 64))
    mains = [1.0 + alphas[r] + (betas[r + 1] if r + 1 < chips else 0.0) for r in range(chips)]
    before = None
    for r in range(chips):
        q = crosses[r] * before if r > 0 else zero
        main = mains[r] - crosses[r] * q if r > 0 else mains[r]
        before = 1.0 / main
        comp[0, r] = q
        comp[1, r] = before
        comp[4, r] = crosses[r]
    after = None
    for r in range(chips - 1, -1, -1):
        q = crosses[r + 1] * after if r + 1 < chips else zero
        main = mains[r] - crosses[r + 1] * q if r + 1 < chips else mains[r]
        after = 1.0 / main
        comp[2, r] = q
        comp[3, r] = main

    parity = lax.rem(z, 2)
    first_unit = (z // 2) * 3 + parity * (2 - core)
    has = [None, parity == core]
    for j in range(2):
        m = group_masks(2 * core + jnp.minimum(first_unit + j, HALF - 1) // 6)
        for i in range(2):
            for r in range(chips):
                ucoef[j, i, r] = pick([one(comp.at[i, r], o) for o in range(4)], m)

    edge_off = offv[core * (LINES - 1)]
    z_low = jnp.maximum(z - 1, 0)

    def edge_comp(i, r):
        return jnp.broadcast_to(comp[i, r, pl.ds(edge_off, 1), :], (8, 128))

    def edge_local(i):
        return jnp.broadcast_to(lcoef[i, pl.ds(edge_off, 1), :], (8, 128))

    def edge_copy(n, zz):
        return remote(em.at[jnp.where(zz > z, 0, 1)], er.at[z], es_sem.at[n], er_sem.at[z], same_core(zz))

    def edge_send():
        pair_edge.wait_recv()
        a_mine, b_mine = esum[core, 0:8, :], esum[core, 8:16, :]
        a_other, b_other = epart[0:8, :], epart[8:16, :]
        edge_t = jnp.where(on_low, a_mine, a_other) + jnp.where(on_low, b_other, b_mine)
        edge_a = jnp.where(on_low, a_other, a_mine) + edge_local(1) * edge_t
        edge_b = jnp.where(on_low, b_mine, b_other) + edge_local(0) * edge_t
        ends[0] = edge_t
        ends[1] = edge_a
        ends[2] = edge_b
        em[0] = edge_a + edge_comp(0, z) * edge_b
        em[1] = edge_b + edge_comp(2, z_low) * edge_a
        for n, step in enumerate(steps):
            edge_copy(n, chip_at(step)).start()

    @pl.when(me_h > 1)
    def _():
        edge_send()

    def answer(j, n, zz):
        return remote(m2.at[j, zz], got.at[first_unit + j], s2_sem.at[j, n], r2_sem.at[first_unit + j],
                      same_core(zz))

    def solve_unit(j):
        for step in steps:
            zz = chip_at(step)
            remote(chip_rows.at[0], r1.at[j, zz], s1_sem.at[0], r1_sem.at[j, zz], same_core(zz)).wait_recv()
        values = []
        for r in range(chips):
            t = r1[j, r, 0:8, :]
            if r + 1 < chips:
                t = t + r1[j, r + 1, 8:16, :]
            values.append(t if r == 0 else t + ucoef[j, 0, r] * values[r - 1])
        s = values[chips - 1] * ucoef[j, 1, chips - 1]
        for r in range(chips - 1, -1, -1):
            m2[j, r, 8:16, :] = s
            if r + 1 < chips:
                m2[j, r + 1, 0:8, :] = s
            if r > 0:
                s = values[r - 1] * ucoef[j, 1, r - 1] + ucoef[j, 0, r] * s
        m2[j, 0, 0:8, :] = zero
        for n, step in enumerate(steps):
            answer(j, n, chip_at(step)).start()
        got[first_unit + j] = m2[j, z]

    solve_unit(0)

    @pl.when(has[1])
    def _():
        solve_unit(1)

    @pl.when(me_h <= 1)
    def _():
        halo_sums()
        edge_send()

    sol2 = sol.reshape(levels * 6 * LINES, 128)
    for e in range(2):
        line = edge_line[e]
        prev = delta[e, 0]
        for k in range(1, levels - 1):
            prev = delta[e, k] + one(wv.at[k], line) * prev
            delta[e, k] = prev
        x = zero
        for k in range(levels - 2, -1, -1):
            x = one(iv.at[k], line) * delta[e, k] + one(wv.at[k + 1], line) * x
            rows = pl.ds(k * 6 * LINES + line, 6, stride=LINES)
            sol2[rows, :] = sol2[rows, :] + x[0:6, :]

    for i in range(HALF):
        @pl.when(w_solver(i, core) != z)
        def _():
            remote(m2.at[0, 0], got.at[i], s2_sem.at[0, 0], r2_sem.at[i], same_core(w_solver(i, core))).wait_recv()
    for i in range(HALF):
        low_k, high_k, pivot_k = own[i // 6]
        s_low, s_high = got[i, 0:8, :], got[i, 8:16, :]
        s_mid = middle[i] * pivot_k + low_k * s_low + high_k * s_high
        back[core * HALF + i, 0:8, :] = jnp.where(on_low, s_low, s_mid)
        back[core * HALF + i, 8:16, :] = jnp.where(on_low, s_mid, s_high)
        pass_on[i, 0:8, :] = jnp.where(on_low, s_mid, s_low)
        pass_on[i, 8:16, :] = jnp.where(on_low, s_high, s_mid)
    pair_ends = remote(pass_on, back.at[pl.ds(core * HALF, HALF)], pair_send.at[3], pair_recv.at[3], partner)
    pair_ends.start()

    for step in steps:
        zz = chip_at(step)
        remote(em.at[0], er.at[zz], es_sem.at[0], er_sem.at[zz], same_core(zz)).wait_recv()
    v = zero
    w = zero
    for r in range(chips):
        v = jnp.where(r < z, er[r] + edge_comp(0, r) * v, v)
    for r in range(chips - 1, 0, -1):
        w = jnp.where(r > z, er[r] + edge_comp(2, r - 1) * w, w)
    edge_t = ends[0]
    v = v + ends[2]
    w = w + ends[1]
    q_here = edge_comp(0, z)
    u_here = edge_comp(4, z)
    edge_high = (w + q_here * v) / (edge_comp(3, z) - u_here * q_here)
    edge_low = jnp.where(z > 0, (v + u_here * edge_high) * edge_comp(1, z_low), 0.0)
    edge_mid = edge_local(2) * edge_t + edge_local(0) * edge_low + edge_local(1) * edge_high
    edge_out[0:8, :] = jnp.where(on_low, edge_mid, edge_low)
    edge_out[8:16, :] = jnp.where(on_low, edge_high, edge_mid)
    pair_last = remote(edge_out, edge_in, pair_send.at[4], pair_recv.at[4], partner)
    pair_last.start()
    back2 = back.reshape((UNITS + 2) * 16, 128)

    def add_to_line(e, parts):
        for w in range(2):
            rows = pl.ds(e * (UNITS - 6) * 16 + 8 * w + 7 * e, 6, stride=16)
            back2[rows, :] = back2[rows, :] + parts[w][0:6, :]

    for e in range(2):
        @pl.when(core == e)
        def _():
            add_to_line(e, (edge_low, edge_mid) if e == 0 else (edge_mid, edge_high))

    for copy in (*halo, pair_coef, pair_rows, pair_edge):
        copy.wait_send()
    for n, step in enumerate(steps):
        coef_copy(n, chip_at(step)).wait_send()
        edge_copy(n, chip_at(step)).wait_send()
        answer(0, n, chip_at(step)).wait_send()
    for n, zz, j, unit in targets():
        @pl.when(zz != z)
        def _():
            target_copy(n, zz, j, unit).wait_send()

    @pl.when(has[1])
    def _():
        for n, step in enumerate(steps):
            answer(1, n, chip_at(step)).wait_send()
    pair_ends.wait()
    pair_last.wait()
    for e in range(2):
        @pl.when(core == 1 - e)
        def _():
            add_to_line(e, (edge_in[0:8, :], edge_in[8:16, :]))


def w_solver(i, core):
    return (i // 3) * 2 + (i % 3 + core) // 2


def assemble_kernel(sol, back, low, high, out, stage, sem):
    levels = sol.shape[0]
    per = levels // CHUNKS

    def copies(c):
        lev = pl.ds(c * per, per)
        return [
            pltpu.make_async_copy(
                stage.at[f, lev], out.at[f, lev], sem.at[c, f])
            for f in range(3)
        ]

    def chunk(c, carry):
        for g in range(GROUPS):
            rows = slice(8 * g, 8 * g + 8)
            prev = [back[g * 6 + q, 0:8, :] for q in range(6)]
            here = [back[g * 6 + q, 8:16, :] for q in range(6)]
            for l in range(per):
                k = c * per + l
                lo = low[k, rows, :]
                hi = high[k, rows, :]
                for q in range(6):
                    h, f = q // 3, q % 3
                    stage[f, k, rows, 128 * h:128 * h + 128] = sol[k, q, rows, :] + (lo * prev[q] + hi * here[q])
        for copy in copies(c):
            copy.start()
        return carry

    lax.fori_loop(0, CHUNKS, chunk, 0)
    for c in range(CHUNKS):
        for copy in copies(c):
            copy.wait()


def body(n_h, n_d, fields, diffusivity, offsets, coupling, inverse):
    f32 = jnp.float32
    levels = fields.shape[1]
    chips = n_d // 2
    hbm_spec = pl.BlockSpec(memory_space=pltpu.HBM)
    vmem_spec = pl.BlockSpec(memory_space=pltpu.VMEM)
    V = lambda *shape: pltpu.VMEM(shape, f32)
    dma = lambda *shape: pltpu.SemaphoreType.DMA(shape)
    sol, back, low, high = pl.pallas_call(
        functools.partial(columns_kernel, n_h, n_d),
        out_shape=(
            V(levels, 6, LINES, 128),
            V(UNITS + 2, 16, 128),
            V(levels, LINES, 128),
            V(levels, LINES, 128),
        ),
        in_specs=[hbm_spec] * 5,
        out_specs=(vmem_spec,) * 4,
        scratch_shapes=[
            V(levels, 6, PAD, 128),
            V(levels, 2, LINES, 128),
            pltpu.SMEM((LINES,), jnp.int32),
            V(4, levels),
            V(4, levels, levels),
            pltpu.VMEM((GROUPS, 8, 128), jnp.int32),
            V(levels, LINES, 128),
            V(levels, LINES, 128),
            V(2, levels, 8, 128),
            V(2, levels * 6, 128),
            V(2, levels * 6 + 16, 128),
            V(8, 128),
            V(8, 128),
            V(8, 128),
            V(chips, 8, 128),
            V(UNITS, 16, 128),
            V(HALF, 16, 128),
            V(HALF, 16, 128),
            V(HALF + 2, 8, 128),
            V(2, chips, 16, 128),
            V(2, chips, 16, 128),
            V(HALF + 2, 16, 128),
            V(HALF, 16, 128),
            V(2, 16, 128),
            V(16, 128),
            V(2, 8, 128),
            V(chips, 8, 128),
            V(5, chips, 8, 128),
            V(2, 2, chips, 8, 128),
            V(3, 8, 128),
            V(3, 8, 128),
            V(16, 128),
            V(16, 128),
            dma(2, 6),
            dma(CHUNKS, 8),
            dma(3),
            dma(2),
            dma(2),
            dma(5),
            dma(5),
            dma(chips),
            dma(chips),
            dma(HALF),
            dma(2, chips),
            dma(2, chips),
            dma(HALF),
            dma(chips),
            dma(chips),
            pltpu.SemaphoreType.REGULAR((2,)),
        ],
        compiler_params=pltpu.CompilerParams(
            collective_id=0, has_side_effects=True, vmem_limit_bytes=48 * 1024 * 1024),
        name="columns",
    )(*(pltpu.with_memory_space_constraint(x, pltpu.HBM)
        for x in (fields, diffusivity, offsets, coupling, inverse)))
    return pl.pallas_call(
        assemble_kernel,
        out_shape=jax.ShapeDtypeStruct(fields.shape, f32),
        in_specs=[vmem_spec] * 4,
        out_specs=hbm_spec,
        scratch_shapes=[
            V(3, levels, LINES, 256),
            dma(CHUNKS, 3),
        ],
        compiler_params=pltpu.CompilerParams(vmem_limit_bytes=48 * 1024 * 1024),
        name="assemble",
    )(sol, back, low, high)


def solution(mesh):
    return jax.shard_map(
        functools.partial(body, mesh.shape["horiz"], mesh.shape["depth"]),
        mesh=mesh,
        in_specs=(
            P(None, "depth", "horiz", None),
            P("depth", "horiz", None),
            P("horiz"),
            P(None, "depth"),
            P(None, "depth", None),
        ),
        out_specs=P(None, "depth", "horiz", None),
        check_vma=False,
    )
```
